32 devices in a mesh: leaf: 8 (over z, x), rhs: 4 (over y, core).
Axes of the slice: x: 2, y: 2, z: 4, core: 2. Of those that a mesh axis runs over, the one named last changes fastest.
Arguments:
- right_sides: bfloat16 [8192, 4096], P('leaf', 'rhs'), may hold values from -6 to 6
- leaf_inverse: bfloat16 [8192, 1024], P(('leaf', 'rhs')), may hold values from -0.1875 to 0.1875
- project_factors: bfloat16 [3, 8192, 128], P(None, 'leaf'), may hold values from -0.1875 to 0.1875
- correct_factors: bfloat16 [3, 8192, 128], P(None, 'leaf'), may hold values from -0.5 to 0.5
- coupling_first: bfloat16 [4, 256, 256], P(None, 'rhs'), may hold values from -0.375 to 0.375
- coupling_second: bfloat16 [2, 256, 256], P(None, 'rhs'), may hold values from -0.375 to 0.375
- coupling_third: bfloat16 [1, 256, 256], P(None, 'rhs'), may hold values from -0.375 to 0.375
Outputs:
- solution: bfloat16 [8192, 4096], P('leaf', 'rhs')
The draws below stay inside these ranges and needn't reach their ends.
All inputs are finite; a program needn't handle non-finite values.
Results may differ from the reference program's by a relative error of at most 0.014.
Values may be sent and summed in bfloat16 or wider, within the bound.
A program may use at most 64 MiB of HBM per device.

```python
import jax
import jax.numpy as jnp
from jax import lax

LEAF = 1024
R = 128
LEVELS = 3
ORDER = 8192
COLS = 4096
N_LEAF = 8


def block_levels(key, dims, split, low, high):
    loudness, own = 1.0, jax.random.fold_in(key, 6)
    for axis_at, blocks in split:
        draws = jnp.exp(jax.random.uniform(jax.random.fold_in(own, axis_at), (blocks,), jnp.float32, low / len(split), high / len(split)))
        loudness = loudness * jnp.repeat(draws, dims[axis_at] // blocks).reshape([-1 if axis == axis_at else 1 for axis in range(len(dims))])
    return loudness


def normal_values(key, shape, spread, reach, shards=(), dtype=jnp.bfloat16):
    result = jax.random.normal(key, shape, jnp.float32) * spread
    if len(shards) > 0:
        result = block_levels(key, shape, shards, -0.22, 0.18) * result
    return jnp.clip(result, min=-reach, max=reach).astype(dtype)


def setup_inputs(seed: int = 0) -> dict:
    key_of = jax.random.split(jax.random.key(seed), 8)
    right_sides = normal_values(key_of[0], (ORDER, COLS), 1.0, 6.0, ((0, 8), (1, 4)))
    leaf_inverse = normal_values(key_of[1], (ORDER, LEAF), LEAF ** -0.5, 0.1875, ((0, 32),))
    project_factors = normal_values(key_of[2], (LEVELS, ORDER, R), LEAF ** -0.5, 0.1875, ((1, 8),))
    correct_factors = normal_values(key_of[3], (LEVELS, ORDER, R), R ** -0.5, 0.5, ((1, 8),))
    coupling_first = normal_values(key_of[4], (N_LEAF // 2, 2 * R, 2 * R), (2 * R) ** -0.5, 0.375, ((1, 4),))
    coupling_second = normal_values(key_of[5], (N_LEAF // 4, 2 * R, 2 * R), (2 * R) ** -0.5, 0.375, ((1, 4),))
    coupling_third = normal_values(key_of[6], (N_LEAF // 8, 2 * R, 2 * R), (2 * R) ** -0.5, 0.375, ((1, 4),))
    return dict(right_sides=right_sides, leaf_inverse=leaf_inverse, project_factors=project_factors, correct_factors=correct_factors, coupling_first=coupling_first, coupling_second=coupling_second, coupling_third=coupling_third)


def leaf_products(left, right):
    return lax.map(lambda pair: jnp.dot(pair[0], pair[1], preferred_element_type=jnp.float32), (left, right))


def reference(right_sides, leaf_inverse, project_factors, correct_factors, coupling_first, coupling_second, coupling_third):
    count = ORDER // LEAF
    blocks = right_sides.reshape(count, LEAF, COLS)
    inverse = leaf_inverse.reshape(count, LEAF, LEAF)
    start = leaf_products(inverse, blocks).astype(jnp.bfloat16)
    current = start.astype(jnp.float32)
    tables = (coupling_first, coupling_second, coupling_third)
    for level in range(LEVELS):
        rounded = current.astype(jnp.bfloat16)
        factors = project_factors[level].reshape(count, LEAF, R)
        terms = lax.map(lambda pair: jnp.dot(pair[0].T, pair[1], preferred_element_type=jnp.float32), (factors, rounded))
        group = 2 ** level
        projection = jnp.sum(terms.reshape(count // group, group, R, COLS), axis=1).astype(jnp.bfloat16)
        nodes = count // (2 * group)
        stacked = projection.reshape(nodes, 2 * R, COLS)
        answer = leaf_products(tables[level], stacked).astype(jnp.bfloat16)
        children = answer.reshape(2 * nodes, R, COLS)
        per_leaf = jnp.repeat(children, group, axis=0)
        left = correct_factors[level].reshape(count, LEAF, R)
        current = current - leaf_products(left, per_leaf)
    return current.reshape(ORDER, COLS).astype(jnp.bfloat16)
```

```python
import jax
import jax.numpy as jnp
from jax import lax
from jax.experimental import pallas as pl
from jax.experimental.pallas import tpu as pltpu
from jax.sharding import PartitionSpec as P

LEVELS = 3
CHUNKS = 4
PIECES = 4
BF = jnp.bfloat16
F32 = jnp.float32


def mm(a, b):
    return jnp.dot(a, b, preferred_element_type=F32)


def bit_of(index, stride):
    return lax.rem(lax.div(index, stride), 2)


def flip(index, stride):
    return index + stride * (1 - 2 * bit_of(index, stride))


def span(which, size):
    return pl.ds(pl.multiple_of(which * size, size), size)


def kernel(
    b_hbm, a_hbm, p_hbm, c_hbm, w0_hbm, w1_hbm, w2_hbm, out_v,
    b_v, a_v, p_v, pt_v, c_v, w_v, g_v, gs_v, h_v, qf, q_s, q_r, q_v,
    pf, st0, p1f, p1_s, p1_r, p2f, x2_s, x2_r, n_s, n_r, st1, st2, a_cat, start, acc,
    lsem, ssem, rsem,
):
    i = lax.axis_index("leaf")
    r = lax.axis_index("rhs")
    blk = a_hbm.shape[0]
    depth = a_hbm.shape[1]
    cols = b_hbm.shape[1]
    rank = p_hbm.shape[2]
    cw = cols // CHUNKS
    hw = cw // 2
    half = depth // 2
    piece = depth // PIECES
    mate = {"rhs": flip(r, 1)}
    across = {"rhs": flip(r, 2)}
    sib = {"leaf": flip(i, 1)}
    near = {"leaf": flip(i, 2)}
    far = {"leaf": flip(i, 4)}
    diag = {"leaf": flip(flip(i, 1), 2)}
    sides = [bit_of(i, 1), bit_of(i, 2), bit_of(i, 4)]
    core = bit_of(r, 1)
    chip = bit_of(r, 2)

    copies = []

    def send(src, dst, to):
        copy = pltpu.make_async_remote_copy(
            src_ref=src, dst_ref=dst, send_sem=ssem.at[0], recv_sem=rsem.at[len(copies)],
            device_id=to, device_id_type=pl.DeviceIdType.MESH,
        )
        copy.start()
        copies.append(copy)
        return copy

    def share(ref, to):
        return send(ref, ref, to)

    nloc = [0]

    def fetch(src, dst):
        copy = pltpu.make_async_copy(src, dst, lsem.at[nloc[0]])
        nloc[0] += 1
        copy.start()
        return copy

    mine = [span(s, rank) for s in sides]
    block = span(r, blk)
    pair_rows = span(chip, 2 * blk)
    other_rows = span(1 - chip, 2 * blk)
    half_cols = span(core, half)
    rest_cols = span(1 - core, half)

    la = fetch(a_hbm, a_v.at[block, :])
    lp = [fetch(p_hbm.at[0], p_v.at[:, pl.ds(0, rank)])]
    lw = [
        fetch(w_hbm.at[lax.div(i, 2 << level)], w_v.at[level, r])
        for level, w_hbm in enumerate((w0_hbm, w1_hbm, w2_hbm))
    ]
    lp += [fetch(p_hbm.at[l], p_v.at[:, pl.ds(l * rank, rank)]) for l in range(1, LEVELS)]
    lc = [fetch(c_hbm.at[l], c_v.at[:, pl.ds(l * rank, rank)]) for l in range(LEVELS)]
    lb = fetch(b_hbm, b_v)

    barrier = pltpu.get_barrier_semaphore()
    for to in (mate, across, sib, near, far, diag):
        pl.semaphore_signal(barrier, inc=1, device_id=to, device_id_type=pl.DeviceIdType.MESH)
    la.wait()
    pl.semaphore_wait(barrier, 6)

    a_mate = share(a_v.at[block, rest_cols], mate)
    for copy in lw:
        copy.wait()
    w_early = [share(w_v.at[l, r, :, mine[l]], across) for l in range(2)]
    a_mate2 = share(a_v.at[block, half_cols], mate)
    w_mate = share(w_v.at[:, r], mate)
    lp[0].wait()
    pt_v[0] = p_v[:, pl.ds(0, rank)].T
    a_mate.wait_recv()
    q_across = []
    for l in range(LEVELS):
        if l > 0:
            lp[l].wait()
            pt_v[l] = p_v[:, pl.ds(l * rank, rank)].T
        part = mm(pt_v[l, :, pair_rows], a_v[pair_rows, half_cols])
        qf[l] = part
        q_s[l] = part.astype(BF)
        q_across.append(send(q_s.at[l], q_r.at[l], across))
    w_late = [share(w_v.at[l, r, :, span(1 - sides[l], rank)], across) for l in range(2)]
    w_late.append(share(w_v.at[2, r], across))
    a_across = [share(a_v.at[block, pl.ds(k * piece, piece)], across) for k in range(PIECES)]

    for copy in lc:
        copy.wait()
    for n, (l, k) in enumerate(((1, 0), (2, 0), (2, 1))):
        g_v[n, :, mine[0]] = mm(pt_v[l], c_v[:, pl.ds(k * rank, rank)]).astype(BF)
    g_send = share(g_v.at[:, :, mine[0]], sib)

    over = flip(r, 2)
    w_relay = []
    for l in range(2):
        w_early[l].wait_recv()
        w_relay.append(share(w_v.at[l, over, :, mine[l]], mate))
    lb.wait()
    a_mate2.wait_recv()
    for c in range(CHUNKS):
        own = pl.ds(c * cw, cw)
        start[:, own] = mm(a_v[pair_rows, :], b_v[:, own])

    def gather_q(l):
        q_across[l].wait_recv()
        q_v[l, core] = (qf[l] + q_r[l].astype(F32)).astype(BF)
        relayed = share(q_v.at[l, core], mate)
        for c in range(CHUNKS):
            pf[c] = mm(q_v[l, core], b_v[half_cols, pl.ds(c * cw, cw)])
        relayed.wait_recv()

    def project(l, c):
        return pf[c] + mm(q_v[l, 1 - core], b_v[rest_cols, pl.ds(c * cw, cw)])

    x0, x1, x2 = {}, {}, {}

    def send0(c):
        x0[c] = share(st0.at[c, mine[0], :], sib)

    def send1(c):
        x1[c] = send(p1_s.at[c], p1_r.at[c], sib)

    gather_q(0)
    for c in range(CHUNKS):
        st0[c, mine[0], :] = project(0, c).astype(BF)
        if c < CHUNKS // 2:
            send0(c)

    w_mate.wait_recv()
    g_send.wait_recv()
    w_relay[0].wait_recv()
    w_cols = w_v[0, :, :, mine[0]].reshape(2 * rank, rank)
    for n in range(2):
        h_v[n] = mm(g_v[n], w_cols).astype(BF)
    pair_sum = g_v[2, :, pl.ds(0, rank)].astype(F32) + g_v[2, :, pl.ds(rank, rank)].astype(F32)
    gs_v[:, mine[1]] = pair_sum.astype(BF)
    gs_send = share(gs_v.at[:, mine[1]], near)

    gather_q(1)
    for c in range(CHUNKS):
        part = project(1, c) - mm(h_v[0], st0[c, mine[0], :])
        p1f[c] = part
        p1_s[c] = part.astype(BF)
        if c < CHUNKS // 2:
            send1(c)

    w_relay[1].wait_recv()
    gs_send.wait_recv()
    h_v[2] = mm(gs_v[...], w_v[1, :, :, mine[1]].reshape(2 * rank, rank)).astype(BF)

    gather_q(2)
    keep = span(sides[0], hw)
    give = span(1 - sides[0], hw)
    for c in range(CHUNKS):
        p2f[c] = project(2, c) - mm(h_v[1], st0[c, mine[0], :]) - mm(h_v[2], p1_s[c])
        x2_s[c] = p2f[c, :, give].astype(BF)
        if c % 2 == 1:
            two = pl.ds(c - 1, 2)
            x2[c // 2] = send(x2_s.at[two], x2_r.at[two], sib)
    for c in range(CHUNKS // 2, CHUNKS):
        send1(c)
    for c in range(CHUNKS // 2, CHUNKS):
        send0(c)
    for l in range(3):
        w_late[l].wait_recv()
        lanes = span(1 - sides[l], rank) if l < 2 else pl.ds(0, 2 * rank)
        w_relay.append(share(w_v.at[l, over, :, lanes], mate))

    def answer_rows(l):
        return w_v[l, pl.ds(pl.multiple_of(sides[l] * 2, 2), 2), :, :].reshape(rank, 2 * rank)

    z1, n1, f1, n2, relay = {}, {}, {}, {}, {}

    def first(c):
        x0[c].wait_recv()
        a_cat[c, pl.ds(0, rank), :] = mm(answer_rows(0), st0[c]).astype(BF)

    def second_sum(c):
        x1[c].wait_recv()
        st1[c, mine[1], :] = (p1f[c] + p1_r[c].astype(F32)).astype(BF)
        z1[c] = share(st1.at[c, mine[1], :], near)

    def second(c):
        z1[c].wait_recv()
        a_cat[c, pl.ds(rank, rank), :] = mm(answer_rows(1), st1[c]).astype(BF)

    def third_near(j):
        x2[j].wait_recv()
        theirs = 2 * j + 1 - sides[1]
        n_s[j] = (p2f[theirs, :, keep] + x2_r[theirs].astype(F32)).astype(BF)
        n1[j] = send(n_s.at[j], n_r.at[j], near)

    def third_far(j):
        n1[j].wait_recv()
        ours = 2 * j + sides[1]
        total = p2f[ours, :, keep] + x2_r[ours].astype(F32) + n_r[j].astype(F32)
        st2[j, mine[2], :] = total.astype(BF)
        f1[j] = share(st2.at[j, mine[2], :], far)

    def third(j):
        f1[j].wait_recv()
        spot = (2 * j + sides[1], pl.ds(2 * rank, rank), keep)
        a_cat[spot] = mm(answer_rows(2), st2[j]).astype(BF)
        n2[j] = [share(a_cat.at[spot], to) for to in (diag, sib, near)]

    def relay_piece(k):
        a_across[k].wait_recv()
        relay[k] = share(a_v.at[span(over, blk), pl.ds(k * piece, piece)], mate)

    def add_pieces(k, count, fresh):
        deep = pl.ds(k * piece, count * piece)
        for c in range(CHUNKS):
            own = pl.ds(c * cw, cw)
            part = mm(a_v[other_rows, deep], b_v[deep, own])
            acc[:, own] = part if fresh else acc[:, own] + part

    def finish_ours(c):
        own = pl.ds(c * cw, cw)
        out_v[pair_rows, own] = (start[:, own] - mm(c_v[pair_rows, :], a_cat[c])).astype(BF)

    def finish_theirs(c):
        own = pl.ds(c * cw, cw)
        deep = pl.ds((PIECES - 1) * piece, piece)
        last = mm(a_v[other_rows, deep], b_v[deep, own]) - mm(c_v[other_rows, :], a_cat[c])
        out_v[other_rows, own] = (acc[:, own] + last).astype(BF)

    second_sum(0)
    second_sum(1)
    third_near(0)
    for l in range(2, 5):
        w_relay[l].wait_recv()
    first(0)
    first(1)
    third_near(1)
    second(0)
    second(1)
    relay_piece(0)
    third_far(0)
    second_sum(2)
    third_far(1)
    relay_piece(1)
    second_sum(3)
    relay[0].wait_recv()
    relay[1].wait_recv()
    add_pieces(0, 2, True)
    third(0)
    first(2)
    second(2)
    third(1)
    relay_piece(2)
    first(3)
    second(3)
    relay[2].wait_recv()
    add_pieces(2, 1, False)
    relay_piece(3)
    for j in range(CHUNKS // 2):
        for copy in n2[j]:
            copy.wait_recv()
        finish_ours(2 * j)
        finish_ours(2 * j + 1)
    relay[3].wait_recv()
    for c in range(CHUNKS):
        finish_theirs(c)
    for copy in copies:
        copy.wait_send()


def local(right_sides, leaf_inverse, project_factors, correct_factors, *couplings):
    rows, cols = right_sides.shape
    blk, depth = leaf_inverse.shape
    levels, _, rank = project_factors.shape
    parts = lax.axis_size("rhs")
    cw = cols // CHUNKS
    whole = lambda dtype: pltpu.VMEM((CHUNKS, rank, cw), dtype)
    thin = lambda dtype: pltpu.VMEM((CHUNKS, rank, cw // 2), dtype)
    part = lambda dtype: pltpu.VMEM((CHUNKS // 2, rank, cw // 2), dtype)
    any_spec = pl.BlockSpec(memory_space=pltpu.HBM)
    return pl.pallas_call(
        kernel,
        out_shape=jax.ShapeDtypeStruct((rows, cols), BF),
        in_specs=[any_spec] * 7,
        out_specs=pl.BlockSpec(memory_space=pltpu.VMEM),
        scratch_shapes=[
            pltpu.VMEM((rows, cols), BF),
            pltpu.VMEM((rows, depth), BF),
            pltpu.VMEM((rows, levels * rank), BF),
            pltpu.VMEM((levels, rank, rows), BF),
            pltpu.VMEM((rows, levels * rank), BF),
            pltpu.VMEM((levels, parts) + couplings[0].shape[1:], BF),
            pltpu.VMEM((3, rank, 2 * rank), BF),
            pltpu.VMEM((rank, 2 * rank), BF),
            pltpu.VMEM((3, rank, rank), BF),
            pltpu.VMEM((levels, rank, depth // 2), F32),
            pltpu.VMEM((levels, rank, depth // 2), BF),
            pltpu.VMEM((levels, rank, depth // 2), BF),
            pltpu.VMEM((levels, 2, rank, depth // 2), BF),
            whole(F32),
            pltpu.VMEM((CHUNKS, 2 * rank, cw), BF),
            whole(F32), whole(BF), whole(BF), whole(F32), thin(BF), thin(BF), part(BF), part(BF),
            pltpu.VMEM((CHUNKS, 2 * rank, cw), BF),
            pltpu.VMEM((CHUNKS // 2, 2 * rank, cw // 2), BF),
            pltpu.VMEM((CHUNKS, levels * rank, cw), BF),
            pltpu.VMEM((rows // 2, cols), F32),
            pltpu.VMEM((rows // 2, cols), F32),
            pltpu.SemaphoreType.DMA((11,)),
            pltpu.SemaphoreType.DMA((1,)),
            pltpu.SemaphoreType.DMA((60,)),
        ],
        compiler_params=pltpu.CompilerParams(
            collective_id=0, has_side_effects=True, vmem_limit_bytes=56 * 1024 * 1024
        ),
    )(*(
        pltpu.with_memory_space_constraint(x, pltpu.HBM)
        for x in (right_sides, leaf_inverse, project_factors, correct_factors, *couplings)
    ))


def solution(mesh):
    in_specs = (
        P("leaf", "rhs"),
        P(("leaf", "rhs"), None),
        P(None, "leaf", None),
        P(None, "leaf", None),
        P(None, "rhs", None),
        P(None, "rhs", None),
        P(None, "rhs", None),
    )
    out_specs = P("leaf", "rhs")
    return jax.shard_map(local, mesh=mesh, in_specs=in_specs, out_specs=out_specs, check_vma=False)
```

```python
import jax
import jax.numpy as jnp
from jax import lax
from jax.experimental import pallas as pl
from jax.experimental.pallas import tpu as pltpu
from jax.sharding import PartitionSpec as P

LEVELS = 3
CHUNKS = 4
PIECES = 4
BF = jnp.bfloat16
F32 = jnp.float32


def mm(a, b):
    return jnp.dot(a, b, preferred_element_type=F32)


def bit_of(index, stride):
    return lax.rem(lax.div(index, stride), 2)


def flip(index, stride):
    return index + stride * (1 - 2 * bit_of(index, stride))


def span(which, size):
    return pl.ds(pl.multiple_of(which * size, size), size)


def kernel(
    b_hbm, a_hbm, p_hbm, c_hbm, w0_hbm, w1_hbm, w2_hbm, out_v,
    b_v, a_v, p_v, pt_v, c_v, w_v, g_v, gs_v, h_v, qf, q_s, q_r, q_v,
    pf, st0, p1f, p1_s, p1_r, p2f, p2_s, p2_r, st1, st2, a_cat, acc,
    lsem, ssem, rsem,
):
    i = lax.axis_index("leaf")
    r = lax.axis_index("rhs")
    blk = a_hbm.shape[0]
    depth = a_hbm.shape[1]
    cols = b_hbm.shape[1]
    rank = p_hbm.shape[2]
    cw = cols // CHUNKS
    hw = cw // 2
    half = depth // 2
    piece = depth // PIECES
    mate = {"rhs": flip(r, 1)}
    across = {"rhs": flip(r, 2)}
    sib = {"leaf": flip(i, 1)}
    near = {"leaf": flip(i, 2)}
    far = {"leaf": flip(i, 4)}
    diag = {"leaf": flip(flip(i, 1), 2)}
    sides = [bit_of(i, 1), bit_of(i, 2), bit_of(i, 4)]
    core = bit_of(r, 1)
    chip = bit_of(r, 2)

    copies = []

    def send(src, dst, to):
        copy = pltpu.make_async_remote_copy(
            src_ref=src, dst_ref=dst, send_sem=ssem.at[0], recv_sem=rsem.at[len(copies)],
            device_id=to, device_id_type=pl.DeviceIdType.MESH,
        )
        copy.start()
        copies.append(copy)
        return copy

    def share(ref, to):
        return send(ref, ref, to)

    nloc = [0]

    def fetch(src, dst):
        copy = pltpu.make_async_copy(src, dst, lsem.at[nloc[0]])
        nloc[0] += 1
        copy.start()
        return copy

    mine = [span(s, rank) for s in sides]
    block = span(r, blk)
    pair_rows = span(chip, 2 * blk)
    other_rows = span(1 - chip, 2 * blk)
    half_cols = span(core, half)
    rest_cols = span(1 - core, half)

    la = fetch(a_hbm, a_v.at[block, :])
    lp = [fetch(p_hbm.at[0], p_v.at[:, pl.ds(0, rank)])]
    lw = [
        fetch(w_hbm.at[lax.div(i, 2 << level)], w_v.at[level, r])
        for level, w_hbm in enumerate((w0_hbm, w1_hbm, w2_hbm))
    ]
    lp += [fetch(p_hbm.at[l], p_v.at[:, pl.ds(l * rank, rank)]) for l in range(1, LEVELS)]
    lc = [fetch(c_hbm.at[l], c_v.at[:, pl.ds(l * rank, rank)]) for l in range(LEVELS)]
    lb = fetch(b_hbm, b_v)

    barrier = pltpu.get_barrier_semaphore()
    for to in (mate, across, sib, near, far, diag):
        pl.semaphore_signal(barrier, inc=1, device_id=to, device_id_type=pl.DeviceIdType.MESH)
    la.wait()
    pl.semaphore_wait(barrier, 6)

    a_mate = share(a_v.at[block, rest_cols], mate)
    for copy in lw:
        copy.wait()
    w_early = [share(w_v.at[l, r, :, mine[l]], across) for l in range(2)]
    lp[0].wait()
    pt_v[0] = p_v[:, pl.ds(0, rank)].T
    a_mate.wait_recv()
    q_across = []
    for l in range(LEVELS):
        if l > 0:
            lp[l].wait()
            pt_v[l] = p_v[:, pl.ds(l * rank, rank)].T
        part = mm(pt_v[l, :, pair_rows], a_v[pair_rows, half_cols])
        qf[l] = part
        q_s[l] = part.astype(BF)
        q_across.append(send(q_s.at[l], q_r.at[l], across))
    a_mate2 = share(a_v.at[block, half_cols], mate)
    w_mate = share(w_v.at[:, r], mate)
    w_late = [share(w_v.at[l, r, :, span(1 - sides[l], rank)], across) for l in range(2)]
    w_late.append(share(w_v.at[2, r], across))
    a_across = [share(a_v.at[block, pl.ds(k * piece, piece)], across) for k in range(PIECES)]

    for copy in lc:
        copy.wait()
    for n, (l, k) in enumerate(((1, 0), (2, 0), (2, 1))):
        g_v[n, :, mine[0]] = mm(pt_v[l], c_v[:, pl.ds(k * rank, rank)]).astype(BF)
    g_send = share(g_v.at[:, :, mine[0]], sib)

    over = flip(r, 2)
    w_relay = []
    for l in range(2):
        w_early[l].wait_recv()
        w_relay.append(share(w_v.at[l, over, :, mine[l]], mate))
    lb.wait()
    a_mate2.wait_recv()
    for c in range(CHUNKS):
        own = pl.ds(c * cw, cw)
        acc[pair_rows, own] = mm(a_v[pair_rows, :], b_v[:, own])

    def gather_q(l):
        q_across[l].wait_recv()
        q_v[l, core] = (qf[l] + q_r[l].astype(F32)).astype(BF)
        relayed = share(q_v.at[l, core], mate)
        for c in range(CHUNKS):
            pf[c] = mm(q_v[l, core], b_v[half_cols, pl.ds(c * cw, cw)])
        relayed.wait_recv()

    def project(l, c):
        return pf[c] + mm(q_v[l, 1 - core], b_v[rest_cols, span(c, cw)])

    x0, x1, x2 = {}, {}, {}

    def send0(c):
        x0[c] = share(st0.at[c, mine[0], :], sib)

    def send1(c):
        x1[c] = send(p1_s.at[c], p1_r.at[c], sib)

    gather_q(0)
    for c in range(CHUNKS):
        st0[c, mine[0], :] = project(0, c).astype(BF)
        if c < CHUNKS // 2:
            send0(c)

    w_mate.wait_recv()
    g_send.wait_recv()
    w_relay[0].wait_recv()
    w_cols = w_v[0, :, :, mine[0]].reshape(2 * rank, rank)
    for n in range(2):
        h_v[n] = mm(g_v[n], w_cols).astype(BF)
    pair_sum = g_v[2, :, pl.ds(0, rank)].astype(F32) + g_v[2, :, pl.ds(rank, rank)].astype(F32)
    gs_v[:, mine[1]] = pair_sum.astype(BF)
    gs_send = share(gs_v.at[:, mine[1]], near)

    gather_q(1)
    for c in range(CHUNKS):
        part = project(1, c) - mm(h_v[0], st0[c, mine[0], :])
        p1f[c] = part
        p1_s[c] = part.astype(BF)
        if c < CHUNKS // 2:
            send1(c)

    w_relay[1].wait_recv()
    gs_send.wait_recv()
    h_v[2] = mm(gs_v[...], w_v[1, :, :, mine[1]].reshape(2 * rank, rank)).astype(BF)

    gather_q(2)
    spot = 2 * sides[1] + sides[0]
    for n, (to, who) in enumerate(((diag, 3 - spot), (sib, flip(spot, 1)), (near, flip(spot, 2)), (None, spot))):
        part = project(2, who) - mm(h_v[1], st0[who, mine[0], :]) - mm(h_v[2], p1_s[who])
        if to is None:
            p2f[...] = part
        else:
            p2_s[n] = part.astype(BF)
            x2[n] = send(p2_s.at[n], p2_r.at[n], to)
    for c in range(CHUNKS // 2, CHUNKS):
        send1(c)
    for c in range(CHUNKS // 2, CHUNKS):
        send0(c)
    for l in range(3):
        w_late[l].wait_recv()
        lanes = span(1 - sides[l], rank) if l < 2 else pl.ds(0, 2 * rank)
        w_relay.append(share(w_v.at[l, over, :, lanes], mate))

    def answer_rows(l):
        return w_v[l, pl.ds(pl.multiple_of(sides[l] * 2, 2), 2), :, :].reshape(rank, 2 * rank)

    z1, f1, n2, relay = {}, {}, {}, {}

    def first(c):
        x0[c].wait_recv()
        a_cat[c, pl.ds(0, rank), :] = mm(answer_rows(0), st0[c]).astype(BF)

    def second_sum(c):
        x1[c].wait_recv()
        st1[c, mine[1], :] = (p1f[c] + p1_r[c].astype(F32)).astype(BF)
        z1[c] = share(st1.at[c, mine[1], :], near)

    def second(c):
        z1[c].wait_recv()
        a_cat[c, pl.ds(rank, rank), :] = mm(answer_rows(1), st1[c]).astype(BF)

    def third_far():
        for n in range(3):
            x2[n].wait_recv()
        for j in range(2):
            lanes = pl.ds(j * hw, hw)
            total = p2f[:, lanes]
            for n in range(3):
                total = total + p2_r[n, :, lanes].astype(F32)
            st2[j, mine[2], :] = total.astype(BF)
            f1[j] = share(st2.at[j, mine[2], :], far)

    def third(j):
        f1[j].wait_recv()
        where = (spot, pl.ds(2 * rank, rank), pl.ds(j * hw, hw))
        a_cat[where] = mm(answer_rows(2), st2[j]).astype(BF)
        n2[j] = [share(a_cat.at[where], to) for to in (diag, sib, near)]

    def relay_piece(k):
        a_across[k].wait_recv()
        relay[k] = share(a_v.at[span(over, blk), pl.ds(k * piece, piece)], mate)

    def add_pieces(k, count, fresh):
        deep = pl.ds(k * piece, count * piece)
        for c in range(CHUNKS):
            own = pl.ds(c * cw, cw)
            part = mm(a_v[other_rows, deep], b_v[deep, own])
            acc[other_rows, own] = part if fresh else acc[other_rows, own] + part

    def take_two(c, rows):
        own = pl.ds(c * cw, cw)
        acc[rows, own] = acc[rows, own] - mm(c_v[rows, pl.ds(0, 2 * rank)], a_cat[c, pl.ds(0, 2 * rank), :])

    def finish(c):
        own = pl.ds(c * cw, cw)
        last = mm(c_v[:, pl.ds(2 * rank, rank)], a_cat[c, pl.ds(2 * rank, rank), :])
        out_v[:, own] = (acc[:, own] - last).astype(BF)

    second_sum(0)
    second_sum(1)
    for l in range(2, 5):
        w_relay[l].wait_recv()
    first(0)
    first(1)
    relay_piece(0)
    third_far()
    second(0)
    second(1)
    take_two(0, pair_rows)
    take_two(1, pair_rows)
    relay_piece(1)
    relay[0].wait_recv()
    add_pieces(0, 1, True)
    take_two(0, other_rows)
    take_two(1, other_rows)
    second_sum(2)
    third(0)
    second_sum(3)
    third(1)
    relay_piece(2)
    relay[1].wait_recv()
    add_pieces(1, 1, False)
    for c in (2, 3):
        second(c)
        first(c)
        take_two(c, pair_rows)
        take_two(c, other_rows)
    relay_piece(3)
    relay[2].wait_recv()
    add_pieces(2, 1, False)
    relay[3].wait_recv()
    add_pieces(3, 1, False)
    for j in range(2):
        for copy in n2[j]:
            copy.wait_recv()
    for c in range(CHUNKS):
        finish(c)
    for copy in copies:
        copy.wait_send()


def local(right_sides, leaf_inverse, project_factors, correct_factors, *couplings):
    rows, cols = right_sides.shape
    blk, depth = leaf_inverse.shape
    levels, _, rank = project_factors.shape
    parts = lax.axis_size("rhs")
    cw = cols // CHUNKS
    whole = lambda dtype: pltpu.VMEM((CHUNKS, rank, cw), dtype)
    any_spec = pl.BlockSpec(memory_space=pltpu.HBM)
    return pl.pallas_call(
        kernel,
        out_shape=jax.ShapeDtypeStruct((rows, cols), BF),
        in_specs=[any_spec] * 7,
        out_specs=pl.BlockSpec(memory_space=pltpu.VMEM),
        scratch_shapes=[
            pltpu.VMEM((rows, cols), BF),
            pltpu.VMEM((rows, depth), BF),
            pltpu.VMEM((rows, levels * rank), BF),
            pltpu.VMEM((levels, rank, rows), BF),
            pltpu.VMEM((rows, levels * rank), BF),
            pltpu.VMEM((levels, parts) + couplings[0].shape[1:], BF),
            pltpu.VMEM((3, rank, 2 * rank), BF),
            pltpu.VMEM((rank, 2 * rank), BF),
            pltpu.VMEM((3, rank, rank), BF),
            pltpu.VMEM((levels, rank, depth // 2), F32),
            pltpu.VMEM((levels, rank, depth // 2), BF),
            pltpu.VMEM((levels, rank, depth // 2), BF),
            pltpu.VMEM((levels, 2, rank, depth // 2), BF),
            whole(F32),
            pltpu.VMEM((CHUNKS, 2 * rank, cw), BF),
            whole(F32), whole(BF), whole(BF),
            pltpu.VMEM((rank, cw), F32), pltpu.VMEM((3, rank, cw), BF), pltpu.VMEM((3, rank, cw), BF),
            pltpu.VMEM((CHUNKS, 2 * rank, cw), BF),
            pltpu.VMEM((2, 2 * rank, cw // 2), BF),
            pltpu.VMEM((CHUNKS, levels * rank, cw), BF),
            pltpu.VMEM((rows, cols), F32),
            pltpu.SemaphoreType.DMA((11,)),
            pltpu.SemaphoreType.DMA((1,)),
            pltpu.SemaphoreType.DMA((52,)),
        ],
        compiler_params=pltpu.CompilerParams(
            collective_id=0, has_side_effects=True, vmem_limit_bytes=40 * 1024 * 1024
        ),
    )(*(
        pltpu.with_memory_space_constraint(x, pltpu.HBM)
        for x in (right_sides, leaf_inverse, project_factors, correct_factors, *couplings)
    ))


def solution(mesh):
    in_specs = (
        P("leaf", "rhs"),
        P(("leaf", "rhs"), None),
        P(None, "leaf", None),
        P(None, "leaf", None),
        P(None, "rhs", None),
        P(None, "rhs", None),
        P(None, "rhs", None),
    )
    out_specs = P("leaf", "rhs")
    return jax.shard_map(local, mesh=mesh, in_specs=in_specs, out_specs=out_specs, check_vma=False)
```

```python
import jax
import jax.numpy as jnp
from jax import lax
from jax.experimental import pallas as pl
from jax.experimental.pallas import tpu as pltpu
from jax.sharding import PartitionSpec as P

LEVELS = 3
CHUNKS = 4
PIECES = 4
BF = jnp.bfloat16
F32 = jnp.float32


def mm(a, b):
    return jnp.dot(a, b, preferred_element_type=F32)


def bit_of(index, stride):
    return lax.rem(lax.div(index, stride), 2)


def flip(index, stride):
    return index + stride * (1 - 2 * bit_of(index, stride))


def span(which, size):
    return pl.ds(pl.multiple_of(which * size, size), size)


def kernel(
    b_hbm, a_hbm, p_hbm, c_hbm, w0_hbm, w1_hbm, w2_hbm, out_v,
    b_v, a_v, p_v, pt_v, w_v, g_v, gs_v, h_v, qf, q_s, q_r, q_v,
    pf, st0, p1f, p1_s, p1_r, p2f, p2_s, p2_r, st1, st2, acc,
    lsem, ssem, rsem,
):
    i = lax.axis_index("leaf")
    r = lax.axis_index("rhs")
    blk = a_hbm.shape[0]
    depth = a_hbm.shape[1]
    cols = b_hbm.shape[1]
    rank = p_hbm.shape[2]
    cw = cols // CHUNKS
    hw = cw // 2
    half = depth // 2
    piece = depth // PIECES
    mate = {"rhs": flip(r, 1)}
    across = {"rhs": flip(r, 2)}
    sib = {"leaf": flip(i, 1)}
    near = {"leaf": flip(i, 2)}
    far = {"leaf": flip(i, 4)}
    diag = {"leaf": flip(flip(i, 1), 2)}
    sides = [bit_of(i, 1), bit_of(i, 2), bit_of(i, 4)]
    core = bit_of(r, 1)
    chip = bit_of(r, 2)

    copies = []

    def send(src, dst, to):
        copy = pltpu.make_async_remote_copy(
            src_ref=src, dst_ref=dst, send_sem=ssem.at[0], recv_sem=rsem.at[len(copies)],
            device_id=to, device_id_type=pl.DeviceIdType.MESH,
        )
        copy.start()
        copies.append(copy)
        return copy

    def share(ref, to):
        return send(ref, ref, to)

    nloc = [0]

    def fetch(src, dst):
        copy = pltpu.make_async_copy(src, dst, lsem.at[nloc[0]])
        nloc[0] += 1
        copy.start()
        return copy

    mine = [span(s, rank) for s in sides]
    block = span(r, blk)
    pair_rows = span(chip, 2 * blk)
    other_rows = span(1 - chip, 2 * blk)
    half_cols = span(core, half)
    rest_cols = span(1 - core, half)

    la = fetch(a_hbm, a_v.at[block, pl.ds(0, depth)])
    lp = [fetch(p_hbm.at[0], p_v.at[:, pl.ds(0, rank)])]
    lw = [
        fetch(w_hbm.at[lax.div(i, 2 << level)], w_v.at[level, r])
        for level, w_hbm in enumerate((w0_hbm, w1_hbm, w2_hbm))
    ]
    lp += [fetch(p_hbm.at[l], p_v.at[:, pl.ds(l * rank, rank)]) for l in range(1, LEVELS)]
    lc = [fetch(c_hbm.at[l], a_v.at[:, pl.ds(depth + l * rank, rank)]) for l in range(LEVELS)]
    lb = fetch(b_hbm, b_v.at[pl.ds(0, depth)])

    barrier = pltpu.get_barrier_semaphore()
    for to in (mate, across, sib, near, far, diag):
        pl.semaphore_signal(barrier, inc=1, device_id=to, device_id_type=pl.DeviceIdType.MESH)
    la.wait()
    pl.semaphore_wait(barrier, 6)

    a_mate = share(a_v.at[block, rest_cols], mate)
    for copy in lw:
        copy.wait()
    w_early = [share(w_v.at[l, r, :, mine[l]], across) for l in range(2)]
    lp[0].wait()
    pt_v[0] = p_v[:, pl.ds(0, rank)].T
    a_mate.wait_recv()
    q_across = []
    for l in range(LEVELS):
        if l > 0:
            lp[l].wait()
            pt_v[l] = p_v[:, pl.ds(l * rank, rank)].T
        part = mm(pt_v[l, :, pair_rows], a_v[pair_rows, half_cols])
        qf[l] = part
        q_s[l] = part.astype(BF)
        q_across.append(send(q_s.at[l], q_r.at[l], across))
    a_mate2 = share(a_v.at[block, half_cols], mate)
    w_mate = share(w_v.at[:, r], mate)
    w_late = [share(w_v.at[l, r, :, span(1 - sides[l], rank)], across) for l in range(2)]
    w_late.append(share(w_v.at[2, r], across))
    a_across = [share(a_v.at[block, pl.ds(k * piece, piece)], across) for k in range(PIECES)]

    for copy in lc:
        copy.wait()
    for n, (l, k) in enumerate(((1, 0), (2, 0), (2, 1))):
        g_v[n, :, mine[0]] = mm(pt_v[l], a_v[:, pl.ds(depth + k * rank, rank)]).astype(BF)
    g_send = share(g_v.at[:, :, mine[0]], sib)

    over = flip(r, 2)
    w_relay = []
    for l in range(2):
        w_early[l].wait_recv()
        w_relay.append(share(w_v.at[l, over, :, mine[l]], mate))
    lb.wait()
    a_mate2.wait_recv()
    for c in range(CHUNKS):
        own = pl.ds(c * cw, cw)
        acc[pair_rows, own] = mm(a_v[pair_rows, pl.ds(0, depth)], b_v[pl.ds(0, depth), own])

    def gather_q(l):
        q_across[l].wait_recv()
        q_v[l, core] = (qf[l] + q_r[l].astype(F32)).astype(BF)
        relayed = share(q_v.at[l, core], mate)
        for c in range(CHUNKS):
            pf[c] = mm(q_v[l, core], b_v[half_cols, pl.ds(c * cw, cw)])
        relayed.wait_recv()

    def project(l, c):
        return pf[c] + mm(q_v[l, 1 - core], b_v[rest_cols, span(c, cw)])

    x0, x1, x2 = {}, {}, {}

    def send0(c):
        x0[c] = share(st0.at[c, mine[0], :], sib)

    def send1(c):
        x1[c] = send(p1_s.at[c], p1_r.at[c], sib)

    gather_q(0)
    for c in range(CHUNKS):
        st0[c, mine[0], :] = project(0, c).astype(BF)
        if c < CHUNKS // 2:
            send0(c)

    w_mate.wait_recv()
    g_send.wait_recv()
    w_relay[0].wait_recv()
    w_cols = w_v[0, :, :, mine[0]].reshape(2 * rank, rank)
    for n in range(2):
        h_v[n] = mm(g_v[n], w_cols).astype(BF)
    pair_sum = g_v[2, :, pl.ds(0, rank)].astype(F32) + g_v[2, :, pl.ds(rank, rank)].astype(F32)
    gs_v[:, mine[1]] = pair_sum.astype(BF)
    gs_send = share(gs_v.at[:, mine[1]], near)

    gather_q(1)
    for c in range(CHUNKS):
        part = project(1, c) - mm(h_v[0], st0[c, mine[0], :])
        p1f[c] = part
        p1_s[c] = part.astype(BF)
        if c < CHUNKS // 2:
            send1(c)

    w_relay[1].wait_recv()
    gs_send.wait_recv()
    h_v[2] = mm(gs_v[...], w_v[1, :, :, mine[1]].reshape(2 * rank, rank)).astype(BF)

    gather_q(2)
    spot = 2 * sides[1] + sides[0]
    for n, (to, who) in enumerate(((diag, 3 - spot), (sib, flip(spot, 1)), (near, flip(spot, 2)), (None, spot))):
        part = project(2, who) - mm(h_v[1], st0[who, mine[0], :]) - mm(h_v[2], p1_s[who])
        if to is None:
            p2f[...] = part
        else:
            p2_s[n] = part.astype(BF)
            x2[n] = send(p2_s.at[n], p2_r.at[n], to)
    for c in range(CHUNKS // 2, CHUNKS):
        send1(c)
    for c in range(CHUNKS // 2, CHUNKS):
        send0(c)
    for l in range(3):
        w_late[l].wait_recv()
        lanes = span(1 - sides[l], rank) if l < 2 else pl.ds(0, 2 * rank)
        w_relay.append(share(w_v.at[l, over, :, lanes], mate))

    def answer_rows(l):
        return w_v[l, pl.ds(pl.multiple_of(sides[l] * 2, 2), 2), :, :].reshape(rank, 2 * rank)

    z1, f1, n2, relay = {}, {}, {}, {}

    def first(c):
        x0[c].wait_recv()
        b_v[pl.ds(depth, rank), pl.ds(c * cw, cw)] = (-mm(answer_rows(0), st0[c])).astype(BF)

    def second_sum(c):
        x1[c].wait_recv()
        st1[c, mine[1], :] = (p1f[c] + p1_r[c].astype(F32)).astype(BF)
        z1[c] = share(st1.at[c, mine[1], :], near)

    def second(c):
        z1[c].wait_recv()
        b_v[pl.ds(depth + rank, rank), pl.ds(c * cw, cw)] = (-mm(answer_rows(1), st1[c])).astype(BF)

    def third_far():
        for n in range(3):
            x2[n].wait_recv()
        for j in range(2):
            lanes = pl.ds(j * hw, hw)
            total = p2f[:, lanes]
            for n in range(3):
                total = total + p2_r[n, :, lanes].astype(F32)
            st2[j, mine[2], :] = total.astype(BF)
            f1[j] = share(st2.at[j, mine[2], :], far)

    def third(j):
        f1[j].wait_recv()
        where = (pl.ds(depth + 2 * rank, rank), span(2 * spot + j, hw))
        b_v[where] = (-mm(answer_rows(2), st2[j])).astype(BF)
        n2[j] = [share(b_v.at[where], to) for to in (diag, sib, near)]

    def relay_piece(k):
        a_across[k].wait_recv()
        relay[k] = share(a_v.at[span(over, blk), pl.ds(k * piece, piece)], mate)

    early = depth - piece

    def add_pieces():
        for c in range(CHUNKS):
            own = pl.ds(c * cw, cw)
            acc[other_rows, own] = mm(a_v[other_rows, pl.ds(0, early)], b_v[pl.ds(0, early), own])

    def finish(c, rows, start):
        own = pl.ds(c * cw, cw)
        deep = pl.ds(start, depth + LEVELS * rank - start)
        out_v[rows, own] = (acc[rows, own] + mm(a_v[rows, deep], b_v[deep, own])).astype(BF)

    second_sum(0)
    second_sum(1)
    for l in range(2, 5):
        w_relay[l].wait_recv()
    first(0)
    first(1)
    relay_piece(0)
    third_far()
    relay_piece(1)
    second_sum(2)
    second(0)
    second_sum(3)
    second(1)
    relay_piece(2)
    third(0)
    third(1)
    first(2)
    first(3)
    for k in range(3):
        relay[k].wait_recv()
    add_pieces()
    second(2)
    relay_piece(3)
    second(3)
    for j in range(2):
        for copy in n2[j]:
            copy.wait_recv()
    for c in range(CHUNKS):
        finish(c, pair_rows, depth)
    relay[3].wait_recv()
    for c in range(CHUNKS):
        finish(c, other_rows, early)
    for copy in copies:
        copy.wait_send()


def local(right_sides, leaf_inverse, project_factors, correct_factors, *couplings):
    rows, cols = right_sides.shape
    blk, depth = leaf_inverse.shape
    levels, _, rank = project_factors.shape
    parts = lax.axis_size("rhs")
    cw = cols // CHUNKS
    whole = lambda dtype: pltpu.VMEM((CHUNKS, rank, cw), dtype)
    any_spec = pl.BlockSpec(memory_space=pltpu.HBM)
    return pl.pallas_call(
        kernel,
        out_shape=jax.ShapeDtypeStruct((rows, cols), BF),
        in_specs=[any_spec] * 7,
        out_specs=pl.BlockSpec(memory_space=pltpu.VMEM),
        scratch_shapes=[
            pltpu.VMEM((depth + levels * rank, cols), BF),
            pltpu.VMEM((rows, depth + levels * rank), BF),
            pltpu.VMEM((rows, levels * rank), BF),
            pltpu.VMEM((levels, rank, rows), BF),
            pltpu.VMEM((levels, parts) + couplings[0].shape[1:], BF),
            pltpu.VMEM((3, rank, 2 * rank), BF),
            pltpu.VMEM((rank, 2 * rank), BF),
            pltpu.VMEM((3, rank, rank), BF),
            pltpu.VMEM((levels, rank, depth // 2), F32),
            pltpu.VMEM((levels, rank, depth // 2), BF),
            pltpu.VMEM((levels, rank, depth // 2), BF),
            pltpu.VMEM((levels, 2, rank, depth // 2), BF),
            whole(F32),
            pltpu.VMEM((CHUNKS, 2 * rank, cw), BF),
            whole(F32), whole(BF), whole(BF),
            pltpu.VMEM((rank, cw), F32), pltpu.VMEM((3, rank, cw), BF), pltpu.VMEM((3, rank, cw), BF),
            pltpu.VMEM((CHUNKS, 2 * rank, cw), BF),
            pltpu.VMEM((2, 2 * rank, cw // 2), BF),
            pltpu.VMEM((rows, cols), F32),
            pltpu.SemaphoreType.DMA((11,)),
            pltpu.SemaphoreType.DMA((1,)),
            pltpu.SemaphoreType.DMA((52,)),
        ],
        compiler_params=pltpu.CompilerParams(
            collective_id=0, has_side_effects=True, vmem_limit_bytes=40 * 1024 * 1024
        ),
    )(*(
        pltpu.with_memory_space_constraint(x, pltpu.HBM)
        for x in (right_sides, leaf_inverse, project_factors, correct_factors, *couplings)
    ))


def solution(mesh):
    in_specs = (
        P("leaf", "rhs"),
        P(("leaf", "rhs"), None),
        P(None, "leaf", None),
        P(None, "leaf", None),
        P(None, "rhs", None),
        P(None, "rhs", None),
        P(None, "rhs", None),
    )
    out_specs = P("leaf", "rhs")
    return jax.shard_map(local, mesh=mesh, in_specs=in_specs, out_specs=out_specs, check_vma=False)
```

```python
import jax
import jax.numpy as jnp
from jax import lax
from jax.experimental import pallas as pl
from jax.experimental.pallas import tpu as pltpu
from jax.sharding import PartitionSpec as P

LEVELS = 3
CHUNKS = 4
PIECES = 4
BF = jnp.bfloat16
F32 = jnp.float32


def mm(a, b):
    return jnp.dot(a, b, preferred_element_type=F32)


def bit_of(index, stride):
    return lax.rem(lax.div(index, stride), 2)


def flip(index, stride):
    return index + stride * (1 - 2 * bit_of(index, stride))


def span(which, size):
    return pl.ds(pl.multiple_of(which * size, size), size)


def kernel(
    b_hbm, a_hbm, p_hbm, c_hbm, w0_hbm, w1_hbm, w2_hbm, out_v,
    b_v, a_v, p_v, pt_v, w_v, g_v, gs_v, h_v, qf, q_s, q_r, q_v,
    pf, st0, p1f, p1_s, p1_r, p2f, p2_s, p2_r, st1, st2, acc,
    lsem, ssem, rsem, msem,
):
    i = lax.axis_index("leaf")
    r = lax.axis_index("rhs")
    blk = a_hbm.shape[0]
    depth = a_hbm.shape[1]
    cols = b_hbm.shape[1]
    rank = p_hbm.shape[2]
    cw = cols // CHUNKS
    hw = cw // 2
    half = depth // 2
    piece = depth // PIECES
    mate = {"rhs": flip(r, 1)}
    across = {"rhs": flip(r, 2)}
    sib = {"leaf": flip(i, 1)}
    near = {"leaf": flip(i, 2)}
    far = {"leaf": flip(i, 4)}
    diag = {"leaf": flip(flip(i, 1), 2)}
    mid = {"leaf": flip(flip(i, 2), 4)}
    sides = [bit_of(i, 1), bit_of(i, 2), bit_of(i, 4)]
    core = bit_of(r, 1)
    chip = bit_of(r, 2)

    copies = []

    def send(src, dst, to):
        copy = pltpu.make_async_remote_copy(
            src_ref=src, dst_ref=dst, send_sem=ssem.at[0], recv_sem=rsem.at[len(copies)],
            device_id=to, device_id_type=pl.DeviceIdType.MESH,
        )
        copy.start()
        copies.append(copy)
        return copy

    def share(ref, to):
        return send(ref, ref, to)

    nloc = [0]

    def fetch(src, dst):
        copy = pltpu.make_async_copy(src, dst, lsem.at[nloc[0]])
        nloc[0] += 1
        copy.start()
        return copy

    mine = [span(s, rank) for s in sides]
    block = span(r, blk)
    pair_rows = span(chip, 2 * blk)
    other_rows = span(1 - chip, 2 * blk)
    half_cols = span(core, half)
    rest_cols = span(1 - core, half)

    la = fetch(a_hbm, a_v.at[block, pl.ds(0, depth)])
    lp = [fetch(p_hbm.at[0], p_v.at[:, pl.ds(0, rank)])]
    lw = [
        fetch(w_hbm.at[lax.div(i, 2 << level)], w_v.at[level, r])
        for level, w_hbm in enumerate((w0_hbm, w1_hbm, w2_hbm))
    ]
    lp += [fetch(p_hbm.at[l], p_v.at[:, pl.ds(l * rank, rank)]) for l in range(1, LEVELS)]
    lc = [fetch(c_hbm.at[l], a_v.at[:, pl.ds(depth + l * rank, rank)]) for l in range(LEVELS)]
    lb = fetch(b_hbm, b_v.at[pl.ds(0, depth)])

    barrier = pltpu.get_barrier_semaphore()
    inner = lax.rem(sides[1] + sides[2], 2)
    for to in (mate, across, sib, near):
        pl.semaphore_signal(barrier, inc=1, device_id=to, device_id_type=pl.DeviceIdType.MESH)

    @pl.when(inner == 1)
    def _():
        pl.semaphore_signal(barrier, inc=1, device_id=mid, device_id_type=pl.DeviceIdType.MESH)

    la.wait()
    pl.semaphore_wait(barrier, 4 + inner)

    @pl.when(inner == 1)
    def _():
        pl.semaphore_signal(msem, inc=1, device_id=mid, device_id_type=pl.DeviceIdType.MESH)


    a_mate = share(a_v.at[block, rest_cols], mate)
    for copy in lw:
        copy.wait()
    w_early = [share(w_v.at[l, r, :, mine[l]], across) for l in range(2)]
    lp[0].wait()
    pt_v[0] = p_v[:, pl.ds(0, rank)].T
    a_mate.wait_recv()
    q_across = []
    for l in range(LEVELS):
        if l > 0:
            lp[l].wait()
            pt_v[l] = p_v[:, pl.ds(l * rank, rank)].T
        part = mm(pt_v[l, :, pair_rows], a_v[pair_rows, half_cols])
        qf[l] = part
        q_s[l] = part.astype(BF)
        q_across.append(send(q_s.at[l], q_r.at[l], across))
    a_mate2 = share(a_v.at[block, half_cols], mate)
    w_mate = share(w_v.at[:, r], mate)
    w_late = [share(w_v.at[l, r, :, span(1 - sides[l], rank)], across) for l in range(2)]
    w_late.append(share(w_v.at[2, r], across))
    a_across = [share(a_v.at[block, pl.ds(k * piece, piece)], across) for k in range(PIECES)]

    for copy in lc:
        copy.wait()
    for n, (l, k) in enumerate(((1, 0), (2, 0), (2, 1))):
        g_v[n, :, mine[0]] = mm(pt_v[l], a_v[:, pl.ds(depth + k * rank, rank)]).astype(BF)
    g_send = share(g_v.at[:, :, mine[0]], sib)

    over = flip(r, 2)
    w_relay = []
    for l in range(2):
        w_early[l].wait_recv()
        w_relay.append(share(w_v.at[l, over, :, mine[l]], mate))
    lb.wait()
    a_mate2.wait_recv()
    for c in range(CHUNKS):
        own = pl.ds(c * cw, cw)
        acc[pair_rows, own] = mm(a_v[pair_rows, pl.ds(0, depth)], b_v[pl.ds(0, depth), own])

    def gather_q(l):
        q_across[l].wait_recv()
        q_v[l, core] = (qf[l] + q_r[l].astype(F32)).astype(BF)
        relayed = share(q_v.at[l, core], mate)
        for c in range(CHUNKS):
            pf[c] = mm(q_v[l, core], b_v[half_cols, pl.ds(c * cw, cw)])
        relayed.wait_recv()

    def project(l, c):
        return pf[c] + mm(q_v[l, 1 - core], b_v[rest_cols, span(c, cw)])

    x0, x1, x2 = {}, {}, {}

    def send0(c):
        x0[c] = share(st0.at[c, mine[0], :], sib)

    def send1(c):
        x1[c] = send(p1_s.at[c], p1_r.at[c], sib)

    gather_q(0)
    for c in range(CHUNKS):
        st0[c, mine[0], :] = project(0, c).astype(BF)
        if c < CHUNKS // 2:
            send0(c)

    w_mate.wait_recv()
    g_send.wait_recv()
    w_relay[0].wait_recv()
    w_cols = w_v[0, :, :, mine[0]].reshape(2 * rank, rank)
    for n in range(2):
        h_v[n] = mm(g_v[n], w_cols).astype(BF)
    pair_sum = g_v[2, :, pl.ds(0, rank)].astype(F32) + g_v[2, :, pl.ds(rank, rank)].astype(F32)
    gs_v[:, mine[1]] = pair_sum.astype(BF)
    gs_send = share(gs_v.at[:, mine[1]], near)

    gather_q(1)
    for c in range(CHUNKS):
        part = project(1, c) - mm(h_v[0], st0[c, mine[0], :])
        p1f[c] = part
        p1_s[c] = part.astype(BF)
        if c < CHUNKS // 2:
            send1(c)

    w_relay[1].wait_recv()
    gs_send.wait_recv()
    h_v[2] = mm(gs_v[...], w_v[1, :, :, mine[1]].reshape(2 * rank, rank)).astype(BF)

    gather_q(2)
    spot = 2 * sides[1] + sides[0]
    spots = (3 - spot, flip(spot, 1), flip(spot, 2), spot)
    team = (diag, sib, near)

    def level_two(n):
        who = spots[n]
        part = project(2, who) - mm(h_v[1], st0[who, mine[0], :]) - mm(h_v[2], p1_s[who])
        if n == 3:
            p2f[...] = part
        else:
            for h in range(2):
                p2_s[n, h] = part[:, h * hw:(h + 1) * hw].astype(BF)

    def send2(n, h):
        x2[n, h] = send(p2_s.at[n, h], p2_r.at[n, h], team[n])

    level_two(0)
    send2(0, 0)
    level_two(1)
    send2(1, 0)
    send2(0, 1)
    send2(1, 1)
    level_two(2)
    send2(2, 0)
    send2(2, 1)
    level_two(3)
    for c in range(CHUNKS // 2, CHUNKS):
        send1(c)
    for c in range(CHUNKS // 2, CHUNKS):
        send0(c)
    for l in range(3):
        w_late[l].wait_recv()
        lanes = span(1 - sides[l], rank) if l < 2 else pl.ds(0, 2 * rank)
        w_relay.append(share(w_v.at[l, over, :, lanes], mate))

    def answer_rows(l):
        return w_v[l, pl.ds(pl.multiple_of(sides[l] * 2, 2), 2), :, :].reshape(rank, 2 * rank)

    z1, f1, n2, relay = {}, {}, {}, {}

    def first(c):
        x0[c].wait_recv()
        b_v[pl.ds(depth, rank), pl.ds(c * cw, cw)] = (-mm(answer_rows(0), st0[c])).astype(BF)

    def second_sum(c):
        x1[c].wait_recv()
        st1[c, mine[1], :] = (p1f[c] + p1_r[c].astype(F32)).astype(BF)
        z1[c] = share(st1.at[c, mine[1], :], near)

    def second(c):
        z1[c].wait_recv()
        b_v[pl.ds(depth + rank, rank), pl.ds(c * cw, cw)] = (-mm(answer_rows(1), st1[c])).astype(BF)

    def third_far(j):
        total = p2f[:, pl.ds(j * hw, hw)]
        for n in range(3):
            x2[n, j].wait_recv()
            total = total + p2_r[n, j].astype(F32)
        st2[j, mine[2], :] = total.astype(BF)
        f1[j] = share(st2.at[j, mine[2], :], far)

    def third(j):
        f1[j].wait_recv()
        where = (pl.ds(depth + 2 * rank, rank), span(2 * spot + j, hw))
        b_v[where] = (-mm(answer_rows(2), st2[j])).astype(BF)
        n2[j] = [share(b_v.at[where], to) for to in team]

    def relay_piece(k):
        a_across[k].wait_recv()
        relay[k] = share(a_v.at[span(over, blk), pl.ds(k * piece, piece)], mate)

    early = depth - piece

    def add_pieces():
        for c in range(CHUNKS):
            own = pl.ds(c * cw, cw)
            acc[other_rows, own] = mm(a_v[other_rows, pl.ds(0, early)], b_v[pl.ds(0, early), own])

    def finish(c, rows, start):
        own = span(c, cw)
        deep = pl.ds(start, depth + LEVELS * rank - start)
        out_v[rows, own] = (acc[rows, own] + mm(a_v[rows, deep], b_v[deep, own])).astype(BF)

    for l in range(2, 5):
        w_relay[l].wait_recv()
    first(0)
    first(1)
    second_sum(0)
    second_sum(1)
    relay_piece(0)

    @pl.when(inner == 1)
    def _():
        pl.semaphore_wait(msem, 1)

    third_far(0)
    third_far(1)
    relay_piece(1)
    second_sum(2)
    second(0)
    second_sum(3)
    second(1)
    third(0)
    third(1)
    relay_piece(2)
    first(2)
    first(3)
    for k in range(3):
        relay[k].wait_recv()
    add_pieces()
    second(2)
    relay_piece(3)
    second(3)
    finish(spot, pair_rows, depth)
    relay[3].wait_recv()
    finish(spot, other_rows, early)
    for n in (2, 1, 0):
        for j in range(2):
            n2[j][n].wait_recv()
        finish(spots[n], pair_rows, depth)
        finish(spots[n], other_rows, early)
    for copy in copies:
        copy.wait_send()


def local(right_sides, leaf_inverse, project_factors, correct_factors, *couplings):
    rows, cols = right_sides.shape
    blk, depth = leaf_inverse.shape
    levels, _, rank = project_factors.shape
    parts = lax.axis_size("rhs")
    cw = cols // CHUNKS
    whole = lambda dtype: pltpu.VMEM((CHUNKS, rank, cw), dtype)
    any_spec = pl.BlockSpec(memory_space=pltpu.HBM)
    return pl.pallas_call(
        kernel,
        out_shape=jax.ShapeDtypeStruct((rows, cols), BF),
        in_specs=[any_spec] * 7,
        out_specs=pl.BlockSpec(memory_space=pltpu.VMEM),
        scratch_shapes=[
            pltpu.VMEM((depth + levels * rank, cols), BF),
            pltpu.VMEM((rows, depth + levels * rank), BF),
            pltpu.VMEM((rows, levels * rank), BF),
            pltpu.VMEM((levels, rank, rows), BF),
            pltpu.VMEM((levels, parts) + couplings[0].shape[1:], BF),
            pltpu.VMEM((3, rank, 2 * rank), BF),
            pltpu.VMEM((rank, 2 * rank), BF),
            pltpu.VMEM((3, rank, rank), BF),
            pltpu.VMEM((levels, rank, depth // 2), F32),
            pltpu.VMEM((levels, rank, depth // 2), BF),
            pltpu.VMEM((levels, rank, depth // 2), BF),
            pltpu.VMEM((levels, 2, rank, depth // 2), BF),
            whole(F32),
            pltpu.VMEM((CHUNKS, 2 * rank, cw), BF),
            whole(F32), whole(BF), whole(BF),
            pltpu.VMEM((rank, cw), F32), pltpu.VMEM((3, 2, rank, cw // 2), BF),
            pltpu.VMEM((3, 2, rank, cw // 2), BF),
            pltpu.VMEM((CHUNKS, 2 * rank, cw), BF),
            pltpu.VMEM((2, 2 * rank, cw // 2), BF),
            pltpu.VMEM((rows, cols), F32),
            pltpu.SemaphoreType.DMA((11,)),
            pltpu.SemaphoreType.DMA((1,)),
            pltpu.SemaphoreType.DMA((55,)),
            pltpu.SemaphoreType.REGULAR,
        ],
        compiler_params=pltpu.CompilerParams(
            collective_id=0, has_side_effects=True, vmem_limit_bytes=40 * 1024 * 1024
        ),
    )(*(
        pltpu.with_memory_space_constraint(x, pltpu.HBM)
        for x in (right_sides, leaf_inverse, project_factors, correct_factors, *couplings)
    ))


def solution(mesh):
    in_specs = (
        P("leaf", "rhs"),
        P(("leaf", "rhs"), None),
        P(None, "leaf", None),
        P(None, "leaf", None),
        P(None, "rhs", None),
        P(None, "rhs", None),
        P(None, "rhs", None),
    )
    out_specs = P("leaf", "rhs")
    return jax.shard_map(local, mesh=mesh, in_specs=in_specs, out_specs=out_specs, check_vma=False)
```

```python
import jax
import jax.numpy as jnp
from jax import lax
from jax.experimental import pallas as pl
from jax.experimental.pallas import tpu as pltpu
from jax.sharding import PartitionSpec as P

LEVELS = 3
CHUNKS = 4
PIECES = 4
BF = jnp.bfloat16
F32 = jnp.float32


def mm(a, b):
    return jnp.dot(a, b, preferred_element_type=F32)


def bit_of(index, stride):
    return lax.rem(lax.div(index, stride), 2)


def flip(index, stride):
    return index + stride * (1 - 2 * bit_of(index, stride))


def span(which, size):
    return pl.ds(pl.multiple_of(which * size, size), size)


def kernel(
    b_hbm, a_hbm, p_hbm, c_hbm, w0_hbm, w1_hbm, w2_hbm, out_v,
    b_v, a_v, p_v, pt_v, w_v, g_v, gs_v, h_v, qf, q_s, q_r, q_v,
    pf, st0, p1f, p1_s, p1_r, p2f, p2_s, p2_r, st1, st2, uf, u_s, u_r, acc,
    lsem, ssem, rsem, msem,
):
    i = lax.axis_index("leaf")
    r = lax.axis_index("rhs")
    blk = a_hbm.shape[0]
    depth = a_hbm.shape[1]
    cols = b_hbm.shape[1]
    rank = p_hbm.shape[2]
    cw = cols // CHUNKS
    hw = cw // 2
    half = depth // 2
    piece = depth // PIECES
    mate = {"rhs": flip(r, 1)}
    across = {"rhs": flip(r, 2)}
    sib = {"leaf": flip(i, 1)}
    near = {"leaf": flip(i, 2)}
    far = {"leaf": flip(i, 4)}
    diag = {"leaf": flip(flip(i, 1), 2)}
    mid = {"leaf": flip(flip(i, 2), 4)}
    sides = [bit_of(i, 1), bit_of(i, 2), bit_of(i, 4)]
    core = bit_of(r, 1)
    chip = bit_of(r, 2)

    copies = []

    def send(src, dst, to):
        copy = pltpu.make_async_remote_copy(
            src_ref=src, dst_ref=dst, send_sem=ssem.at[0], recv_sem=rsem.at[len(copies)],
            device_id=to, device_id_type=pl.DeviceIdType.MESH,
        )
        copy.start()
        copies.append(copy)
        return copy

    def share(ref, to):
        return send(ref, ref, to)

    nloc = [0]

    def fetch(src, dst):
        copy = pltpu.make_async_copy(src, dst, lsem.at[nloc[0]])
        nloc[0] += 1
        copy.start()
        return copy

    mine = [span(s, rank) for s in sides]
    block = span(r, blk)
    pair_rows = span(chip, 2 * blk)
    other_rows = span(1 - chip, 2 * blk)
    half_cols = span(core, half)
    rest_cols = span(1 - core, half)

    la = fetch(a_hbm, a_v.at[block, pl.ds(0, depth)])
    lp = [fetch(p_hbm.at[0], p_v.at[:, pl.ds(0, rank)])]
    lw = [
        fetch(w_hbm.at[lax.div(i, 2 << level)], w_v.at[level, r])
        for level, w_hbm in enumerate((w0_hbm, w1_hbm, w2_hbm))
    ]
    lp += [fetch(p_hbm.at[l], p_v.at[:, pl.ds(l * rank, rank)]) for l in range(1, LEVELS)]
    lc = [fetch(c_hbm.at[l], a_v.at[:, pl.ds(depth + l * rank, rank)]) for l in range(LEVELS)]
    lb = fetch(b_hbm, b_v.at[pl.ds(0, depth)])

    barrier = pltpu.get_barrier_semaphore()
    inner = lax.rem(sides[1] + sides[2], 2)
    for to in (mate, across, sib, near):
        pl.semaphore_signal(barrier, inc=1, device_id=to, device_id_type=pl.DeviceIdType.MESH)

    @pl.when(inner == 1)
    def _():
        pl.semaphore_signal(barrier, inc=1, device_id=mid, device_id_type=pl.DeviceIdType.MESH)

    la.wait()
    pl.semaphore_wait(barrier, 4 + inner)

    @pl.when(inner == 1)
    def _():
        pl.semaphore_signal(msem, inc=1, device_id=mid, device_id_type=pl.DeviceIdType.MESH)


    a_mate = share(a_v.at[block, rest_cols], mate)
    for copy in lw:
        copy.wait()
    w_early = [share(w_v.at[l, r, :, mine[l]], across) for l in range(2)]
    lp[0].wait()
    pt_v[0] = p_v[:, pl.ds(0, rank)].T
    a_mate.wait_recv()
    q_across = []
    for l in range(LEVELS):
        if l > 0:
            lp[l].wait()
            pt_v[l] = p_v[:, pl.ds(l * rank, rank)].T
        part = mm(pt_v[l, :, pair_rows], a_v[pair_rows, half_cols])
        qf[l] = part
        q_s[l] = part.astype(BF)
        q_across.append(send(q_s.at[l], q_r.at[l], across))
    a_mate2 = share(a_v.at[block, half_cols], mate)
    w_mate = share(w_v.at[:, r], mate)
    w_late = [share(w_v.at[l, r, :, span(1 - sides[l], rank)], across) for l in range(2)]
    w_late.append(share(w_v.at[2, r], across))
    a_across = [share(a_v.at[block, pl.ds(k * piece, piece)], across) for k in range(PIECES)]

    for copy in lc:
        copy.wait()
    for n, (l, k) in enumerate(((1, 0), (2, 0), (2, 1))):
        g_v[n, :, mine[0]] = mm(pt_v[l], a_v[:, pl.ds(depth + k * rank, rank)]).astype(BF)
    g_send = share(g_v.at[:, :, mine[0]], sib)

    over = flip(r, 2)
    w_relay = []
    for l in range(2):
        w_early[l].wait_recv()
        w_relay.append(share(w_v.at[l, over, :, mine[l]], mate))
    lb.wait()
    a_mate2.wait_recv()
    for c in range(CHUNKS):
        own = pl.ds(c * cw, cw)
        acc[pair_rows, own] = mm(a_v[pair_rows, pl.ds(0, depth)], b_v[pl.ds(0, depth), own])

    def gather_q(l):
        q_across[l].wait_recv()
        q_v[l, core] = (qf[l] + q_r[l].astype(F32)).astype(BF)
        relayed = share(q_v.at[l, core], mate)
        for c in range(CHUNKS):
            pf[c] = mm(q_v[l, core], b_v[half_cols, pl.ds(c * cw, cw)])
        relayed.wait_recv()

    def project(l, c):
        return pf[c] + mm(q_v[l, 1 - core], b_v[rest_cols, span(c, cw)])

    x0, x1, x2, z1, f1, n2, u1, relay = {}, {}, {}, {}, {}, {}, {}, {}

    def send0(c):
        x0[c] = share(st0.at[c, mine[0], :], sib)

    def send1(c):
        x1[c] = send(p1_s.at[c], p1_r.at[c], sib)

    gather_q(0)
    for c in range(CHUNKS):
        st0[c, mine[0], :] = project(0, c).astype(BF)
        send0(c)

    w_mate.wait_recv()
    g_send.wait_recv()
    w_relay[0].wait_recv()
    w_cols = w_v[0, :, :, mine[0]].reshape(2 * rank, rank)
    for n in range(2):
        h_v[n] = mm(g_v[n], w_cols).astype(BF)
    pair_sum = g_v[2, :, pl.ds(0, rank)].astype(F32) + g_v[2, :, pl.ds(rank, rank)].astype(F32)
    gs_v[:, mine[1]] = pair_sum.astype(BF)
    gs_send = share(gs_v.at[:, mine[1]], near)

    gather_q(1)
    for c in range(CHUNKS):
        part = project(1, c) - mm(h_v[0], st0[c, mine[0], :])
        p1f[c] = part
        p1_s[c] = part.astype(BF)
        if c < CHUNKS // 2:
            st1[c, mine[1], :] = part.astype(BF)
            z1[c] = send(p1_s.at[c], st1.at[c, mine[1], :], near)

    w_relay[1].wait_recv()
    gs_send.wait_recv()
    h_v[2] = mm(gs_v[...], w_v[1, :, :, mine[1]].reshape(2 * rank, rank)).astype(BF)

    gather_q(2)
    spot = 2 * sides[1] + sides[0]
    spots = (3 - spot, flip(spot, 1), flip(spot, 2), spot)
    team = (diag, sib, near)

    def level_two(n):
        who = spots[n]
        part = project(2, who) - mm(h_v[1], st0[who, mine[0], :]) - mm(h_v[2], p1_s[who])
        if n == 3:
            p2f[...] = part
        else:
            for h in range(2):
                p2_s[n, h] = part[:, h * hw:(h + 1) * hw].astype(BF)

    def send2(n, h):
        x2[n, h] = send(p2_s.at[n, h], p2_r.at[n, h], team[n])

    level_two(0)
    send2(0, 0)
    level_two(1)
    send2(1, 0)
    send2(0, 1)
    send2(1, 1)
    level_two(2)
    send2(2, 0)
    send2(2, 1)
    level_two(3)
    for c in range(CHUNKS // 2, CHUNKS):
        send1(c)
    for l in range(3):
        w_late[l].wait_recv()
        lanes = span(1 - sides[l], rank) if l < 2 else pl.ds(0, 2 * rank)
        w_relay.append(share(w_v.at[l, over, :, lanes], mate))

    def answer_rows(l):
        return w_v[l, pl.ds(pl.multiple_of(sides[l] * 2, 2), 2), :, :].reshape(rank, 2 * rank)


    def first(c):
        x0[c].wait_recv()
        b_v[pl.ds(depth, rank), pl.ds(c * cw, cw)] = (-mm(answer_rows(0), st0[c])).astype(BF)

    def second_sum(c):
        x1[c].wait_recv()
        st1[c, mine[1], :] = (p1f[c] + p1_r[c].astype(F32)).astype(BF)
        z1[c] = share(st1.at[c, mine[1], :], near)

    def second(c):
        z1[c].wait_recv()
        b_v[pl.ds(depth + rank, rank), pl.ds(c * cw, cw)] = (-mm(answer_rows(1), st1[c])).astype(BF)

    def second_part(c):
        z1[c].wait_recv()
        part = mm(answer_rows(1), st1[c])
        uf[c] = part
        u_s[c] = part.astype(BF)
        u1[c] = send(u_s.at[c], u_r.at[c], sib)

    def second_join(c):
        u1[c].wait_recv()
        b_v[pl.ds(depth + rank, rank), pl.ds(c * cw, cw)] = (-(uf[c] + u_r[c].astype(F32))).astype(BF)

    def third_far(j):
        total = p2f[:, pl.ds(j * hw, hw)]
        for n in range(3):
            x2[n, j].wait_recv()
            total = total + p2_r[n, j].astype(F32)
        st2[j, mine[2], :] = total.astype(BF)
        f1[j] = share(st2.at[j, mine[2], :], far)

    def third(j):
        f1[j].wait_recv()
        where = (pl.ds(depth + 2 * rank, rank), span(2 * spot + j, hw))
        b_v[where] = (-mm(answer_rows(2), st2[j])).astype(BF)
        n2[j] = [share(b_v.at[where], to) for to in team]

    def relay_piece(k):
        a_across[k].wait_recv()
        relay[k] = share(a_v.at[span(over, blk), pl.ds(k * piece, piece)], mate)

    early = depth - piece

    def add_pieces():
        for c in range(CHUNKS):
            own = pl.ds(c * cw, cw)
            acc[other_rows, own] = mm(a_v[other_rows, pl.ds(0, early)], b_v[pl.ds(0, early), own])

    def add_last():
        deep = pl.ds(early, piece)
        for c in range(CHUNKS):
            own = pl.ds(c * cw, cw)
            acc[other_rows, own] = acc[other_rows, own] + mm(a_v[other_rows, deep], b_v[deep, own])

    def finish(c):
        own = span(c, cw)
        deep = pl.ds(depth, LEVELS * rank)
        out_v[:, own] = (acc[:, own] + mm(a_v[:, deep], b_v[deep, own])).astype(BF)

    for l in range(2, 5):
        w_relay[l].wait_recv()
    first(0)
    first(1)
    second_part(0)
    second_part(1)
    relay_piece(0)

    @pl.when(inner == 1)
    def _():
        pl.semaphore_wait(msem, 1)

    third_far(0)
    third_far(1)
    relay_piece(1)
    first(2)
    first(3)
    second_sum(2)
    second_sum(3)
    relay_piece(2)
    third(0)
    third(1)
    second_join(0)
    second_join(1)
    relay_piece(3)
    for k in range(3):
        relay[k].wait_recv()
    add_pieces()
    second(2)
    second(3)
    relay[3].wait_recv()
    add_last()
    finish(spot)
    for n in (2, 1, 0):
        for j in range(2):
            n2[j][n].wait_recv()
    for n in range(3):
        finish(spots[n])
    for copy in copies:
        copy.wait_send()


def local(right_sides, leaf_inverse, project_factors, correct_factors, *couplings):
    rows, cols = right_sides.shape
    blk, depth = leaf_inverse.shape
    levels, _, rank = project_factors.shape
    parts = lax.axis_size("rhs")
    cw = cols // CHUNKS
    whole = lambda dtype: pltpu.VMEM((CHUNKS, rank, cw), dtype)
    any_spec = pl.BlockSpec(memory_space=pltpu.HBM)
    return pl.pallas_call(
        kernel,
        out_shape=jax.ShapeDtypeStruct((rows, cols), BF),
        in_specs=[any_spec] * 7,
        out_specs=pl.BlockSpec(memory_space=pltpu.VMEM),
        scratch_shapes=[
            pltpu.VMEM((depth + levels * rank, cols), BF),
            pltpu.VMEM((rows, depth + levels * rank), BF),
            pltpu.VMEM((rows, levels * rank), BF),
            pltpu.VMEM((levels, rank, rows), BF),
            pltpu.VMEM((levels, parts) + couplings[0].shape[1:], BF),
            pltpu.VMEM((3, rank, 2 * rank), BF),
            pltpu.VMEM((rank, 2 * rank), BF),
            pltpu.VMEM((3, rank, rank), BF),
            pltpu.VMEM((levels, rank, depth // 2), F32),
            pltpu.VMEM((levels, rank, depth // 2), BF),
            pltpu.VMEM((levels, rank, depth // 2), BF),
            pltpu.VMEM((levels, 2, rank, depth // 2), BF),
            whole(F32),
            pltpu.VMEM((CHUNKS, 2 * rank, cw), BF),
            whole(F32), whole(BF), whole(BF),
            pltpu.VMEM((rank, cw), F32), pltpu.VMEM((3, 2, rank, cw // 2), BF),
            pltpu.VMEM((3, 2, rank, cw // 2), BF),
            pltpu.VMEM((CHUNKS, 2 * rank, cw), BF),
            pltpu.VMEM((2, 2 * rank, cw // 2), BF),
            pltpu.VMEM((2, rank, cw), F32),
            pltpu.VMEM((2, rank, cw), BF),
            pltpu.VMEM((2, rank, cw), BF),
            pltpu.VMEM((rows, cols), F32),
            pltpu.SemaphoreType.DMA((11,)),
            pltpu.SemaphoreType.DMA((1,)),
            pltpu.SemaphoreType.DMA((55,)),
            pltpu.SemaphoreType.REGULAR,
        ],
        compiler_params=pltpu.CompilerParams(
            collective_id=0, has_side_effects=True, vmem_limit_bytes=40 * 1024 * 1024
        ),
    )(*(
        pltpu.with_memory_space_constraint(x, pltpu.HBM)
        for x in (right_sides, leaf_inverse, project_factors, correct_factors, *couplings)
    ))


def solution(mesh):
    in_specs = (
        P("leaf", "rhs"),
        P(("leaf", "rhs"), None),
        P(None, "leaf", None),
        P(None, "leaf", None),
        P(None, "rhs", None),
        P(None, "rhs", None),
        P(None, "rhs", None),
    )
    out_specs = P("leaf", "rhs")
    return jax.shard_map(local, mesh=mesh, in_specs=in_specs, out_specs=out_specs, check_vma=False)
```

```python
import jax
import jax.numpy as jnp
from jax import lax
from jax.experimental import pallas as pl
from jax.experimental.pallas import tpu as pltpu
from jax.sharding import PartitionSpec as P

LEVELS = 3
CHUNKS = 4
PIECES = 4
RECVS = 36
FETCHES = 7
BF = jnp.bfloat16
F32 = jnp.float32


def mm(a, b):
    return jnp.dot(a, b, preferred_element_type=F32)


def bit_of(index, stride):
    return lax.rem(lax.div(index, stride), 2)


def flip(index, stride):
    return index + stride * (1 - 2 * bit_of(index, stride))


def span(which, size):
    return pl.ds(pl.multiple_of(which * size, size), size)


def kernel(
    b_hbm, a_hbm, p_hbm, c_hbm, w0_hbm, w1_hbm, w2_hbm, out_v,
    b_v, a_v, p_v, pt_v, w_v, g_v, gs_v, h_v, qf, q_s, q_r, q_v,
    pf, st0, p1f, p1_s, p1_r, p2f, p2_s, p2_r, st1, st2, uf, u_s, u_r, acc,
    lsem, ssem, rsem, msem,
):
    i = lax.axis_index("leaf")
    r = lax.axis_index("rhs")
    blk = a_hbm.shape[0]
    depth = a_hbm.shape[1]
    cols = b_hbm.shape[1]
    rank = p_hbm.shape[2]
    cw = cols // CHUNKS
    hw = cw // 2
    half = depth // 2
    piece = depth // PIECES
    mate = {"rhs": flip(r, 1)}
    across = {"rhs": flip(r, 2)}
    sib = {"leaf": flip(i, 1)}
    near = {"leaf": flip(i, 2)}
    far = {"leaf": flip(i, 4)}
    diag = {"leaf": flip(flip(i, 1), 2)}
    mid = {"leaf": flip(flip(i, 2), 4)}
    sides = [bit_of(i, 1), bit_of(i, 2), bit_of(i, 4)]
    core = bit_of(r, 1)
    chip = bit_of(r, 2)

    copies = []
    slots = {}

    def slot(key):
        return slots.setdefault(key, len(slots))

    def send(src, dst, to, key):
        copy = pltpu.make_async_remote_copy(
            src_ref=src, dst_ref=dst, send_sem=ssem.at[0], recv_sem=rsem.at[slot(key)],
            device_id=to, device_id_type=pl.DeviceIdType.MESH,
        )
        copy.start()
        copies.append(copy)
        return copy

    def arrive(key, ref):
        pltpu.make_async_copy(ref, ref, rsem.at[slot(key)]).wait()

    def fetched(key, ref):
        pltpu.make_async_copy(ref, ref, lsem.at[places[key]]).wait()

    def share(ref, to, key):
        return send(ref, ref, to, key)

    places = {}

    def fetch(src, dst, key):
        copy = pltpu.make_async_copy(src, dst, lsem.at[places.setdefault(key, len(places))])
        copy.start()
        return copy

    mine = [span(s, rank) for s in sides]
    block = span(r, blk)
    pair_rows = span(chip, 2 * blk)
    other_rows = span(1 - chip, 2 * blk)
    half_cols = span(core, half)
    rest_cols = span(1 - core, half)

    la = fetch(a_hbm, a_v.at[block, pl.ds(0, depth)], "a")
    lp = [fetch(p_hbm.at[0], p_v.at[:, pl.ds(0, rank)], "p0")]
    [
        fetch(w_hbm.at[lax.div(i, 2 << level)], w_v.at[level, r], "w")
        for level, w_hbm in enumerate((w0_hbm, w1_hbm, w2_hbm))
    ]
    lp += [fetch(p_hbm.at[l], p_v.at[:, pl.ds(l * rank, rank)], f"p{l}") for l in range(1, LEVELS)]
    [fetch(c_hbm.at[l], a_v.at[:, pl.ds(depth + l * rank, rank)], "c") for l in range(LEVELS)]
    lb = fetch(b_hbm, b_v.at[pl.ds(0, depth)], "b")

    barrier = pltpu.get_barrier_semaphore()
    inner = lax.rem(sides[1] + sides[2], 2)
    for to in (mate, across, sib, near):
        pl.semaphore_signal(barrier, inc=1, device_id=to, device_id_type=pl.DeviceIdType.MESH)

    @pl.when(inner == 1)
    def _():
        pl.semaphore_signal(barrier, inc=1, device_id=mid, device_id_type=pl.DeviceIdType.MESH)

    la.wait()
    pl.semaphore_wait(barrier, 4 + inner)

    @pl.when(inner == 1)
    def _():
        pl.semaphore_signal(msem, inc=1, device_id=mid, device_id_type=pl.DeviceIdType.MESH)


    a_mate = share(a_v.at[block, rest_cols], mate, "am")
    fetched("w", w_v.at[:, r])
    [share(w_v.at[l, r, :, mine[l]], across, "we") for l in range(2)]
    lp[0].wait()
    pt_v[0] = p_v[:, pl.ds(0, rank)].T
    a_mate.wait_recv()
    q_across = []
    for l in range(LEVELS):
        if l > 0:
            lp[l].wait()
            pt_v[l] = p_v[:, pl.ds(l * rank, rank)].T
        part = mm(pt_v[l, :, pair_rows], a_v[pair_rows, half_cols])
        qf[l] = part
        q_s[l] = part.astype(BF)
        q_across.append(send(q_s.at[l], q_r.at[l], across, f"q{l}"))
    a_mate2 = share(a_v.at[block, half_cols], mate, "an")
    w_mate = share(w_v.at[:, r], mate, "wm")
    [share(w_v.at[l, r, :, span(1 - sides[l], rank)], across, "wl") for l in range(2)]
    share(w_v.at[2, r], across, "wl")
    a_across = [share(a_v.at[block, pl.ds(k * piece, piece)], across, f"a{k}") for k in range(PIECES)]

    fetched("c", a_v.at[:, pl.ds(depth, LEVELS * rank)])
    for n, (l, k) in enumerate(((1, 0), (2, 0), (2, 1))):
        g_v[n, :, mine[0]] = mm(pt_v[l], a_v[:, pl.ds(depth + k * rank, rank)]).astype(BF)
    g_send = share(g_v.at[:, :, mine[0]], sib, "g")

    over = flip(r, 2)
    arrive("we", w_v.at[0, r])
    for l in range(2):
        share(w_v.at[l, over, :, mine[l]], mate, "re")
    lb.wait()
    a_mate2.wait_recv()
    for c in range(CHUNKS):
        own = pl.ds(c * cw, cw)
        acc[pair_rows, own] = mm(a_v[pair_rows, pl.ds(0, depth)], b_v[pl.ds(0, depth), own])

    def gather_q(l):
        q_across[l].wait_recv()
        q_v[l, core] = (qf[l] + q_r[l].astype(F32)).astype(BF)
        relayed = share(q_v.at[l, core], mate, f"m{l}")
        for c in range(CHUNKS):
            pf[c] = mm(q_v[l, core], b_v[half_cols, pl.ds(c * cw, cw)])
        relayed.wait_recv()

    def project(l, c):
        return pf[c] + mm(q_v[l, 1 - core], b_v[rest_cols, span(c, cw)])

    x1, z1, f1, u1, relay = {}, {}, {}, {}, {}

    def send0(c):
        share(st0.at[c, mine[0], :], sib, f"x{c // 2}")

    def send1(c):
        x1[c] = send(p1_s.at[c], p1_r.at[c], sib, f"y{c}")

    gather_q(0)
    for c in range(CHUNKS):
        st0[c, mine[0], :] = project(0, c).astype(BF)
        send0(c)

    w_mate.wait_recv()
    g_send.wait_recv()
    arrive("re", w_v.at[0, r])
    w_cols = w_v[0, :, :, mine[0]].reshape(2 * rank, rank)
    for n in range(2):
        h_v[n] = mm(g_v[n], w_cols).astype(BF)
    pair_sum = g_v[2, :, pl.ds(0, rank)].astype(F32) + g_v[2, :, pl.ds(rank, rank)].astype(F32)
    gs_v[:, mine[1]] = pair_sum.astype(BF)
    gs_send = share(gs_v.at[:, mine[1]], near, "gs")

    gather_q(1)
    for c in range(CHUNKS):
        part = project(1, c) - mm(h_v[0], st0[c, mine[0], :])
        p1f[c] = part
        p1_s[c] = part.astype(BF)
        if c < CHUNKS // 2:
            st1[c, mine[1], :] = part.astype(BF)
            z1[c] = send(p1_s.at[c], st1.at[c, mine[1], :], near, f"z{c}")

    gs_send.wait_recv()
    h_v[2] = mm(gs_v[...], w_v[1, :, :, mine[1]].reshape(2 * rank, rank)).astype(BF)

    gather_q(2)
    spot = 2 * sides[1] + sides[0]
    spots = (3 - spot, flip(spot, 1), flip(spot, 2), spot)
    team = (diag, sib, near)

    def level_two(n):
        who = spots[n]
        part = project(2, who) - mm(h_v[1], st0[who, mine[0], :]) - mm(h_v[2], p1_s[who])
        if n == 3:
            p2f[...] = part
        else:
            for h in range(2):
                p2_s[h, n] = part[:, h * hw:(h + 1) * hw].astype(BF)

    def send2(n, h):
        send(p2_s.at[h, n], p2_r.at[h, n], team[n], f"t{h}")

    level_two(0)
    send2(0, 0)
    level_two(1)
    send2(1, 0)
    send2(0, 1)
    send2(1, 1)
    level_two(2)
    send2(2, 0)
    send2(2, 1)
    level_two(3)
    for c in range(CHUNKS // 2, CHUNKS):
        send1(c)
    arrive("wl", w_v.at[pl.ds(0, 2), r])
    for l in range(3):
        lanes = span(1 - sides[l], rank) if l < 2 else pl.ds(0, 2 * rank)
        share(w_v.at[l, over, :, lanes], mate, "rl")

    def answer_rows(l):
        return w_v[l, pl.ds(pl.multiple_of(sides[l] * 2, 2), 2), :, :].reshape(rank, 2 * rank)


    def first(pair):
        arrive(f"x{pair[0] // 2}", st0.at[pl.ds(pair[0], 2), mine[0], :])
        for c in pair:
            b_v[pl.ds(depth, rank), pl.ds(c * cw, cw)] = (-mm(answer_rows(0), st0[c])).astype(BF)

    def second_sum(c):
        x1[c].wait_recv()
        st1[c, mine[1], :] = (p1f[c] + p1_r[c].astype(F32)).astype(BF)
        z1[c] = share(st1.at[c, mine[1], :], near, f"z{c}")

    def second(c):
        z1[c].wait_recv()
        b_v[pl.ds(depth + rank, rank), pl.ds(c * cw, cw)] = (-mm(answer_rows(1), st1[c])).astype(BF)

    def second_part(c):
        z1[c].wait_recv()
        part = mm(answer_rows(1), st1[c])
        uf[c] = part
        u_s[c] = part.astype(BF)
        u1[c] = send(u_s.at[c], u_r.at[c], sib, f"u{c}")

    def second_join(c):
        u1[c].wait_recv()
        b_v[pl.ds(depth + rank, rank), pl.ds(c * cw, cw)] = (-(uf[c] + u_r[c].astype(F32))).astype(BF)

    def third_far(j):
        total = p2f[:, pl.ds(j * hw, hw)]
        arrive(f"t{j}", p2_r.at[j])
        for n in range(3):
            total = total + p2_r[j, n].astype(F32)
        st2[j, mine[2], :] = total.astype(BF)
        f1[j] = share(st2.at[j, mine[2], :], far, f"f{j}")

    def third(j):
        f1[j].wait_recv()
        where = (pl.ds(depth + 2 * rank, rank), span(2 * spot + j, hw))
        b_v[where] = (-mm(answer_rows(2), st2[j])).astype(BF)
        for to in team:
            share(b_v.at[where], to, "n")

    def relay_piece(k):
        a_across[k].wait_recv()
        relay[k] = share(a_v.at[span(over, blk), pl.ds(k * piece, piece)], mate, "r3" if k == PIECES - 1 else "r")

    early = depth - piece

    def add_pieces():
        for c in range(CHUNKS):
            own = pl.ds(c * cw, cw)
            acc[other_rows, own] = mm(a_v[other_rows, pl.ds(0, early)], b_v[pl.ds(0, early), own])

    def add_last():
        deep = pl.ds(early, piece)
        for c in range(CHUNKS):
            own = pl.ds(c * cw, cw)
            acc[other_rows, own] = acc[other_rows, own] + mm(a_v[other_rows, deep], b_v[deep, own])

    def finish(c):
        own = pl.ds(c * cw, cw)
        deep = pl.ds(depth, LEVELS * rank)
        out_v[:, own] = (acc[:, own] + mm(a_v[:, deep], b_v[deep, own])).astype(BF)

    arrive("rl", w_v.at[pl.ds(0, 2), r])
    first((0, 1))
    second_part(0)
    second_part(1)
    relay_piece(0)

    @pl.when(inner == 1)
    def _():
        pl.semaphore_wait(msem, 1)

    third_far(0)
    third_far(1)
    relay_piece(1)
    first((2, 3))
    second_sum(2)
    second_sum(3)
    relay_piece(2)
    third(0)
    third(1)
    second_join(0)
    second_join(1)
    relay_piece(3)
    arrive("r", a_v.at[block, pl.ds(0, early)])
    add_pieces()
    second(2)
    second(3)
    relay[3].wait_recv()
    add_last()
    arrive("n", b_v.at[pl.ds(depth + 2 * rank, rank), pl.ds(0, (CHUNKS - 1) * cw)])
    for c in range(CHUNKS):
        finish(c)
    assert len(slots) == RECVS and len(places) == FETCHES, (len(slots), len(places))
    for copy in copies:
        copy.wait_send()


def local(right_sides, leaf_inverse, project_factors, correct_factors, *couplings):
    rows, cols = right_sides.shape
    blk, depth = leaf_inverse.shape
    levels, _, rank = project_factors.shape
    parts = lax.axis_size("rhs")
    cw = cols // CHUNKS
    whole = lambda dtype: pltpu.VMEM((CHUNKS, rank, cw), dtype)
    any_spec = pl.BlockSpec(memory_space=pltpu.HBM)
    return pl.pallas_call(
        kernel,
        out_shape=jax.ShapeDtypeStruct((rows, cols), BF),
        in_specs=[any_spec] * 7,
        out_specs=pl.BlockSpec(memory_space=pltpu.VMEM),
        scratch_shapes=[
            pltpu.VMEM((depth + levels * rank, cols), BF),
            pltpu.VMEM((rows, depth + levels * rank), BF),
            pltpu.VMEM((rows, levels * rank), BF),
            pltpu.VMEM((levels, rank, rows), BF),
            pltpu.VMEM((levels, parts) + couplings[0].shape[1:], BF),
            pltpu.VMEM((3, rank, 2 * rank), BF),
            pltpu.VMEM((rank, 2 * rank), BF),
            pltpu.VMEM((3, rank, rank), BF),
            pltpu.VMEM((levels, rank, depth // 2), F32),
            pltpu.VMEM((levels, rank, depth // 2), BF),
            pltpu.VMEM((levels, rank, depth // 2), BF),
            pltpu.VMEM((levels, 2, rank, depth // 2), BF),
            whole(F32),
            pltpu.VMEM((CHUNKS, 2 * rank, cw), BF),
            whole(F32), whole(BF), whole(BF),
            pltpu.VMEM((rank, cw), F32), pltpu.VMEM((2, 3, rank, cw // 2), BF),
            pltpu.VMEM((2, 3, rank, cw // 2), BF),
            pltpu.VMEM((CHUNKS, 2 * rank, cw), BF),
            pltpu.VMEM((2, 2 * rank, cw // 2), BF),
            pltpu.VMEM((2, rank, cw), F32),
            pltpu.VMEM((2, rank, cw), BF),
            pltpu.VMEM((2, rank, cw), BF),
            pltpu.VMEM((rows, cols), F32),
            pltpu.SemaphoreType.DMA((FETCHES,)),
            pltpu.SemaphoreType.DMA((1,)),
            pltpu.SemaphoreType.DMA((RECVS,)),
            pltpu.SemaphoreType.REGULAR,
        ],
        compiler_params=pltpu.CompilerParams(
            collective_id=0, has_side_effects=True, vmem_limit_bytes=40 * 1024 * 1024
        ),
    )(*(
        pltpu.with_memory_space_constraint(x, pltpu.HBM)
        for x in (right_sides, leaf_inverse, project_factors, correct_factors, *couplings)
    ))


def solution(mesh):
    in_specs = (
        P("leaf", "rhs"),
        P(("leaf", "rhs"), None),
        P(None, "leaf", None),
        P(None, "leaf", None),
        P(None, "rhs", None),
        P(None, "rhs", None),
        P(None, "rhs", None),
    )
    out_specs = P("leaf", "rhs")
    return jax.shard_map(local, mesh=mesh, in_specs=in_specs, out_specs=out_specs, check_vma=False)
```

```python
import jax
import jax.numpy as jnp
from jax import lax
from jax.experimental import pallas as pl
from jax.experimental.pallas import tpu as pltpu
from jax.sharding import PartitionSpec as P

LEVELS = 3
CHUNKS = 4
PIECES = 4
ZFIRST = 3
RECVS = 36
FETCHES = 7
BF = jnp.bfloat16
F32 = jnp.float32


def mm(a, b):
    return jnp.dot(a, b, preferred_element_type=F32)


def bit_of(index, stride):
    return lax.rem(lax.div(index, stride), 2)


def flip(index, stride):
    return index + stride * (1 - 2 * bit_of(index, stride))


def span(which, size):
    return pl.ds(pl.multiple_of(which * size, size), size)


def kernel(
    b_hbm, a_hbm, p_hbm, c_hbm, w0_hbm, w1_hbm, w2_hbm, out_v,
    b_v, a_v, p_v, pt_v, w_v, g_v, gs_v, h_v, qf, q_s, q_r, q_v,
    pf, st0, p1f, p1_s, p1_r, p2f, p2_s, p2_r, st1, st2, uf, u_s, u_r, acc,
    lsem, ssem, rsem, msem,
):
    i = lax.axis_index("leaf")
    r = lax.axis_index("rhs")
    blk = a_hbm.shape[0]
    depth = a_hbm.shape[1]
    cols = b_hbm.shape[1]
    rank = p_hbm.shape[2]
    cw = cols // CHUNKS
    hw = cw // 2
    half = depth // 2
    piece = depth // PIECES
    mate = {"rhs": flip(r, 1)}
    across = {"rhs": flip(r, 2)}
    sib = {"leaf": flip(i, 1)}
    near = {"leaf": flip(i, 2)}
    far = {"leaf": flip(i, 4)}
    diag = {"leaf": flip(flip(i, 1), 2)}
    mid = {"leaf": flip(flip(i, 2), 4)}
    sides = [bit_of(i, 1), bit_of(i, 2), bit_of(i, 4)]
    core = bit_of(r, 1)
    chip = bit_of(r, 2)

    copies = []
    slots = {}

    def slot(key):
        return slots.setdefault(key, len(slots))

    def send(src, dst, to, key):
        copy = pltpu.make_async_remote_copy(
            src_ref=src, dst_ref=dst, send_sem=ssem.at[0], recv_sem=rsem.at[slot(key)],
            device_id=to, device_id_type=pl.DeviceIdType.MESH,
        )
        copy.start()
        copies.append(copy)
        return copy

    def arrive(key, ref):
        pltpu.make_async_copy(ref, ref, rsem.at[slot(key)]).wait()

    def fetched(key, ref):
        pltpu.make_async_copy(ref, ref, lsem.at[places[key]]).wait()

    def share(ref, to, key):
        return send(ref, ref, to, key)

    places = {}

    def fetch(src, dst, key):
        copy = pltpu.make_async_copy(src, dst, lsem.at[places.setdefault(key, len(places))])
        copy.start()
        return copy

    mine = [span(s, rank) for s in sides]
    block = span(r, blk)
    pair_rows = span(chip, 2 * blk)
    other_rows = span(1 - chip, 2 * blk)
    half_cols = span(core, half)
    rest_cols = span(1 - core, half)

    la = fetch(a_hbm, a_v.at[block, pl.ds(0, depth)], "a")
    lp = [fetch(p_hbm.at[0], p_v.at[:, pl.ds(0, rank)], "p0")]
    [
        fetch(w_hbm.at[lax.div(i, 2 << level)], w_v.at[level, r], "w")
        for level, w_hbm in enumerate((w0_hbm, w1_hbm, w2_hbm))
    ]
    lp += [fetch(p_hbm.at[l], p_v.at[:, pl.ds(l * rank, rank)], f"p{l}") for l in range(1, LEVELS)]
    [fetch(c_hbm.at[l], a_v.at[:, pl.ds(depth + l * rank, rank)], "c") for l in range(LEVELS)]
    lb = fetch(b_hbm, b_v.at[pl.ds(0, depth)], "b")

    barrier = pltpu.get_barrier_semaphore()
    inner = lax.rem(sides[1] + sides[2], 2)
    for to in (mate, across, sib, near):
        pl.semaphore_signal(barrier, inc=1, device_id=to, device_id_type=pl.DeviceIdType.MESH)

    @pl.when(inner == 1)
    def _():
        pl.semaphore_signal(barrier, inc=1, device_id=mid, device_id_type=pl.DeviceIdType.MESH)

    la.wait()
    pl.semaphore_wait(barrier, 4 + inner)

    @pl.when(inner == 1)
    def _():
        pl.semaphore_signal(msem, inc=1, device_id=mid, device_id_type=pl.DeviceIdType.MESH)


    a_mate = share(a_v.at[block, rest_cols], mate, "am")
    fetched("w", w_v.at[:, r])
    [share(w_v.at[l, r, :, mine[l]], across, "we") for l in range(2)]
    lp[0].wait()
    pt_v[0] = p_v[:, pl.ds(0, rank)].T
    a_mate.wait_recv()
    q_across = []
    for l in range(LEVELS):
        if l > 0:
            lp[l].wait()
            pt_v[l] = p_v[:, pl.ds(l * rank, rank)].T
        part = mm(pt_v[l, :, pair_rows], a_v[pair_rows, half_cols])
        qf[l] = part
        q_s[l] = part.astype(BF)
        q_across.append(send(q_s.at[l], q_r.at[l], across, f"q{l}"))
    a_mate2 = share(a_v.at[block, half_cols], mate, "an")
    w_mate = share(w_v.at[:, r], mate, "wm")
    [share(w_v.at[l, r, :, span(1 - sides[l], rank)], across, "wl") for l in range(2)]
    share(w_v.at[2, r], across, "wl")
    a_across = [share(a_v.at[block, pl.ds(k * piece, piece)], across, f"a{k}") for k in range(PIECES)]

    fetched("c", a_v.at[:, pl.ds(depth, LEVELS * rank)])
    for n, (l, k) in enumerate(((1, 0), (2, 0), (2, 1))):
        g_v[n, :, mine[0]] = mm(pt_v[l], a_v[:, pl.ds(depth + k * rank, rank)]).astype(BF)
    g_send = share(g_v.at[:, :, mine[0]], sib, "g")

    over = flip(r, 2)
    arrive("we", w_v.at[0, r])
    for l in range(2):
        share(w_v.at[l, over, :, mine[l]], mate, "re")
    lb.wait()
    a_mate2.wait_recv()
    for c in range(CHUNKS):
        own = pl.ds(c * cw, cw)
        acc[pair_rows, own] = mm(a_v[pair_rows, pl.ds(0, depth)], b_v[pl.ds(0, depth), own])

    def gather_q(l):
        q_across[l].wait_recv()
        q_v[l, core] = (qf[l] + q_r[l].astype(F32)).astype(BF)
        relayed = share(q_v.at[l, core], mate, f"m{l}")
        for c in range(CHUNKS):
            pf[c] = mm(q_v[l, core], b_v[half_cols, pl.ds(c * cw, cw)])
        relayed.wait_recv()

    def project(l, c):
        return pf[c] + mm(q_v[l, 1 - core], b_v[rest_cols, span(c, cw)])

    x1, z1, f1, u1, relay = {}, {}, {}, {}, {}

    def send0(c):
        share(st0.at[c, mine[0], :], sib, f"x{c // 2}")

    def send1(c):
        x1[c] = send(p1_s.at[c], p1_r.at[c], sib, f"y{c}")

    gather_q(0)
    for c in range(CHUNKS):
        st0[c, mine[0], :] = project(0, c).astype(BF)
        send0(c)

    w_mate.wait_recv()
    g_send.wait_recv()
    arrive("re", w_v.at[0, r])
    w_cols = w_v[0, :, :, mine[0]].reshape(2 * rank, rank)
    for n in range(2):
        h_v[n] = mm(g_v[n], w_cols).astype(BF)
    pair_sum = g_v[2, :, pl.ds(0, rank)].astype(F32) + g_v[2, :, pl.ds(rank, rank)].astype(F32)
    gs_v[:, mine[1]] = pair_sum.astype(BF)
    gs_send = share(gs_v.at[:, mine[1]], near, "gs")

    def cross(c):
        z1[c] = send(p1_s.at[c], st1.at[c, mine[1], :], near, f"z{c}")

    gather_q(1)
    for c in range(CHUNKS):
        part = project(1, c) - mm(h_v[0], st0[c, mine[0], :])
        p1f[c] = part
        p1_s[c] = part.astype(BF)
        if c < ZFIRST:
            st1[c, mine[1], :] = part.astype(BF)
        if c < 2:
            cross(c)

    gs_send.wait_recv()
    h_v[2] = mm(gs_v[...], w_v[1, :, :, mine[1]].reshape(2 * rank, rank)).astype(BF)

    gather_q(2)
    spot = 2 * sides[1] + sides[0]
    spots = (3 - spot, flip(spot, 1), flip(spot, 2), spot)
    team = (diag, sib, near)

    def level_two(n):
        who = spots[n]
        part = project(2, who) - mm(h_v[1], st0[who, mine[0], :]) - mm(h_v[2], p1_s[who])
        if n == 3:
            p2f[...] = part
        else:
            for h in range(2):
                p2_s[h, n] = part[:, h * hw:(h + 1) * hw].astype(BF)

    def send2(n, h):
        send(p2_s.at[h, n], p2_r.at[h, n], team[n], f"t{h}")

    level_two(0)
    send2(0, 0)
    level_two(1)
    send2(1, 0)
    send2(0, 1)
    send2(1, 1)
    level_two(2)
    send2(2, 0)
    send2(2, 1)
    level_two(3)
    cross(2)
    send1(3)
    arrive("wl", w_v.at[pl.ds(0, 2), r])
    for l in range(3):
        lanes = span(1 - sides[l], rank) if l < 2 else pl.ds(0, 2 * rank)
        share(w_v.at[l, over, :, lanes], mate, "rl")

    def answer_rows(l):
        return w_v[l, pl.ds(pl.multiple_of(sides[l] * 2, 2), 2), :, :].reshape(rank, 2 * rank)


    def first(pair):
        arrive(f"x{pair[0] // 2}", st0.at[pl.ds(pair[0], 2), mine[0], :])
        for c in pair:
            b_v[pl.ds(depth, rank), pl.ds(c * cw, cw)] = (-mm(answer_rows(0), st0[c])).astype(BF)

    def second_sum(c):
        x1[c].wait_recv()
        st1[c, mine[1], :] = (p1f[c] + p1_r[c].astype(F32)).astype(BF)
        z1[c] = share(st1.at[c, mine[1], :], near, f"z{c}")

    def second(c):
        z1[c].wait_recv()
        b_v[pl.ds(depth + rank, rank), pl.ds(c * cw, cw)] = (-mm(answer_rows(1), st1[c])).astype(BF)

    def second_part(c):
        z1[c].wait_recv()
        part = mm(answer_rows(1), st1[c])
        uf[c] = part
        u_s[c] = part.astype(BF)
        u1[c] = send(u_s.at[c], u_r.at[c], sib, f"u{c}")

    def second_join(c):
        u1[c].wait_recv()
        b_v[pl.ds(depth + rank, rank), pl.ds(c * cw, cw)] = (-(uf[c] + u_r[c].astype(F32))).astype(BF)

    def third_far(j):
        total = p2f[:, pl.ds(j * hw, hw)]
        arrive(f"t{j}", p2_r.at[j])
        for n in range(3):
            total = total + p2_r[j, n].astype(F32)
        st2[j, mine[2], :] = total.astype(BF)
        f1[j] = share(st2.at[j, mine[2], :], far, f"f{j}")

    def third(j):
        f1[j].wait_recv()
        where = (pl.ds(depth + 2 * rank, rank), span(2 * spot + j, hw))
        b_v[where] = (-mm(answer_rows(2), st2[j])).astype(BF)
        for to in team:
            share(b_v.at[where], to, "n")

    def relay_piece(k):
        a_across[k].wait_recv()
        relay[k] = share(a_v.at[span(over, blk), pl.ds(k * piece, piece)], mate, "r3" if k == PIECES - 1 else "r")

    early = depth - piece

    def add_pieces():
        for c in range(CHUNKS):
            own = pl.ds(c * cw, cw)
            acc[other_rows, own] = mm(a_v[other_rows, pl.ds(0, early)], b_v[pl.ds(0, early), own])

    def add_last():
        deep = pl.ds(early, piece)
        for c in range(CHUNKS):
            own = pl.ds(c * cw, cw)
            acc[other_rows, own] = acc[other_rows, own] + mm(a_v[other_rows, deep], b_v[deep, own])

    def finish(c):
        own = pl.ds(c * cw, cw)
        deep = pl.ds(depth, LEVELS * rank)
        out_v[:, own] = (acc[:, own] + mm(a_v[:, deep], b_v[deep, own])).astype(BF)

    arrive("rl", w_v.at[pl.ds(0, 2), r])
    first((0, 1))
    second_part(0)
    second_part(1)
    relay_piece(0)

    @pl.when(inner == 1)
    def _():
        pl.semaphore_wait(msem, 1)

    third_far(0)
    third_far(1)
    relay_piece(1)
    first((2, 3))
    second_sum(3)
    second_part(2)
    relay_piece(2)
    third(0)
    third(1)
    second_join(0)
    second_join(1)
    relay_piece(3)
    arrive("r", a_v.at[block, pl.ds(0, early)])
    add_pieces()
    second(3)
    second_join(2)
    relay[3].wait_recv()
    add_last()
    arrive("n", b_v.at[pl.ds(depth + 2 * rank, rank), pl.ds(0, (CHUNKS - 1) * cw)])
    for c in range(CHUNKS):
        finish(c)
    assert len(slots) == RECVS and len(places) == FETCHES, (len(slots), len(places))
    for copy in copies:
        copy.wait_send()


def local(right_sides, leaf_inverse, project_factors, correct_factors, *couplings):
    rows, cols = right_sides.shape
    blk, depth = leaf_inverse.shape
    levels, _, rank = project_factors.shape
    parts = lax.axis_size("rhs")
    cw = cols // CHUNKS
    whole = lambda dtype: pltpu.VMEM((CHUNKS, rank, cw), dtype)
    any_spec = pl.BlockSpec(memory_space=pltpu.HBM)
    return pl.pallas_call(
        kernel,
        out_shape=jax.ShapeDtypeStruct((rows, cols), BF),
        in_specs=[any_spec] * 7,
        out_specs=pl.BlockSpec(memory_space=pltpu.VMEM),
        scratch_shapes=[
            pltpu.VMEM((depth + levels * rank, cols), BF),
            pltpu.VMEM((rows, depth + levels * rank), BF),
            pltpu.VMEM((rows, levels * rank), BF),
            pltpu.VMEM((levels, rank, rows), BF),
            pltpu.VMEM((levels, parts) + couplings[0].shape[1:], BF),
            pltpu.VMEM((3, rank, 2 * rank), BF),
            pltpu.VMEM((rank, 2 * rank), BF),
            pltpu.VMEM((3, rank, rank), BF),
            pltpu.VMEM((levels, rank, depth // 2), F32),
            pltpu.VMEM((levels, rank, depth // 2), BF),
            pltpu.VMEM((levels, rank, depth // 2), BF),
            pltpu.VMEM((levels, 2, rank, depth // 2), BF),
            whole(F32),
            pltpu.VMEM((CHUNKS, 2 * rank, cw), BF),
            whole(F32), whole(BF), whole(BF),
            pltpu.VMEM((rank, cw), F32), pltpu.VMEM((2, 3, rank, cw // 2), BF),
            pltpu.VMEM((2, 3, rank, cw // 2), BF),
            pltpu.VMEM((CHUNKS, 2 * rank, cw), BF),
            pltpu.VMEM((2, 2 * rank, cw // 2), BF),
            pltpu.VMEM((ZFIRST, rank, cw), F32),
            pltpu.VMEM((ZFIRST, rank, cw), BF),
            pltpu.VMEM((ZFIRST, rank, cw), BF),
            pltpu.VMEM((rows, cols), F32),
            pltpu.SemaphoreType.DMA((FETCHES,)),
            pltpu.SemaphoreType.DMA((1,)),
            pltpu.SemaphoreType.DMA((RECVS,)),
            pltpu.SemaphoreType.REGULAR,
        ],
        compiler_params=pltpu.CompilerParams(
            collective_id=0, has_side_effects=True, vmem_limit_bytes=40 * 1024 * 1024
        ),
    )(*(
        pltpu.with_memory_space_constraint(x, pltpu.HBM)
        for x in (right_sides, leaf_inverse, project_factors, correct_factors, *couplings)
    ))


def solution(mesh):
    in_specs = (
        P("leaf", "rhs"),
        P(("leaf", "rhs"), None),
        P(None, "leaf", None),
        P(None, "leaf", None),
        P(None, "rhs", None),
        P(None, "rhs", None),
        P(None, "rhs", None),
    )
    out_specs = P("leaf", "rhs")
    return jax.shard_map(local, mesh=mesh, in_specs=in_specs, out_specs=out_specs, check_vma=False)
```

```python
import jax
import jax.numpy as jnp
from jax import lax
from jax.experimental import pallas as pl
from jax.experimental.pallas import tpu as pltpu
from jax.sharding import PartitionSpec as P

LEVELS = 3
CHUNKS = 4
PIECES = 4
ZFIRST = 3
RECVS = 41
FETCHES = 7
BF = jnp.bfloat16
F32 = jnp.float32


def mm(a, b):
    return jnp.dot(a, b, preferred_element_type=F32)


def bit_of(index, stride):
    return lax.rem(lax.div(index, stride), 2)


def flip(index, stride):
    return index + stride * (1 - 2 * bit_of(index, stride))


def span(which, size):
    return pl.ds(pl.multiple_of(which * size, size), size)


def kernel(
    b_hbm, a_hbm, p_hbm, c_hbm, w0_hbm, w1_hbm, w2_hbm, out_v,
    b_v, a_v, p_v, pt_v, w_v, g_v, gs_v, h_v, qf, q_s, q_r, q_v,
    pf, st0, p1f, p1_s, p1_r, p2f, p2_s, p2_r, st1, st2, a2_s, uf, u_s, u_r, acc,
    lsem, ssem, rsem, msem,
):
    i = lax.axis_index("leaf")
    r = lax.axis_index("rhs")
    blk = a_hbm.shape[0]
    depth = a_hbm.shape[1]
    cols = b_hbm.shape[1]
    rank = p_hbm.shape[2]
    cw = cols // CHUNKS
    hw = cw // 2
    half = depth // 2
    piece = depth // PIECES
    mate = {"rhs": flip(r, 1)}
    across = {"rhs": flip(r, 2)}
    sib = {"leaf": flip(i, 1)}
    near = {"leaf": flip(i, 2)}
    far = {"leaf": flip(i, 4)}
    mid = {"leaf": flip(flip(i, 2), 4)}
    sides = [bit_of(i, 1), bit_of(i, 2), bit_of(i, 4)]
    core = bit_of(r, 1)
    chip = bit_of(r, 2)

    copies = []
    slots = {}

    def slot(key):
        return slots.setdefault(key, len(slots))

    def send(src, dst, to, key, extra=None, keep=True):
        place = slot(key) if extra is None else slot(key) + extra
        copy = pltpu.make_async_remote_copy(
            src_ref=src, dst_ref=dst, send_sem=ssem.at[0], recv_sem=rsem.at[place],
            device_id=to, device_id_type=pl.DeviceIdType.MESH,
        )
        copy.start()
        if keep:
            copies.append(copy)
        return copy

    def arrive(key, ref):
        pltpu.make_async_copy(ref, ref, rsem.at[slot(key)]).wait()

    def fetched(key, ref):
        pltpu.make_async_copy(ref, ref, lsem.at[places[key]]).wait()

    def share(ref, to, key):
        return send(ref, ref, to, key)

    places = {}

    def fetch(src, dst, key):
        copy = pltpu.make_async_copy(src, dst, lsem.at[places.setdefault(key, len(places))])
        copy.start()
        return copy

    mine = [span(s, rank) for s in sides]
    block = span(r, blk)
    pair_rows = span(chip, 2 * blk)
    other_rows = span(1 - chip, 2 * blk)
    half_cols = span(core, half)
    rest_cols = span(1 - core, half)

    la = fetch(a_hbm, a_v.at[block, pl.ds(0, depth)], "a")
    lp = [fetch(p_hbm.at[0], p_v.at[:, pl.ds(0, rank)], "p0")]
    [
        fetch(w_hbm.at[lax.div(i, 2 << level)], w_v.at[level, r], "w")
        for level, w_hbm in enumerate((w0_hbm, w1_hbm, w2_hbm))
    ]
    lp += [fetch(p_hbm.at[l], p_v.at[:, pl.ds(l * rank, rank)], f"p{l}") for l in range(1, LEVELS)]
    [fetch(c_hbm.at[l], a_v.at[:, pl.ds(depth + l * rank, rank)], "c") for l in range(LEVELS)]
    lb = fetch(b_hbm, b_v.at[pl.ds(0, depth)], "b")

    barrier = pltpu.get_barrier_semaphore()
    inner = lax.rem(sides[1] + sides[2], 2)
    for to in (mate, across, sib, near):
        pl.semaphore_signal(barrier, inc=1, device_id=to, device_id_type=pl.DeviceIdType.MESH)

    @pl.when(inner == 1)
    def _():
        pl.semaphore_signal(barrier, inc=1, device_id=mid, device_id_type=pl.DeviceIdType.MESH)

    la.wait()
    pl.semaphore_wait(barrier, 4 + inner)

    @pl.when(inner == 1)
    def _():
        pl.semaphore_signal(msem, inc=1, device_id=mid, device_id_type=pl.DeviceIdType.MESH)


    a_mate = share(a_v.at[block, rest_cols], mate, "am")
    fetched("w", w_v.at[:, r])
    [share(w_v.at[l, r, :, mine[l]], across, "we") for l in range(2)]
    lp[0].wait()
    pt_v[0] = p_v[:, pl.ds(0, rank)].T
    a_mate.wait_recv()
    q_across = []
    for l in range(LEVELS):
        if l > 0:
            lp[l].wait()
            pt_v[l] = p_v[:, pl.ds(l * rank, rank)].T
        part = mm(pt_v[l, :, pair_rows], a_v[pair_rows, half_cols])
        qf[l] = part
        q_s[l] = part.astype(BF)
        q_across.append(send(q_s.at[l], q_r.at[l], across, f"q{l}"))
    a_mate2 = share(a_v.at[block, half_cols], mate, "an")
    w_mate = share(w_v.at[:, r], mate, "wm")
    [share(w_v.at[l, r, :, span(1 - sides[l], rank)], across, "wl") for l in range(2)]
    share(w_v.at[2, r], across, "wl")
    a_across = [share(a_v.at[block, pl.ds(k * piece, piece)], across, f"a{k}") for k in range(PIECES)]

    fetched("c", a_v.at[:, pl.ds(depth, LEVELS * rank)])
    for n, (l, k) in enumerate(((1, 0), (2, 0), (2, 1))):
        g_v[n, :, mine[0]] = mm(pt_v[l], a_v[:, pl.ds(depth + k * rank, rank)]).astype(BF)
    g_send = share(g_v.at[:, :, mine[0]], sib, "g")

    over = flip(r, 2)
    arrive("we", w_v.at[0, r])
    for l in range(2):
        share(w_v.at[l, over, :, mine[l]], mate, "re")
    lb.wait()
    a_mate2.wait_recv()
    for c in range(CHUNKS):
        own = pl.ds(c * cw, cw)
        acc[pair_rows, own] = mm(a_v[pair_rows, pl.ds(0, depth)], b_v[pl.ds(0, depth), own])

    def gather_q(l):
        q_across[l].wait_recv()
        q_v[l, core] = (qf[l] + q_r[l].astype(F32)).astype(BF)
        relayed = share(q_v.at[l, core], mate, f"m{l}")
        for c in range(CHUNKS):
            pf[c] = mm(q_v[l, core], b_v[half_cols, pl.ds(c * cw, cw)])
        relayed.wait_recv()

    def project(l, c):
        return pf[c] + mm(q_v[l, 1 - core], b_v[rest_cols, span(c, cw)])

    x1, z1, f1, u1, relay = {}, {}, {}, {}, {}

    def send0(c):
        share(st0.at[c, mine[0], :], sib, f"x{c // 2}")

    def send1(c):
        x1[c] = send(p1_s.at[c], p1_r.at[c], sib, f"y{c}")

    gather_q(0)
    for c in range(CHUNKS):
        st0[c, mine[0], :] = project(0, c).astype(BF)
        send0(c)

    w_mate.wait_recv()
    g_send.wait_recv()
    arrive("re", w_v.at[0, r])
    w_cols = w_v[0, :, :, mine[0]].reshape(2 * rank, rank)
    for n in range(2):
        h_v[n] = mm(g_v[n], w_cols).astype(BF)
    pair_sum = g_v[2, :, pl.ds(0, rank)].astype(F32) + g_v[2, :, pl.ds(rank, rank)].astype(F32)
    gs_v[:, mine[1]] = pair_sum.astype(BF)
    gs_send = share(gs_v.at[:, mine[1]], near, "gs")

    def cross(c):
        z1[c] = send(p1_s.at[c], st1.at[c, mine[1], :], near, f"z{c}")

    gather_q(1)
    for c in range(CHUNKS):
        part = project(1, c) - mm(h_v[0], st0[c, mine[0], :])
        p1f[c] = part
        p1_s[c] = part.astype(BF)
        if c < ZFIRST:
            st1[c, mine[1], :] = part.astype(BF)
        if c < 2:
            cross(c)

    gs_send.wait_recv()
    h_v[2] = mm(gs_v[...], w_v[1, :, :, mine[1]].reshape(2 * rank, rank)).astype(BF)

    gather_q(2)
    spot = 2 * sides[1] + sides[0]
    spots = (3 - spot, flip(spot, 1), flip(spot, 2), spot)
    leaves = (flip(flip(i, 1), 2), flip(i, 1), flip(i, 2))
    odd_team = [{"leaf": leaf, "rhs": 2 * chip + 1} for leaf in leaves]
    odd_keys = [[slot(f"t{w}{h}") for h in range(2)] for w in range(2)]

    def level_two(n):
        who = spots[n]
        part = project(2, who) - mm(h_v[1], st0[who, mine[0], :]) - mm(h_v[2], p1_s[who])
        if n == 3:
            p2f[core] = part
        else:
            for h in range(2):
                p2_s[h, n] = part[:, h * hw:(h + 1) * hw].astype(BF)

    def send2(n, h):
        send(p2_s.at[h, n], p2_r.at[core, h, n], odd_team[n], f"t0{h}", extra=2 * core)

    level_two(0)
    send2(0, 0)
    level_two(1)
    send2(1, 0)
    send2(0, 1)
    send2(1, 1)
    level_two(2)
    send2(2, 0)
    send2(2, 1)
    level_two(3)

    @pl.when(core == 0)
    def _():
        send(p2f.at[0], p2f.at[0], mate, "tf", keep=False)

    cross(2)
    send1(3)
    arrive("wl", w_v.at[pl.ds(0, 2), r])
    for l in range(3):
        lanes = span(1 - sides[l], rank) if l < 2 else pl.ds(0, 2 * rank)
        share(w_v.at[l, over, :, lanes], mate, "rl")

    def answer_rows(l):
        return w_v[l, pl.ds(pl.multiple_of(sides[l] * 2, 2), 2), :, :].reshape(rank, 2 * rank)


    def first(pair):
        arrive(f"x{pair[0] // 2}", st0.at[pl.ds(pair[0], 2), mine[0], :])
        for c in pair:
            b_v[pl.ds(depth, rank), pl.ds(c * cw, cw)] = (-mm(answer_rows(0), st0[c])).astype(BF)

    def second_sum(c):
        x1[c].wait_recv()
        st1[c, mine[1], :] = (p1f[c] + p1_r[c].astype(F32)).astype(BF)
        z1[c] = share(st1.at[c, mine[1], :], near, f"z{c}")

    def second(c):
        z1[c].wait_recv()
        b_v[pl.ds(depth + rank, rank), pl.ds(c * cw, cw)] = (-mm(answer_rows(1), st1[c])).astype(BF)

    def second_part(c):
        z1[c].wait_recv()
        part = mm(answer_rows(1), st1[c])
        uf[c] = part
        u_s[c] = part.astype(BF)
        u1[c] = send(u_s.at[c], u_r.at[c], sib, f"u{c}")

    def second_join(c):
        u1[c].wait_recv()
        b_v[pl.ds(depth + rank, rank), pl.ds(c * cw, cw)] = (-(uf[c] + u_r[c].astype(F32))).astype(BF)

    where = [(pl.ds(depth + 2 * rank, rank), span(2 * spot + j, hw)) for j in range(2)]
    same_team = [{"leaf": leaf} for leaf in leaves]
    even_team = [{"leaf": leaf, "rhs": flip(r, 1)} for leaf in leaves] + [mate]

    def third_far(w, j):
        total = p2f[w, :, pl.ds(j * hw, hw)]
        arrive(f"t{w}{j}", p2_r.at[w, j])
        for n in range(3):
            total = total + p2_r[w, j, n].astype(F32)
        st2[w, j, mine[2], :] = total.astype(BF)
        ours = st2.at[w, j, mine[2], :]
        send(ours, ours, far, f"f{w}{j}", keep=False)

    def third(w, j):
        arrive(f"f{w}{j}", st2.at[w, j, mine[2], :])
        value = (-mm(answer_rows(2), st2[w, j])).astype(BF)
        if w == 1:
            b_v[where[j]] = value
            for to in same_team:
                send(b_v.at[where[j]], b_v.at[where[j]], to, "n", keep=False)
        else:
            a2_s[j] = value
            for to in even_team:
                send(a2_s.at[j], b_v.at[where[j]], to, "n", keep=False)

    def relay_piece(k):
        a_across[k].wait_recv()
        relay[k] = share(a_v.at[span(over, blk), pl.ds(k * piece, piece)], mate, "r3" if k == PIECES - 1 else "r")

    early = depth - piece

    def add_pieces():
        for c in range(CHUNKS):
            own = pl.ds(c * cw, cw)
            acc[other_rows, own] = mm(a_v[other_rows, pl.ds(0, early)], b_v[pl.ds(0, early), own])

    def add_last():
        deep = pl.ds(early, piece)
        for c in range(CHUNKS):
            own = pl.ds(c * cw, cw)
            acc[other_rows, own] = acc[other_rows, own] + mm(a_v[other_rows, deep], b_v[deep, own])

    def finish(c):
        own = pl.ds(c * cw, cw)
        deep = pl.ds(depth, LEVELS * rank)
        out_v[:, own] = (acc[:, own] + mm(a_v[:, deep], b_v[deep, own])).astype(BF)

    arrive("rl", w_v.at[pl.ds(0, 2), r])
    first((0, 1))
    second_part(0)
    second_part(1)
    relay_piece(0)

    @pl.when(inner == 1)
    def _():
        pl.semaphore_wait(msem, 1)

    @pl.when(core == 1)
    def _():
        arrive("tf", p2f.at[0])
        for j in range(2):
            third_far(1, j)
            third_far(0, j)

    relay_piece(1)
    first((2, 3))
    second_sum(3)
    second_part(2)
    relay_piece(2)

    @pl.when(core == 1)
    def _():
        for j in range(2):
            third(1, j)
            third(0, j)

    second_join(0)
    second_join(1)
    relay_piece(3)
    arrive("r", a_v.at[block, pl.ds(0, early)])
    add_pieces()
    second(3)
    second_join(2)
    relay[3].wait_recv()
    add_last()
    answers = pl.ds(depth + 2 * rank, rank)

    @pl.when(core == 1)
    def _():
        arrive("n", b_v.at[answers, pl.ds(0, (CHUNKS - 1) * cw)])

    @pl.when(core == 0)
    def _():
        arrive("n", b_v.at[answers, pl.ds(0, CHUNKS * cw)])

    for c in range(CHUNKS):
        finish(c)
    assert len(slots) == RECVS and len(places) == FETCHES, (len(slots), len(places))
    for copy in copies:
        copy.wait_send()

    def sent(ref):
        pltpu.make_async_copy(ref, ref, ssem.at[0]).wait()

    @pl.when(core == 1)
    def _():
        for w in range(2):
            sent(b_v.at[answers, pl.ds(0, CHUNKS * cw)])
        sent(st2.at[0, 0])

    @pl.when(core == 0)
    def _():
        sent(p2f.at[0])


def local(right_sides, leaf_inverse, project_factors, correct_factors, *couplings):
    rows, cols = right_sides.shape
    blk, depth = leaf_inverse.shape
    levels, _, rank = project_factors.shape
    parts = lax.axis_size("rhs")
    cw = cols // CHUNKS
    whole = lambda dtype: pltpu.VMEM((CHUNKS, rank, cw), dtype)
    any_spec = pl.BlockSpec(memory_space=pltpu.HBM)
    return pl.pallas_call(
        kernel,
        out_shape=jax.ShapeDtypeStruct((rows, cols), BF),
        in_specs=[any_spec] * 7,
        out_specs=pl.BlockSpec(memory_space=pltpu.VMEM),
        scratch_shapes=[
            pltpu.VMEM((depth + levels * rank, cols), BF),
            pltpu.VMEM((rows, depth + levels * rank), BF),
            pltpu.VMEM((rows, levels * rank), BF),
            pltpu.VMEM((levels, rank, rows), BF),
            pltpu.VMEM((levels, parts) + couplings[0].shape[1:], BF),
            pltpu.VMEM((3, rank, 2 * rank), BF),
            pltpu.VMEM((rank, 2 * rank), BF),
            pltpu.VMEM((3, rank, rank), BF),
            pltpu.VMEM((levels, rank, depth // 2), F32),
            pltpu.VMEM((levels, rank, depth // 2), BF),
            pltpu.VMEM((levels, rank, depth // 2), BF),
            pltpu.VMEM((levels, 2, rank, depth // 2), BF),
            whole(F32),
            pltpu.VMEM((CHUNKS, 2 * rank, cw), BF),
            whole(F32), whole(BF), whole(BF),
            pltpu.VMEM((2, rank, cw), F32), pltpu.VMEM((2, 3, rank, cw // 2), BF),
            pltpu.VMEM((2, 2, 3, rank, cw // 2), BF),
            pltpu.VMEM((CHUNKS, 2 * rank, cw), BF),
            pltpu.VMEM((2, 2, 2 * rank, cw // 2), BF),
            pltpu.VMEM((2, rank, cw // 2), BF),
            pltpu.VMEM((ZFIRST, rank, cw), F32),
            pltpu.VMEM((ZFIRST, rank, cw), BF),
            pltpu.VMEM((ZFIRST, rank, cw), BF),
            pltpu.VMEM((rows, cols), F32),
            pltpu.SemaphoreType.DMA((FETCHES,)),
            pltpu.SemaphoreType.DMA((1,)),
            pltpu.SemaphoreType.DMA((RECVS,)),
            pltpu.SemaphoreType.REGULAR,
        ],
        compiler_params=pltpu.CompilerParams(
            collective_id=0, has_side_effects=True, vmem_limit_bytes=40 * 1024 * 1024
        ),
    )(*(
        pltpu.with_memory_space_constraint(x, pltpu.HBM)
        for x in (right_sides, leaf_inverse, project_factors, correct_factors, *couplings)
    ))


def solution(mesh):
    in_specs = (
        P("leaf", "rhs"),
        P(("leaf", "rhs"), None),
        P(None, "leaf", None),
        P(None, "leaf", None),
        P(None, "rhs", None),
        P(None, "rhs", None),
        P(None, "rhs", None),
    )
    out_specs = P("leaf", "rhs")
    return jax.shard_map(local, mesh=mesh, in_specs=in_specs, out_specs=out_specs, check_vma=False)
```

```python
import jax
import jax.numpy as jnp
from jax import lax
from jax.experimental import pallas as pl
from jax.experimental.pallas import tpu as pltpu
from jax.sharding import PartitionSpec as P

LEVELS = 3
CHUNKS = 4
SPLIT = ((0, 1), (1, 2), (3, 2), (5, 2), (7, 1))
UNITS = 8
ZFIRST = 3
RECVS = 43
FETCHES = 7
BF = jnp.bfloat16
F32 = jnp.float32


def mm(a, b):
    return jnp.dot(a, b, preferred_element_type=F32)


def bit_of(index, stride):
    return lax.rem(lax.div(index, stride), 2)


def flip(index, stride):
    return index + stride * (1 - 2 * bit_of(index, stride))


def span(which, size):
    return pl.ds(pl.multiple_of(which * size, size), size)


def kernel(
    b_hbm, a_hbm, p_hbm, c_hbm, w0_hbm, w1_hbm, w2_hbm, out_v,
    b_v, a_v, p_v, pt_v, w_v, g_v, gs_v, h_v, qf, q_s, q_r, q_v,
    pf, st0, p1f, p1_s, p1_r, p2f, p2_s, p2o, p2_r, st1, st2, a2_s, uf, u_s, u_r, acc,
    lsem, ssem, rsem, msem,
):
    i = lax.axis_index("leaf")
    r = lax.axis_index("rhs")
    blk = a_hbm.shape[0]
    depth = a_hbm.shape[1]
    cols = b_hbm.shape[1]
    rank = p_hbm.shape[2]
    cw = cols // CHUNKS
    hw = cw // 2
    half = depth // 2
    unit = depth // UNITS
    pieces = [pl.ds(at * unit, size * unit) for at, size in SPLIT]
    final = len(SPLIT) - 1
    mate = {"rhs": flip(r, 1)}
    across = {"rhs": flip(r, 2)}
    sib = {"leaf": flip(i, 1)}
    near = {"leaf": flip(i, 2)}
    far = {"leaf": flip(i, 4)}
    mid = {"leaf": flip(flip(i, 2), 4)}
    sides = [bit_of(i, 1), bit_of(i, 2), bit_of(i, 4)]
    core = bit_of(r, 1)
    chip = bit_of(r, 2)

    copies = []
    slots = {}

    def slot(key):
        return slots.setdefault(key, len(slots))

    def send(src, dst, to, key, extra=None, keep=True):
        place = slot(key) if extra is None else slot(key) + extra
        copy = pltpu.make_async_remote_copy(
            src_ref=src, dst_ref=dst, send_sem=ssem.at[0], recv_sem=rsem.at[place],
            device_id=to, device_id_type=pl.DeviceIdType.MESH,
        )
        copy.start()
        if keep:
            copies.append(copy)
        return copy

    def arrive(key, ref):
        pltpu.make_async_copy(ref, ref, rsem.at[slot(key)]).wait()

    def fetched(key, ref):
        pltpu.make_async_copy(ref, ref, lsem.at[places[key]]).wait()

    def share(ref, to, key):
        return send(ref, ref, to, key)

    places = {}

    def fetch(src, dst, key):
        copy = pltpu.make_async_copy(src, dst, lsem.at[places.setdefault(key, len(places))])
        copy.start()
        return copy

    mine = [span(s, rank) for s in sides]
    block = span(r, blk)
    pair_rows = span(chip, 2 * blk)
    other_rows = span(1 - chip, 2 * blk)
    half_cols = span(core, half)
    rest_cols = span(1 - core, half)

    la = fetch(a_hbm, a_v.at[block, pl.ds(0, depth)], "a")
    lp = [fetch(p_hbm.at[0], p_v.at[:, pl.ds(0, rank)], "p0")]
    [
        fetch(w_hbm.at[lax.div(i, 2 << level)], w_v.at[level, r], "w")
        for level, w_hbm in enumerate((w0_hbm, w1_hbm, w2_hbm))
    ]
    lp += [fetch(p_hbm.at[l], p_v.at[:, pl.ds(l * rank, rank)], f"p{l}") for l in range(1, LEVELS)]
    [fetch(c_hbm.at[l], a_v.at[:, pl.ds(depth + l * rank, rank)], "c") for l in range(LEVELS)]
    lb = fetch(b_hbm, b_v.at[pl.ds(0, depth)], "b")

    barrier = pltpu.get_barrier_semaphore()
    inner = lax.rem(sides[1] + sides[2], 2)
    for to in (mate, across, sib, near):
        pl.semaphore_signal(barrier, inc=1, device_id=to, device_id_type=pl.DeviceIdType.MESH)

    @pl.when(inner == 1)
    def _():
        pl.semaphore_signal(barrier, inc=1, device_id=mid, device_id_type=pl.DeviceIdType.MESH)

    la.wait()
    pl.semaphore_wait(barrier, 4 + inner)

    @pl.when(inner == 1)
    def _():
        pl.semaphore_signal(msem, inc=1, device_id=mid, device_id_type=pl.DeviceIdType.MESH)


    a_mate = share(a_v.at[block, rest_cols], mate, "am")
    a_across = [share(a_v.at[block, pieces[0]], across, "a0")]
    fetched("w", w_v.at[:, r])
    [share(w_v.at[l, r, :, mine[l]], across, "we") for l in range(2)]
    lp[0].wait()
    pt_v[0] = p_v[:, pl.ds(0, rank)].T
    a_mate.wait_recv()
    q_across = []
    for l in range(LEVELS):
        if l > 0:
            lp[l].wait()
            pt_v[l] = p_v[:, pl.ds(l * rank, rank)].T
        part = mm(pt_v[l, :, pair_rows], a_v[pair_rows, half_cols])
        qf[l] = part
        q_s[l] = part.astype(BF)
        q_across.append(send(q_s.at[l], q_r.at[l], across, f"q{l}"))
    a_mate2 = share(a_v.at[block, half_cols], mate, "an")
    w_mate = share(w_v.at[:, r], mate, "wm")
    [share(w_v.at[l, r, :, span(1 - sides[l], rank)], across, "wl") for l in range(2)]
    share(w_v.at[2, r], across, "wl")
    for k in range(1, len(SPLIT)):
        a_across.append(share(a_v.at[block, pieces[k]], across, f"a{k}"))

    fetched("c", a_v.at[:, pl.ds(depth, LEVELS * rank)])
    for n, (l, k) in enumerate(((1, 0), (2, 0), (2, 1))):
        g_v[n, :, mine[0]] = mm(pt_v[l], a_v[:, pl.ds(depth + k * rank, rank)]).astype(BF)
    g_send = share(g_v.at[:, :, mine[0]], sib, "g")

    over = flip(r, 2)
    arrive("we", w_v.at[0, r])
    for l in range(2):
        share(w_v.at[l, over, :, mine[l]], mate, "re")
    lb.wait()
    a_mate2.wait_recv()
    for c in range(CHUNKS):
        own = pl.ds(c * cw, cw)
        acc[pair_rows, own] = mm(a_v[pair_rows, pl.ds(0, depth)], b_v[pl.ds(0, depth), own])

    def gather_q(l):
        q_across[l].wait_recv()
        q_v[l, core] = (qf[l] + q_r[l].astype(F32)).astype(BF)
        relayed = share(q_v.at[l, core], mate, f"m{l}")
        for c in range(CHUNKS):
            pf[c] = mm(q_v[l, core], b_v[half_cols, pl.ds(c * cw, cw)])
        relayed.wait_recv()

    def project(l, c):
        return pf[c] + mm(q_v[l, 1 - core], b_v[rest_cols, span(c, cw)])

    x1, z1, f1, u1, relay = {}, {}, {}, {}, {}

    def send0(c):
        share(st0.at[c, mine[0], :], sib, f"x{c // 2}")

    def send1(c):
        x1[c] = send(p1_s.at[c], p1_r.at[c], sib, f"y{c}")

    gather_q(0)
    for c in range(CHUNKS):
        st0[c, mine[0], :] = project(0, c).astype(BF)
        send0(c)

    w_mate.wait_recv()
    g_send.wait_recv()
    arrive("re", w_v.at[0, r])
    w_cols = w_v[0, :, :, mine[0]].reshape(2 * rank, rank)
    for n in range(2):
        h_v[n] = mm(g_v[n], w_cols).astype(BF)
    pair_sum = g_v[2, :, pl.ds(0, rank)].astype(F32) + g_v[2, :, pl.ds(rank, rank)].astype(F32)
    gs_v[:, mine[1]] = pair_sum.astype(BF)
    gs_send = share(gs_v.at[:, mine[1]], near, "gs")

    def cross(c):
        z1[c] = send(p1_s.at[c], st1.at[c, mine[1], :], near, f"z{c}")

    gather_q(1)
    for c in range(CHUNKS):
        part = project(1, c) - mm(h_v[0], st0[c, mine[0], :])
        p1f[c] = part
        p1_s[c] = part.astype(BF)
        if c < ZFIRST:
            st1[c, mine[1], :] = part.astype(BF)
        if c < 2:
            cross(c)

    gs_send.wait_recv()
    h_v[2] = mm(gs_v[...], w_v[1, :, :, mine[1]].reshape(2 * rank, rank)).astype(BF)

    gather_q(2)
    spot = 2 * sides[1] + sides[0]
    spots = (3 - spot, flip(spot, 1), flip(spot, 2), spot)
    leaves = (flip(flip(i, 1), 2), flip(i, 1), flip(i, 2))
    odd_team = [{"leaf": leaf, "rhs": 2 * chip + 1} for leaf in leaves]
    odd_keys = [[slot(f"t{w}{h}") for h in range(2)] for w in range(2)]

    def part_of(who, h):
        return 2 * h + lax.div(who, 2), slice(None), span(lax.rem(who, 2), hw)

    for h in range(2):
        for c in (2 * h, 2 * h + 1):
            part = project(2, c) - mm(h_v[1], st0[c, mine[0], :]) - mm(h_v[2], p1_s[c])
            p2f[c] = part
            p2_s[c] = part.astype(BF)
        for n in range(3):
            send(p2_s.at[part_of(spots[n], h)], p2_r.at[core, h, n], odd_team[n], f"t0{h}", extra=2 * core)
        p2o[core, h] = p2f[part_of(spot, h)]

    @pl.when(core == 0)
    def _():
        send(p2o.at[0], p2o.at[0], mate, "tf", keep=False)

    cross(2)
    send1(3)
    arrive("wl", w_v.at[pl.ds(0, 2), r])
    for l in range(3):
        lanes = span(1 - sides[l], rank) if l < 2 else pl.ds(0, 2 * rank)
        share(w_v.at[l, over, :, lanes], mate, "rl")

    def answer_rows(l):
        return w_v[l, pl.ds(pl.multiple_of(sides[l] * 2, 2), 2), :, :].reshape(rank, 2 * rank)


    def first(pair):
        arrive(f"x{pair[0] // 2}", st0.at[pl.ds(pair[0], 2), mine[0], :])
        for c in pair:
            b_v[pl.ds(depth, rank), pl.ds(c * cw, cw)] = (-mm(answer_rows(0), st0[c])).astype(BF)

    def second_sum(c):
        x1[c].wait_recv()
        st1[c, mine[1], :] = (p1f[c] + p1_r[c].astype(F32)).astype(BF)
        z1[c] = share(st1.at[c, mine[1], :], near, f"z{c}")

    def second(c):
        z1[c].wait_recv()
        b_v[pl.ds(depth + rank, rank), pl.ds(c * cw, cw)] = (-mm(answer_rows(1), st1[c])).astype(BF)

    def second_part(c):
        z1[c].wait_recv()
        part = mm(answer_rows(1), st1[c])
        uf[c] = part
        u_s[c] = part.astype(BF)
        u1[c] = send(u_s.at[c], u_r.at[c], sib, f"u{c}")

    def second_join(c):
        u1[c].wait_recv()
        b_v[pl.ds(depth + rank, rank), pl.ds(c * cw, cw)] = (-(uf[c] + u_r[c].astype(F32))).astype(BF)

    where = [(pl.ds(depth + 2 * rank, rank), span(4 * j + spot, hw)) for j in range(2)]
    same_team = [{"leaf": leaf} for leaf in leaves]
    even_team = [{"leaf": leaf, "rhs": flip(r, 1)} for leaf in leaves] + [mate]

    def third_far(w, j):
        total = p2o[w, j]
        arrive(f"t{w}{j}", p2_r.at[w, j])
        for n in range(3):
            total = total + p2_r[w, j, n].astype(F32)
        st2[w, j, mine[2], :] = total.astype(BF)
        ours = st2.at[w, j, mine[2], :]
        send(ours, ours, far, f"f{w}{j}", keep=False)

    def third(w, j):
        arrive(f"f{w}{j}", st2.at[w, j, mine[2], :])
        value = (-mm(answer_rows(2), st2[w, j])).astype(BF)
        if w == 1:
            b_v[where[j]] = value
            for to in same_team:
                send(b_v.at[where[j]], b_v.at[where[j]], to, f"n{j}", keep=False)
        else:
            a2_s[j] = value
            for to in even_team:
                send(a2_s.at[j], b_v.at[where[j]], to, f"n{j}", keep=False)

    def relay_piece(k):
        a_across[k].wait_recv()
        relay[k] = share(a_v.at[span(over, blk), pieces[k]], mate, "rf" if k == final else "r")

    early = SPLIT[final][0] * unit

    def add_pieces():
        for c in range(CHUNKS):
            own = pl.ds(c * cw, cw)
            acc[other_rows, own] = mm(a_v[other_rows, pl.ds(0, early)], b_v[pl.ds(0, early), own])

    def add_last():
        deep = pieces[final]
        for c in range(CHUNKS):
            own = pl.ds(c * cw, cw)
            acc[other_rows, own] = acc[other_rows, own] + mm(a_v[other_rows, deep], b_v[deep, own])

    def finish(c):
        own = pl.ds(c * cw, cw)
        deep = pl.ds(depth, LEVELS * rank)
        out_v[:, own] = (acc[:, own] + mm(a_v[:, deep], b_v[deep, own])).astype(BF)

    arrive("rl", w_v.at[pl.ds(0, 2), r])
    first((0, 1))
    second_part(0)
    second_part(1)
    relay_piece(0)
    relay_piece(1)

    @pl.when(inner == 1)
    def _():
        pl.semaphore_wait(msem, 1)

    @pl.when(core == 1)
    def _():
        arrive("tf", p2o.at[0])
        for j in range(2):
            third_far(1, j)
            third_far(0, j)

    relay_piece(2)
    first((2, 3))
    second_sum(3)
    second_part(2)
    relay_piece(3)

    @pl.when(core == 1)
    def _():
        for j in range(2):
            third(1, j)
            third(0, j)

    second_join(0)
    second_join(1)
    relay_piece(final)
    arrive("r", a_v.at[block, pl.ds(0, early)])
    add_pieces()
    second(3)
    second_join(2)
    relay[final].wait_recv()
    add_last()
    answers = pl.ds(depth + 2 * rank, rank)

    for j in range(2):

        @pl.when(core == 1)
        def _():
            arrive(f"n{j}", b_v.at[answers, pl.ds(0, 3 * hw)])

        @pl.when(core == 0)
        def _():
            arrive(f"n{j}", b_v.at[answers, pl.ds(0, 4 * hw)])

        finish(2 * j)
        finish(2 * j + 1)
    assert len(slots) == RECVS and len(places) == FETCHES, (len(slots), len(places))
    for copy in copies:
        copy.wait_send()

    def sent(ref):
        pltpu.make_async_copy(ref, ref, ssem.at[0]).wait()

    @pl.when(core == 1)
    def _():
        for w in range(2):
            sent(b_v.at[answers, pl.ds(0, CHUNKS * cw)])
        sent(st2.at[0, 0])

    @pl.when(core == 0)
    def _():
        sent(p2o.at[0])


def local(right_sides, leaf_inverse, project_factors, correct_factors, *couplings):
    rows, cols = right_sides.shape
    blk, depth = leaf_inverse.shape
    levels, _, rank = project_factors.shape
    parts = lax.axis_size("rhs")
    cw = cols // CHUNKS
    whole = lambda dtype: pltpu.VMEM((CHUNKS, rank, cw), dtype)
    any_spec = pl.BlockSpec(memory_space=pltpu.HBM)
    return pl.pallas_call(
        kernel,
        out_shape=jax.ShapeDtypeStruct((rows, cols), BF),
        in_specs=[any_spec] * 7,
        out_specs=pl.BlockSpec(memory_space=pltpu.VMEM),
        scratch_shapes=[
            pltpu.VMEM((depth + levels * rank, cols), BF),
            pltpu.VMEM((rows, depth + levels * rank), BF),
            pltpu.VMEM((rows, levels * rank), BF),
            pltpu.VMEM((levels, rank, rows), BF),
            pltpu.VMEM((levels, parts) + couplings[0].shape[1:], BF),
            pltpu.VMEM((3, rank, 2 * rank), BF),
            pltpu.VMEM((rank, 2 * rank), BF),
            pltpu.VMEM((3, rank, rank), BF),
            pltpu.VMEM((levels, rank, depth // 2), F32),
            pltpu.VMEM((levels, rank, depth // 2), BF),
            pltpu.VMEM((levels, rank, depth // 2), BF),
            pltpu.VMEM((levels, 2, rank, depth // 2), BF),
            whole(F32),
            pltpu.VMEM((CHUNKS, 2 * rank, cw), BF),
            whole(F32), whole(BF), whole(BF),
            whole(F32), whole(BF), pltpu.VMEM((2, 2, rank, cw // 2), F32),
            pltpu.VMEM((2, 2, 3, rank, cw // 2), BF),
            pltpu.VMEM((CHUNKS, 2 * rank, cw), BF),
            pltpu.VMEM((2, 2, 2 * rank, cw // 2), BF),
            pltpu.VMEM((2, rank, cw // 2), BF),
            pltpu.VMEM((ZFIRST, rank, cw), F32),
            pltpu.VMEM((ZFIRST, rank, cw), BF),
            pltpu.VMEM((ZFIRST, rank, cw), BF),
            pltpu.VMEM((rows, cols), F32),
            pltpu.SemaphoreType.DMA((FETCHES,)),
            pltpu.SemaphoreType.DMA((1,)),
            pltpu.SemaphoreType.DMA((RECVS,)),
            pltpu.SemaphoreType.REGULAR,
        ],
        compiler_params=pltpu.CompilerParams(
            collective_id=0, has_side_effects=True, vmem_limit_bytes=40 * 1024 * 1024
        ),
    )(*(
        pltpu.with_memory_space_constraint(x, pltpu.HBM)
        for x in (right_sides, leaf_inverse, project_factors, correct_factors, *couplings)
    ))


def solution(mesh):
    in_specs = (
        P("leaf", "rhs"),
        P(("leaf", "rhs"), None),
        P(None, "leaf", None),
        P(None, "leaf", None),
        P(None, "rhs", None),
        P(None, "rhs", None),
        P(None, "rhs", None),
    )
    out_specs = P("leaf", "rhs")
    return jax.shard_map(local, mesh=mesh, in_specs=in_specs, out_specs=out_specs, check_vma=False)
```

```python
import jax
import jax.numpy as jnp
from jax import lax
from jax.experimental import pallas as pl
from jax.experimental.pallas import tpu as pltpu
from jax.sharding import PartitionSpec as P

LEVELS = 3
CHUNKS = 4
SPLIT = ((0, 1), (1, 2), (3, 2), (5, 2), (7, 1))
UNITS = 8
ZFIRST = 3
RECVS = 43
FETCHES = 7
BF = jnp.bfloat16
F32 = jnp.float32


def mm(a, b):
    return jnp.dot(a, b, preferred_element_type=F32)


def bit_of(index, stride):
    return lax.rem(lax.div(index, stride), 2)


def flip(index, stride):
    return index + stride * (1 - 2 * bit_of(index, stride))


def span(which, size):
    return pl.ds(pl.multiple_of(which * size, size), size)


def kernel(
    b_hbm, a_hbm, p_hbm, c_hbm, w0_hbm, w1_hbm, w2_hbm, out_v,
    b_v, a_v, p_v, pt_v, w_v, g_v, gs_v, h_v, qf, q_s, q_r, q_v,
    pf, st0, p1f, p1_s, p1_r, p2f, p2_s, p2o, p2_r, st1, st2, a2_s, uf, u_s, u_r, acc,
    lsem, ssem, rsem, msem,
):
    i = lax.axis_index("leaf")
    r = lax.axis_index("rhs")
    blk = a_hbm.shape[0]
    depth = a_hbm.shape[1]
    cols = b_hbm.shape[1]
    rank = p_hbm.shape[2]
    cw = cols // CHUNKS
    hw = cw // 2
    half = depth // 2
    unit = depth // UNITS
    pieces = [pl.ds(at * unit, size * unit) for at, size in SPLIT]
    final = len(SPLIT) - 1
    mate = {"rhs": flip(r, 1)}
    across = {"rhs": flip(r, 2)}
    sib = {"leaf": flip(i, 1)}
    near = {"leaf": flip(i, 2)}
    far = {"leaf": flip(i, 4)}
    mid = {"leaf": flip(flip(i, 2), 4)}
    sides = [bit_of(i, 1), bit_of(i, 2), bit_of(i, 4)]
    core = bit_of(r, 1)
    chip = bit_of(r, 2)

    copies = []
    slots = {}

    def slot(key):
        return slots.setdefault(key, len(slots))

    def send(src, dst, to, key, extra=None, keep=True):
        place = slot(key) if extra is None else slot(key) + extra
        copy = pltpu.make_async_remote_copy(
            src_ref=src, dst_ref=dst, send_sem=ssem.at[0], recv_sem=rsem.at[place],
            device_id=to, device_id_type=pl.DeviceIdType.MESH,
        )
        copy.start()
        if keep:
            copies.append(copy)
        return copy

    def arrive(key, ref):
        pltpu.make_async_copy(ref, ref, rsem.at[slot(key)]).wait()

    def fetched(key, ref):
        pltpu.make_async_copy(ref, ref, lsem.at[places[key]]).wait()

    def share(ref, to, key):
        return send(ref, ref, to, key)

    places = {}

    def fetch(src, dst, key):
        copy = pltpu.make_async_copy(src, dst, lsem.at[places.setdefault(key, len(places))])
        copy.start()
        return copy

    mine = [span(s, rank) for s in sides]
    block = span(r, blk)
    pair_rows = span(chip, 2 * blk)
    other_rows = span(1 - chip, 2 * blk)
    half_cols = span(core, half)
    rest_cols = span(1 - core, half)

    la = fetch(a_hbm, a_v.at[block, pl.ds(0, depth)], "a")
    lp = [fetch(p_hbm.at[0], p_v.at[:, pl.ds(0, rank)], "p0")]
    [
        fetch(w_hbm.at[lax.div(i, 2 << level)], w_v.at[level, r], "w")
        for level, w_hbm in enumerate((w0_hbm, w1_hbm, w2_hbm))
    ]
    lp += [fetch(p_hbm.at[l], p_v.at[:, pl.ds(l * rank, rank)], f"p{l}") for l in range(1, LEVELS)]
    [fetch(c_hbm.at[l], a_v.at[:, pl.ds(depth + l * rank, rank)], "c") for l in range(LEVELS)]
    lb = fetch(b_hbm, b_v.at[pl.ds(0, depth)], "b")

    barrier = pltpu.get_barrier_semaphore()
    inner = lax.rem(sides[1] + sides[2], 2)
    for to in (mate, across, sib, near):
        pl.semaphore_signal(barrier, inc=1, device_id=to, device_id_type=pl.DeviceIdType.MESH)

    @pl.when(inner == 1)
    def _():
        pl.semaphore_signal(barrier, inc=1, device_id=mid, device_id_type=pl.DeviceIdType.MESH)

    la.wait()
    pl.semaphore_wait(barrier, 4 + inner)

    @pl.when(inner == 1)
    def _():
        pl.semaphore_signal(msem, inc=1, device_id=mid, device_id_type=pl.DeviceIdType.MESH)


    a_mate = share(a_v.at[block, rest_cols], mate, "am")
    a_across = [share(a_v.at[block, pieces[0]], across, "a0")]
    fetched("w", w_v.at[:, r])
    [share(w_v.at[l, r, :, mine[l]], across, "we") for l in range(2)]
    lp[0].wait()
    pt_v[0] = p_v[:, pl.ds(0, rank)].T
    a_mate.wait_recv()
    q_across = []
    for l in range(LEVELS):
        if l > 0:
            lp[l].wait()
            pt_v[l] = p_v[:, pl.ds(l * rank, rank)].T
        part = mm(pt_v[l, :, pair_rows], a_v[pair_rows, half_cols])
        qf[l] = part
        q_s[l] = part.astype(BF)
        q_across.append(send(q_s.at[l], q_r.at[l], across, f"q{l}"))
    a_mate2 = share(a_v.at[block, half_cols], mate, "an")
    w_mate = share(w_v.at[:, r], mate, "wm")
    [share(w_v.at[l, r, :, span(1 - sides[l], rank)], across, "wl") for l in range(2)]
    share(w_v.at[2, r], across, "wl")
    for k in range(1, len(SPLIT)):
        a_across.append(share(a_v.at[block, pieces[k]], across, f"a{k}"))

    fetched("c", a_v.at[:, pl.ds(depth, LEVELS * rank)])
    for n, (l, k) in enumerate(((1, 0), (2, 0), (2, 1))):
        g_v[n, :, mine[0]] = mm(pt_v[l], a_v[:, pl.ds(depth + k * rank, rank)]).astype(BF)
    g_send = share(g_v.at[:, :, mine[0]], sib, "g")

    over = flip(r, 2)
    arrive("we", w_v.at[0, r])
    for l in range(2):
        share(w_v.at[l, over, :, mine[l]], mate, "re")
    lb.wait()
    a_mate2.wait_recv()
    for c in range(CHUNKS):
        own = pl.ds(c * cw, cw)
        acc[pair_rows, own] = mm(a_v[pair_rows, pl.ds(0, depth)], b_v[pl.ds(0, depth), own])

    def gather_q(l):
        q_across[l].wait_recv()
        q_v[l, core] = (qf[l] + q_r[l].astype(F32)).astype(BF)
        relayed = share(q_v.at[l, core], mate, f"m{l}")
        for c in range(CHUNKS):
            pf[c] = mm(q_v[l, core], b_v[half_cols, pl.ds(c * cw, cw)])
        relayed.wait_recv()

    def project(l, c):
        return pf[c] + mm(q_v[l, 1 - core], b_v[rest_cols, span(c, cw)])

    x1, z1, f1, u1, relay = {}, {}, {}, {}, {}

    def send0(c):
        share(st0.at[c, mine[0], :], sib, f"x{c // 2}")

    def send1(c):
        x1[c] = send(p1_s.at[c], p1_r.at[c], sib, f"y{c}")

    gather_q(0)
    for c in range(CHUNKS):
        st0[c, mine[0], :] = project(0, c).astype(BF)
        send0(c)

    w_mate.wait_recv()
    g_send.wait_recv()
    arrive("re", w_v.at[0, r])
    w_cols = w_v[0, :, :, mine[0]].reshape(2 * rank, rank)
    for n in range(2):
        h_v[n] = mm(g_v[n], w_cols).astype(BF)
    pair_sum = g_v[2, :, pl.ds(0, rank)].astype(F32) + g_v[2, :, pl.ds(rank, rank)].astype(F32)
    gs_v[:, mine[1]] = pair_sum.astype(BF)
    gs_send = share(gs_v.at[:, mine[1]], near, "gs")

    def cross(c):
        z1[c] = send(p1_s.at[c], st1.at[c, mine[1], :], near, f"z{c}")

    gather_q(1)
    for c in range(CHUNKS):
        part = project(1, c) - mm(h_v[0], st0[c, mine[0], :])
        p1f[c] = part
        p1_s[c] = part.astype(BF)
        if c < ZFIRST:
            st1[c, mine[1], :] = part.astype(BF)
        if c < 2:
            cross(c)

    gs_send.wait_recv()
    h_v[2] = mm(gs_v[...], w_v[1, :, :, mine[1]].reshape(2 * rank, rank)).astype(BF)

    gather_q(2)
    spot = 2 * sides[1] + sides[0]
    spots = (3 - spot, flip(spot, 1), flip(spot, 2), spot)
    leaves = (flip(flip(i, 1), 2), flip(i, 1), flip(i, 2))
    odd_team = [{"leaf": leaf, "rhs": 2 * chip + 1} for leaf in leaves]
    odd_keys = [[slot(f"t{w}{h}") for h in range(2)] for w in range(2)]

    def part_of(who, h):
        return 2 * h + lax.div(who, 2), slice(None), span(lax.rem(who, 2), hw)

    for h in range(2):
        for c in (2 * h, 2 * h + 1):
            part = project(2, c) - mm(h_v[1], st0[c, mine[0], :]) - mm(h_v[2], p1_s[c])
            p2f[c] = part
            p2_s[c] = part.astype(BF)
        for n in range(3):
            send(p2_s.at[part_of(spots[n], h)], p2_r.at[core, h, n], odd_team[n], f"t0{h}", extra=2 * core)
        p2o[core, h] = p2f[part_of(spot, h)]

    @pl.when(core == 0)
    def _():
        send(p2o.at[0], p2o.at[0], mate, "tf", keep=False)

    cross(2)
    send1(3)
    arrive("wl", w_v.at[pl.ds(0, 2), r])
    for l in range(3):
        lanes = span(1 - sides[l], rank) if l < 2 else pl.ds(0, 2 * rank)
        share(w_v.at[l, over, :, lanes], mate, "rl")

    def answer_rows(l):
        return w_v[l, pl.ds(pl.multiple_of(sides[l] * 2, 2), 2), :, :].reshape(rank, 2 * rank)


    def first(pair):
        arrive(f"x{pair[0] // 2}", st0.at[pl.ds(pair[0], 2), mine[0], :])
        for c in pair:
            b_v[pl.ds(depth, rank), pl.ds(c * cw, cw)] = (-mm(answer_rows(0), st0[c])).astype(BF)

    def second_sum(c):
        x1[c].wait_recv()
        st1[c, mine[1], :] = (p1f[c] + p1_r[c].astype(F32)).astype(BF)
        z1[c] = share(st1.at[c, mine[1], :], near, f"z{c}")

    def second(c):
        z1[c].wait_recv()
        b_v[pl.ds(depth + rank, rank), pl.ds(c * cw, cw)] = (-mm(answer_rows(1), st1[c])).astype(BF)

    def second_part(c):
        z1[c].wait_recv()
        part = mm(answer_rows(1), st1[c])
        uf[c] = part
        u_s[c] = part.astype(BF)
        u1[c] = send(u_s.at[c], u_r.at[c], sib, f"u{c}")

    def second_join(c):
        u1[c].wait_recv()
        b_v[pl.ds(depth + rank, rank), pl.ds(c * cw, cw)] = (-(uf[c] + u_r[c].astype(F32))).astype(BF)

    where = [(pl.ds(depth + 2 * rank, rank), span(4 * j + spot, hw)) for j in range(2)]
    same_team = [{"leaf": leaf} for leaf in leaves]
    even_team = [{"leaf": leaf, "rhs": flip(r, 1)} for leaf in leaves] + [mate]

    def third_far(w, j):
        total = p2o[w, j]
        arrive(f"t{w}{j}", p2_r.at[w, j])
        for n in range(3):
            total = total + p2_r[w, j, n].astype(F32)
        st2[w, j, mine[2], :] = total.astype(BF)
        ours = st2.at[w, j, mine[2], :]
        send(ours, ours, far, f"f{w}{j}", keep=False)

    def third(w, j):
        arrive(f"f{w}{j}", st2.at[w, j, mine[2], :])
        value = (-mm(answer_rows(2), st2[w, j])).astype(BF)
        if w == 1:
            b_v[where[j]] = value
            for to in same_team:
                send(b_v.at[where[j]], b_v.at[where[j]], to, f"n{j}", keep=False)
        else:
            a2_s[j] = value
            for to in even_team:
                send(a2_s.at[j], b_v.at[where[j]], to, f"n{j}", keep=False)

    def relay_piece(k):
        a_across[k].wait_recv()
        relay[k] = share(a_v.at[span(over, blk), pieces[k]], mate, "rf" if k == final else "r")

    early = SPLIT[final][0] * unit

    def add_pieces():
        for c in range(CHUNKS):
            own = pl.ds(c * cw, cw)
            acc[other_rows, own] = mm(a_v[other_rows, pl.ds(0, early)], b_v[pl.ds(0, early), own])

    def add_last():
        deep = pieces[final]
        for c in range(CHUNKS):
            own = pl.ds(c * cw, cw)
            acc[other_rows, own] = acc[other_rows, own] + mm(a_v[other_rows, deep], b_v[deep, own])

    def finish(c):
        own = pl.ds(c * cw, cw)
        deep = pl.ds(depth, LEVELS * rank)
        out_v[:, own] = (acc[:, own] + mm(a_v[:, deep], b_v[deep, own])).astype(BF)

    arrive("rl", w_v.at[pl.ds(0, 2), r])
    first((0, 1))
    second_part(0)
    second_part(1)
    relay_piece(0)
    relay_piece(1)

    @pl.when(inner == 1)
    def _():
        pl.semaphore_wait(msem, 1)

    @pl.when(core == 1)
    def _():
        arrive("tf", p2o.at[0])
        for j in range(2):
            third_far(1, j)
            third_far(0, j)

    relay_piece(2)
    first((2, 3))
    second_sum(3)
    second_part(2)
    relay_piece(3)

    @pl.when(core == 1)
    def _():
        for j in range(2):
            third(0, j)
            third(1, j)

    second_join(0)
    second_join(1)
    relay_piece(final)
    arrive("r", a_v.at[block, pl.ds(0, early)])
    add_pieces()
    second(3)
    second_join(2)
    relay[final].wait_recv()
    add_last()
    answers = pl.ds(depth + 2 * rank, rank)

    for j in range(2):

        @pl.when(core == 1)
        def _():
            arrive(f"n{j}", b_v.at[answers, pl.ds(0, 3 * hw)])

        @pl.when(core == 0)
        def _():
            arrive(f"n{j}", b_v.at[answers, pl.ds(0, 4 * hw)])

        finish(2 * j)
        finish(2 * j + 1)
    assert len(slots) == RECVS and len(places) == FETCHES, (len(slots), len(places))
    for copy in copies:
        copy.wait_send()

    def sent(ref):
        pltpu.make_async_copy(ref, ref, ssem.at[0]).wait()

    @pl.when(core == 1)
    def _():
        for w in range(2):
            sent(b_v.at[answers, pl.ds(0, CHUNKS * cw)])
        sent(st2.at[0, 0])

    @pl.when(core == 0)
    def _():
        sent(p2o.at[0])


def local(right_sides, leaf_inverse, project_factors, correct_factors, *couplings):
    rows, cols = right_sides.shape
    blk, depth = leaf_inverse.shape
    levels, _, rank = project_factors.shape
    parts = lax.axis_size("rhs")
    cw = cols // CHUNKS
    whole = lambda dtype: pltpu.VMEM((CHUNKS, rank, cw), dtype)
    any_spec = pl.BlockSpec(memory_space=pltpu.HBM)
    return pl.pallas_call(
        kernel,
        out_shape=jax.ShapeDtypeStruct((rows, cols), BF),
        in_specs=[any_spec] * 7,
        out_specs=pl.BlockSpec(memory_space=pltpu.VMEM),
        scratch_shapes=[
            pltpu.VMEM((depth + levels * rank, cols), BF),
            pltpu.VMEM((rows, depth + levels * rank), BF),
            pltpu.VMEM((rows, levels * rank), BF),
            pltpu.VMEM((levels, rank, rows), BF),
            pltpu.VMEM((levels, parts) + couplings[0].shape[1:], BF),
            pltpu.VMEM((3, rank, 2 * rank), BF),
            pltpu.VMEM((rank, 2 * rank), BF),
            pltpu.VMEM((3, rank, rank), BF),
            pltpu.VMEM((levels, rank, depth // 2), F32),
            pltpu.VMEM((levels, rank, depth // 2), BF),
            pltpu.VMEM((levels, rank, depth // 2), BF),
            pltpu.VMEM((levels, 2, rank, depth // 2), BF),
            whole(F32),
            pltpu.VMEM((CHUNKS, 2 * rank, cw), BF),
            whole(F32), whole(BF), whole(BF),
            whole(F32), whole(BF), pltpu.VMEM((2, 2, rank, cw // 2), F32),
            pltpu.VMEM((2, 2, 3, rank, cw // 2), BF),
            pltpu.VMEM((CHUNKS, 2 * rank, cw), BF),
            pltpu.VMEM((2, 2, 2 * rank, cw // 2), BF),
            pltpu.VMEM((2, rank, cw // 2), BF),
            pltpu.VMEM((ZFIRST, rank, cw), F32),
            pltpu.VMEM((ZFIRST, rank, cw), BF),
            pltpu.VMEM((ZFIRST, rank, cw), BF),
            pltpu.VMEM((rows, cols), F32),
            pltpu.SemaphoreType.DMA((FETCHES,)),
            pltpu.SemaphoreType.DMA((1,)),
            pltpu.SemaphoreType.DMA((RECVS,)),
            pltpu.SemaphoreType.REGULAR,
        ],
        compiler_params=pltpu.CompilerParams(
            collective_id=0, has_side_effects=True, vmem_limit_bytes=40 * 1024 * 1024
        ),
    )(*(
        pltpu.with_memory_space_constraint(x, pltpu.HBM)
        for x in (right_sides, leaf_inverse, project_factors, correct_factors, *couplings)
    ))


def solution(mesh):
    in_specs = (
        P("leaf", "rhs"),
        P(("leaf", "rhs"), None),
        P(None, "leaf", None),
        P(None, "leaf", None),
        P(None, "rhs", None),
        P(None, "rhs", None),
        P(None, "rhs", None),
    )
    out_specs = P("leaf", "rhs")
    return jax.shard_map(local, mesh=mesh, in_specs=in_specs, out_specs=out_specs, check_vma=False)
```

```python
import jax
import jax.numpy as jnp
from jax import lax
from jax.experimental import pallas as pl
from jax.experimental.pallas import tpu as pltpu
from jax.sharding import PartitionSpec as P

LEVELS = 3
CHUNKS = 4
SPLIT = ((0, 1), (1, 2), (3, 2), (5, 2), (7, 1))
UNITS = 8
ZFIRST = 3
RECVS = 37
FETCHES = 8
BF = jnp.bfloat16
F32 = jnp.float32


def mm(a, b):
    return jnp.dot(a, b, preferred_element_type=F32)


def bit_of(index, stride):
    return lax.rem(lax.div(index, stride), 2)


def flip(index, stride):
    return index + stride * (1 - 2 * bit_of(index, stride))


def span(which, size):
    return pl.ds(pl.multiple_of(which * size, size), size)


def kernel(
    b_hbm, a_hbm, p_hbm, c_hbm, w0_hbm, w1_hbm, w2_hbm, out_v,
    b_v, a_v, p_v, pt_v, w_v, g_v, gs_v, h_v, qf, q_s, q_r, q_v,
    pf, st0, p1f, p1_s, p1_r, p2f, p2_s, p2o, p2_r, st1, st2, a2_s, uf, u_s, u_r, acc,
    lsem, ssem, rsem, msem,
):
    i = lax.axis_index("leaf")
    r = lax.axis_index("rhs")
    blk = a_hbm.shape[0]
    depth = a_hbm.shape[1]
    cols = b_hbm.shape[1]
    rank = p_hbm.shape[2]
    cw = cols // CHUNKS
    hw = cw // 2
    half = depth // 2
    unit = depth // UNITS
    pieces = [pl.ds(at * unit, size * unit) for at, size in SPLIT]
    final = len(SPLIT) - 1
    mate = {"rhs": flip(r, 1)}
    across = {"rhs": flip(r, 2)}
    sib = {"leaf": flip(i, 1)}
    near = {"leaf": flip(i, 2)}
    far = {"leaf": flip(i, 4)}
    mid = {"leaf": flip(flip(i, 2), 4)}
    sides = [bit_of(i, 1), bit_of(i, 2), bit_of(i, 4)]
    core = bit_of(r, 1)
    chip = bit_of(r, 2)

    copies = []
    slots = {}

    def slot(key):
        return slots.setdefault(key, len(slots))

    def send(src, dst, to, key, extra=None, keep=True):
        place = slot(key) if extra is None else slot(key) + extra
        copy = pltpu.make_async_remote_copy(
            src_ref=src, dst_ref=dst, send_sem=ssem.at[0], recv_sem=rsem.at[place],
            device_id=to, device_id_type=pl.DeviceIdType.MESH,
        )
        copy.start()
        if keep:
            copies.append(copy)
        return copy

    def arrive(key, ref):
        pltpu.make_async_copy(ref, ref, rsem.at[slot(key)]).wait()

    def fetched(key, ref):
        pltpu.make_async_copy(ref, ref, lsem.at[places[key]]).wait()

    def share(ref, to, key):
        return send(ref, ref, to, key)

    places = {}

    def fetch(src, dst, key):
        copy = pltpu.make_async_copy(src, dst, lsem.at[places.setdefault(key, len(places))])
        copy.start()
        return copy

    mine = [span(s, rank) for s in sides]
    block = span(r, blk)
    pair_rows = span(chip, 2 * blk)
    other_rows = span(1 - chip, 2 * blk)
    half_cols = span(core, half)
    rest_cols = span(1 - core, half)

    la = fetch(a_hbm.at[:, rest_cols], a_v.at[block, rest_cols], "a")
    lo = fetch(a_hbm.at[:, half_cols], a_v.at[block, half_cols], "o")
    lp = [fetch(p_hbm.at[0], p_v.at[:, pl.ds(0, rank)], "p0")]
    [
        fetch(w_hbm.at[lax.div(i, 2 << level)], w_v.at[level, r], "w")
        for level, w_hbm in enumerate((w0_hbm, w1_hbm, w2_hbm))
    ]
    lp += [fetch(p_hbm.at[l], p_v.at[:, pl.ds(l * rank, rank)], f"p{l}") for l in range(1, LEVELS)]
    [fetch(c_hbm.at[l], a_v.at[:, pl.ds(depth + l * rank, rank)], "c") for l in range(LEVELS)]
    lb = fetch(b_hbm, b_v.at[pl.ds(0, depth)], "b")

    barrier = pltpu.get_barrier_semaphore()
    inner = lax.rem(sides[1] + sides[2], 2)
    for to in (mate, across, sib, near):
        pl.semaphore_signal(barrier, inc=1, device_id=to, device_id_type=pl.DeviceIdType.MESH)

    @pl.when(inner == 1)
    def _():
        pl.semaphore_signal(barrier, inc=1, device_id=mid, device_id_type=pl.DeviceIdType.MESH)

    la.wait()
    pl.semaphore_wait(barrier, 4 + inner)

    @pl.when(inner == 1)
    def _():
        pl.semaphore_signal(msem, inc=1, device_id=mid, device_id_type=pl.DeviceIdType.MESH)


    a_mate = share(a_v.at[block, rest_cols], mate, "am")
    lo.wait()
    a_across = [share(a_v.at[block, pieces[0]], across, "a1")]
    fetched("w", w_v.at[:, r])
    [share(w_v.at[l, r, :, mine[l]], across, "we") for l in range(2)]
    lp[0].wait()
    pt_v[0] = p_v[:, pl.ds(0, rank)].T
    a_mate.wait_recv()
    q_across = []
    for l in range(LEVELS):
        if l > 0:
            lp[l].wait()
            pt_v[l] = p_v[:, pl.ds(l * rank, rank)].T
        part = mm(pt_v[l, :, pair_rows], a_v[pair_rows, half_cols])
        qf[l] = part
        q_s[l] = part.astype(BF)
        q_across.append(send(q_s.at[l], q_r.at[l], across, f"q{l}"))
    a_mate2 = share(a_v.at[block, half_cols], mate, "an")
    w_mate = share(w_v.at[:, r], mate, "wg")
    [share(w_v.at[l, r, :, span(1 - sides[l], rank)], across, "wl") for l in range(2)]
    share(w_v.at[2, r], across, "wl")
    for k in range(1, len(SPLIT)):
        a_across.append(share(a_v.at[block, pieces[k]], across, f"a{k}"))

    fetched("c", a_v.at[:, pl.ds(depth, LEVELS * rank)])
    for n, (l, k) in enumerate(((1, 0), (2, 0), (2, 1))):
        g_v[n, :, mine[0]] = mm(pt_v[l], a_v[:, pl.ds(depth + k * rank, rank)]).astype(BF)
    g_send = share(g_v.at[:, :, mine[0]], sib, "wg")

    over = flip(r, 2)
    arrive("we", w_v.at[0, r])
    for l in range(2):
        share(w_v.at[l, over, :, mine[l]], mate, "re")
    lb.wait()
    a_mate2.wait_recv()
    for c in range(CHUNKS):
        own = pl.ds(c * cw, cw)
        acc[pair_rows, own] = mm(a_v[pair_rows, pl.ds(0, depth)], b_v[pl.ds(0, depth), own])

    def gather_q(l):
        q_across[l].wait_recv()
        q_v[l, core] = (qf[l] + q_r[l].astype(F32)).astype(BF)
        relayed = share(q_v.at[l, core], mate, f"m{l}")
        for c in range(CHUNKS):
            pf[c] = mm(q_v[l, core], b_v[half_cols, pl.ds(c * cw, cw)])
        relayed.wait_recv()

    def project(l, c):
        return pf[c] + mm(q_v[l, 1 - core], b_v[rest_cols, span(c, cw)])

    x1, z1, f1, u1, relay = {}, {}, {}, {}, {}

    def send0(c):
        share(st0.at[c, mine[0], :], sib, f"x{c // 2}")

    def send1(c):
        x1[c] = send(p1_s.at[c], p1_r.at[c], sib, f"y{c}")

    gather_q(0)
    for c in range(CHUNKS):
        st0[c, mine[0], :] = project(0, c).astype(BF)
        send0(c)

    both = (LEVELS * w0_hbm.shape[1] * w0_hbm.shape[2] + 3 * rank * rank) // cols
    arrive("wg", b_v.at[pl.ds(0, both)])
    arrive("re", w_v.at[0, r])
    w_cols = w_v[0, :, :, mine[0]].reshape(2 * rank, rank)
    for n in range(2):
        h_v[n] = mm(g_v[n], w_cols).astype(BF)
    pair_sum = g_v[2, :, pl.ds(0, rank)].astype(F32) + g_v[2, :, pl.ds(rank, rank)].astype(F32)
    gs_v[:, mine[1]] = pair_sum.astype(BF)
    gs_send = share(gs_v.at[:, mine[1]], near, "gs")

    def cross(c):
        z1[c] = send(p1_s.at[c], st1.at[c, mine[1], :], near, f"z{max(c, 1)}")

    gather_q(1)
    for c in range(CHUNKS):
        part = project(1, c) - mm(h_v[0], st0[c, mine[0], :])
        p1f[c] = part
        p1_s[c] = part.astype(BF)
        if c < ZFIRST:
            st1[c, mine[1], :] = part.astype(BF)
        if c < 2:
            cross(c)

    gs_send.wait_recv()
    h_v[2] = mm(gs_v[...], w_v[1, :, :, mine[1]].reshape(2 * rank, rank)).astype(BF)

    gather_q(2)
    spot = 2 * sides[1] + sides[0]
    spots = (3 - spot, flip(spot, 1), flip(spot, 2), spot)
    leaves = (flip(flip(i, 1), 2), flip(i, 1), flip(i, 2))
    odd_team = [{"leaf": leaf, "rhs": 2 * chip + 1} for leaf in leaves]
    odd_keys = [[slot(f"t{w}{h}") for h in range(2)] for w in range(2)]

    def part_of(who, h):
        return 2 * h + lax.div(who, 2), slice(None), span(lax.rem(who, 2), hw)

    for h in range(2):
        for c in (2 * h, 2 * h + 1):
            part = project(2, c) - mm(h_v[1], st0[c, mine[0], :]) - mm(h_v[2], p1_s[c])
            p2f[c] = part
            p2_s[c] = part.astype(BF)
        for n in range(3):
            send(p2_s.at[part_of(spots[n], h)], p2_r.at[core, h, n], odd_team[n], f"t0{h}", extra=2 * core)
        p2o[core, h] = p2f[part_of(spot, h)]

    @pl.when(core == 0)
    def _():
        send(p2o.at[0], p2o.at[0], mate, "tf", keep=False)

    cross(2)
    send1(3)
    arrive("wl", w_v.at[pl.ds(0, 2), r])
    for l in range(3):
        lanes = span(1 - sides[l], rank) if l < 2 else pl.ds(0, 2 * rank)
        share(w_v.at[l, over, :, lanes], mate, "rl")

    def answer_rows(l):
        return w_v[l, pl.ds(pl.multiple_of(sides[l] * 2, 2), 2), :, :].reshape(rank, 2 * rank)


    def first(pair):
        arrive(f"x{pair[0] // 2}", st0.at[pl.ds(pair[0], 2), mine[0], :])
        for c in pair:
            b_v[pl.ds(depth, rank), pl.ds(c * cw, cw)] = (-mm(answer_rows(0), st0[c])).astype(BF)

    def second_sum(c):
        x1[c].wait_recv()
        st1[c, mine[1], :] = (p1f[c] + p1_r[c].astype(F32)).astype(BF)
        z1[c] = share(st1.at[c, mine[1], :], near, f"z{c}")

    def second(c):
        z1[c].wait_recv()
        b_v[pl.ds(depth + rank, rank), pl.ds(c * cw, cw)] = (-mm(answer_rows(1), st1[c])).astype(BF)

    def second_part(c):
        if c == 0:
            arrive("z1", st1.at[pl.ds(0, 2), mine[1], :])
        elif c > 1:
            z1[c].wait_recv()
        part = mm(answer_rows(1), st1[c])
        uf[c] = part
        u_s[c] = part.astype(BF)
        u1[c] = send(u_s.at[c], u_r.at[c], sib, f"u{max(c, 1)}")

    def second_join(c):
        if c == 0:
            arrive("u1", u_r.at[pl.ds(0, 2)])
        elif c > 1:
            u1[c].wait_recv()
        b_v[pl.ds(depth + rank, rank), pl.ds(c * cw, cw)] = (-(uf[c] + u_r[c].astype(F32))).astype(BF)

    where = [(pl.ds(depth + 2 * rank, rank), span(4 * j + spot, hw)) for j in range(2)]
    same_team = [{"leaf": leaf} for leaf in leaves]
    even_team = [{"leaf": leaf, "rhs": flip(r, 1)} for leaf in leaves] + [mate]

    def third_far(w, j):
        total = p2o[w, j]
        arrive(f"t{w}{j}", p2_r.at[w, j])
        for n in range(3):
            total = total + p2_r[w, j, n].astype(F32)
        st2[w, j, mine[2], :] = total.astype(BF)
        ours = st2.at[w, j, mine[2], :]
        send(ours, ours, far, f"f{j}", keep=False)

    def third(w, j):
        if w == 0:
            arrive(f"f{j}", st2.at[:, j, mine[2], :])
        value = (-mm(answer_rows(2), st2[w, j])).astype(BF)
        if w == 1:
            b_v[where[j]] = value
            for to in same_team:
                send(b_v.at[where[j]], b_v.at[where[j]], to, f"n{j}", keep=False)
        else:
            a2_s[j] = value
            for to in even_team:
                send(a2_s.at[j], b_v.at[where[j]], to, f"n{j}", keep=False)

    def relay_piece(k):
        if k == 1:
            arrive("a1", a_v.at[block, pl.ds(0, SPLIT[2][0] * unit)])
        elif k > 1:
            a_across[k].wait_recv()
        relay[k] = share(a_v.at[span(over, blk), pieces[k]], mate, "rf" if k == final else "r")

    early = SPLIT[final][0] * unit

    def add_pieces():
        for c in range(CHUNKS):
            own = pl.ds(c * cw, cw)
            acc[other_rows, own] = mm(a_v[other_rows, pl.ds(0, early)], b_v[pl.ds(0, early), own])

    def add_last():
        deep = pieces[final]
        for c in range(CHUNKS):
            own = pl.ds(c * cw, cw)
            acc[other_rows, own] = acc[other_rows, own] + mm(a_v[other_rows, deep], b_v[deep, own])

    def finish(c):
        own = pl.ds(c * cw, cw)
        deep = pl.ds(depth, LEVELS * rank)
        out_v[:, own] = (acc[:, own] + mm(a_v[:, deep], b_v[deep, own])).astype(BF)

    arrive("rl", w_v.at[pl.ds(0, 2), r])
    first((0, 1))
    second_part(0)
    second_part(1)
    relay_piece(1)
    relay_piece(0)

    @pl.when(inner == 1)
    def _():
        pl.semaphore_wait(msem, 1)

    @pl.when(core == 1)
    def _():
        arrive("tf", p2o.at[0])
        for j in range(2):
            third_far(1, j)
            third_far(0, j)

    relay_piece(2)
    first((2, 3))
    second_sum(3)
    second_part(2)
    relay_piece(3)

    @pl.when(core == 1)
    def _():
        for j in range(2):
            third(0, j)
            third(1, j)

    second_join(0)
    second_join(1)
    relay_piece(final)
    arrive("r", a_v.at[block, pl.ds(0, early)])
    add_pieces()
    second(3)
    second_join(2)
    relay[final].wait_recv()
    add_last()
    answers = pl.ds(depth + 2 * rank, rank)

    for j in range(2):

        @pl.when(core == 1)
        def _():
            arrive(f"n{j}", b_v.at[answers, pl.ds(0, 3 * hw)])

        @pl.when(core == 0)
        def _():
            arrive(f"n{j}", b_v.at[answers, pl.ds(0, 4 * hw)])

        finish(2 * j)
        finish(2 * j + 1)
    assert len(slots) == RECVS and len(places) == FETCHES, (len(slots), len(places))
    for copy in copies:
        copy.wait_send()

    def sent(ref):
        pltpu.make_async_copy(ref, ref, ssem.at[0]).wait()

    @pl.when(core == 1)
    def _():
        for w in range(2):
            sent(b_v.at[answers, pl.ds(0, CHUNKS * cw)])
        sent(st2.at[0, 0])

    @pl.when(core == 0)
    def _():
        sent(p2o.at[0])


def local(right_sides, leaf_inverse, project_factors, correct_factors, *couplings):
    rows, cols = right_sides.shape
    blk, depth = leaf_inverse.shape
    levels, _, rank = project_factors.shape
    parts = lax.axis_size("rhs")
    cw = cols // CHUNKS
    whole = lambda dtype: pltpu.VMEM((CHUNKS, rank, cw), dtype)
    any_spec = pl.BlockSpec(memory_space=pltpu.HBM)
    return pl.pallas_call(
        kernel,
        out_shape=jax.ShapeDtypeStruct((rows, cols), BF),
        in_specs=[any_spec] * 7,
        out_specs=pl.BlockSpec(memory_space=pltpu.VMEM),
        scratch_shapes=[
            pltpu.VMEM((depth + levels * rank, cols), BF),
            pltpu.VMEM((rows, depth + levels * rank), BF),
            pltpu.VMEM((rows, levels * rank), BF),
            pltpu.VMEM((levels, rank, rows), BF),
            pltpu.VMEM((levels, parts) + couplings[0].shape[1:], BF),
            pltpu.VMEM((3, rank, 2 * rank), BF),
            pltpu.VMEM((rank, 2 * rank), BF),
            pltpu.VMEM((3, rank, rank), BF),
            pltpu.VMEM((levels, rank, depth // 2), F32),
            pltpu.VMEM((levels, rank, depth // 2), BF),
            pltpu.VMEM((levels, rank, depth // 2), BF),
            pltpu.VMEM((levels, 2, rank, depth // 2), BF),
            whole(F32),
            pltpu.VMEM((CHUNKS, 2 * rank, cw), BF),
            whole(F32), whole(BF), whole(BF),
            whole(F32), whole(BF), pltpu.VMEM((2, 2, rank, cw // 2), F32),
            pltpu.VMEM((2, 2, 3, rank, cw // 2), BF),
            pltpu.VMEM((CHUNKS, 2 * rank, cw), BF),
            pltpu.VMEM((2, 2, 2 * rank, cw // 2), BF),
            pltpu.VMEM((2, rank, cw // 2), BF),
            pltpu.VMEM((ZFIRST, rank, cw), F32),
            pltpu.VMEM((ZFIRST, rank, cw), BF),
            pltpu.VMEM((ZFIRST, rank, cw), BF),
            pltpu.VMEM((rows, cols), F32),
            pltpu.SemaphoreType.DMA((FETCHES,)),
            pltpu.SemaphoreType.DMA((1,)),
            pltpu.SemaphoreType.DMA((RECVS,)),
            pltpu.SemaphoreType.REGULAR,
        ],
        compiler_params=pltpu.CompilerParams(
            collective_id=0, has_side_effects=True, vmem_limit_bytes=40 * 1024 * 1024
        ),
    )(*(
        pltpu.with_memory_space_constraint(x, pltpu.HBM)
        for x in (right_sides, leaf_inverse, project_factors, correct_factors, *couplings)
    ))


def solution(mesh):
    in_specs = (
        P("leaf", "rhs"),
        P(("leaf", "rhs"), None),
        P(None, "leaf", None),
        P(None, "leaf", None),
        P(None, "rhs", None),
        P(None, "rhs", None),
        P(None, "rhs", None),
    )
    out_specs = P("leaf", "rhs")
    return jax.shard_map(local, mesh=mesh, in_specs=in_specs, out_specs=out_specs, check_vma=False)
```

```python
import jax
import jax.numpy as jnp
from jax import lax
from jax.experimental import pallas as pl
from jax.experimental.pallas import tpu as pltpu
from jax.sharding import PartitionSpec as P

LEVELS = 3
CHUNKS = 4
SPLIT = ((0, 1), (1, 2), (3, 2), (5, 2), (7, 1))
UNITS = 8
ZFIRST = 3
RECVS = 37
FETCHES = 8
BF = jnp.bfloat16
F32 = jnp.float32


def mm(a, b):
    return jnp.dot(a, b, preferred_element_type=F32)


def bit_of(index, stride):
    return lax.rem(lax.div(index, stride), 2)


def flip(index, stride):
    return index + stride * (1 - 2 * bit_of(index, stride))


def span(which, size):
    return pl.ds(pl.multiple_of(which * size, size), size)


def kernel(
    b_hbm, a_hbm, p_hbm, c_hbm, w0_hbm, w1_hbm, w2_hbm, out_v,
    b_v, a_v, p_v, pt_v, w_v, g_v, gs_v, h_v, qf, q_s, q_r, q_v,
    pf, st0, p1f, p1_s, p1_r, p2f, p2_s, p2o, p2_r, st1, st2, a2_s, uf, u_s, u_r, acc,
    lsem, ssem, rsem, msem,
):
    i = lax.axis_index("leaf")
    r = lax.axis_index("rhs")
    blk = a_hbm.shape[0]
    depth = a_hbm.shape[1]
    cols = b_hbm.shape[1]
    rank = p_hbm.shape[2]
    cw = cols // CHUNKS
    hw = cw // 2
    half = depth // 2
    unit = depth // UNITS
    pieces = [pl.ds(at * unit, size * unit) for at, size in SPLIT]
    final = len(SPLIT) - 1
    mate = {"rhs": flip(r, 1)}
    across = {"rhs": flip(r, 2)}
    sib = {"leaf": flip(i, 1)}
    near = {"leaf": flip(i, 2)}
    far = {"leaf": flip(i, 4)}
    mid = {"leaf": flip(flip(i, 2), 4)}
    sides = [bit_of(i, 1), bit_of(i, 2), bit_of(i, 4)]
    core = bit_of(r, 1)
    chip = bit_of(r, 2)

    copies = []
    slots = {}

    def slot(key):
        return slots.setdefault(key, len(slots))

    def send(src, dst, to, key, extra=None, keep=True):
        place = slot(key) if extra is None else slot(key) + extra
        copy = pltpu.make_async_remote_copy(
            src_ref=src, dst_ref=dst, send_sem=ssem.at[0], recv_sem=rsem.at[place],
            device_id=to, device_id_type=pl.DeviceIdType.MESH,
        )
        copy.start()
        if keep:
            copies.append(copy)
        return copy

    def arrive(key, ref):
        pltpu.make_async_copy(ref, ref, rsem.at[slot(key)]).wait()

    def fetched(key, ref):
        pltpu.make_async_copy(ref, ref, lsem.at[places[key]]).wait()

    def share(ref, to, key):
        return send(ref, ref, to, key)

    places = {}

    def fetch(src, dst, key):
        copy = pltpu.make_async_copy(src, dst, lsem.at[places.setdefault(key, len(places))])
        copy.start()
        return copy

    mine = [span(s, rank) for s in sides]
    block = span(r, blk)
    pair_rows = span(chip, 2 * blk)
    other_rows = span(1 - chip, 2 * blk)
    half_cols = span(core, half)
    rest_cols = span(1 - core, half)

    la = fetch(a_hbm.at[:, rest_cols], a_v.at[block, rest_cols], "a")
    lo = fetch(a_hbm.at[:, half_cols], a_v.at[block, half_cols], "o")
    lp = [fetch(p_hbm.at[0], p_v.at[:, pl.ds(0, rank)], "p0")]
    [
        fetch(w_hbm.at[lax.div(i, 2 << level)], w_v.at[level, r], "w")
        for level, w_hbm in enumerate((w0_hbm, w1_hbm, w2_hbm))
    ]
    lp += [fetch(p_hbm.at[l], p_v.at[:, pl.ds(l * rank, rank)], f"p{l}") for l in range(1, LEVELS)]
    [fetch(c_hbm.at[l], a_v.at[:, pl.ds(depth + l * rank, rank)], "c") for l in range(LEVELS)]
    lb = fetch(b_hbm, b_v.at[pl.ds(0, depth)], "b")

    barrier = pltpu.get_barrier_semaphore()
    inner = lax.rem(sides[1] + sides[2], 2)
    for to in (mate, across, sib, near):
        pl.semaphore_signal(barrier, inc=1, device_id=to, device_id_type=pl.DeviceIdType.MESH)

    @pl.when(inner == 1)
    def _():
        pl.semaphore_signal(barrier, inc=1, device_id=mid, device_id_type=pl.DeviceIdType.MESH)

    la.wait()
    pl.semaphore_wait(barrier, 4 + inner)

    @pl.when(inner == 1)
    def _():
        pl.semaphore_signal(msem, inc=1, device_id=mid, device_id_type=pl.DeviceIdType.MESH)


    a_mate = share(a_v.at[block, rest_cols], mate, "am")
    lo.wait()
    a_across = [share(a_v.at[block, pieces[0]], across, "a1")]
    fetched("w", w_v.at[:, r])
    [share(w_v.at[l, r, :, mine[l]], across, "we") for l in range(2)]
    lp[0].wait()
    pt_v[0] = p_v[:, pl.ds(0, rank)].T
    a_mate.wait_recv()
    q_across = []
    for l in range(LEVELS):
        if l > 0:
            lp[l].wait()
            pt_v[l] = p_v[:, pl.ds(l * rank, rank)].T
        part = mm(pt_v[l, :, pair_rows], a_v[pair_rows, half_cols])
        qf[l] = part
        q_s[l] = part.astype(BF)
        q_across.append(send(q_s.at[l], q_r.at[l], across, f"q{l}"))
    a_mate2 = share(a_v.at[block, half_cols], mate, "an")
    w_mate = share(w_v.at[:, r], mate, "wg")
    [share(w_v.at[l, r, :, span(1 - sides[l], rank)], across, "wl") for l in range(2)]
    share(w_v.at[2, r], across, "wl")
    for k in range(1, len(SPLIT)):
        a_across.append(share(a_v.at[block, pieces[k]], across, f"a{k}"))

    fetched("c", a_v.at[:, pl.ds(depth, LEVELS * rank)])
    for n, (l, k) in enumerate(((1, 0), (2, 0), (2, 1))):
        g_v[n, :, mine[0]] = mm(pt_v[l], a_v[:, pl.ds(depth + k * rank, rank)]).astype(BF)
    g_send = share(g_v.at[:, :, mine[0]], sib, "wg")

    over = flip(r, 2)
    arrive("we", w_v.at[0, r])
    for l in range(2):
        share(w_v.at[l, over, :, mine[l]], mate, "re")
    lb.wait()
    a_mate2.wait_recv()
    for c in range(CHUNKS):
        own = pl.ds(c * cw, cw)
        acc[pair_rows, own] = mm(a_v[pair_rows, pl.ds(0, depth)], b_v[pl.ds(0, depth), own])

    def gather_q(l):
        q_across[l].wait_recv()
        q_v[l, core] = (qf[l] + q_r[l].astype(F32)).astype(BF)
        relayed = share(q_v.at[l, core], mate, f"m{l}")
        for c in range(CHUNKS):
            pf[c] = mm(q_v[l, core], b_v[half_cols, pl.ds(c * cw, cw)])
        relayed.wait_recv()

    def project(l, c):
        return pf[c] + mm(q_v[l, 1 - core], b_v[rest_cols, span(c, cw)])

    x1, z1, f1, u1, relay = {}, {}, {}, {}, {}

    def send0(c):
        share(st0.at[c, mine[0], :], sib, f"x{c // 2}")

    def send1(c):
        x1[c] = send(p1_s.at[c], p1_r.at[c], sib, f"y{c}")

    gather_q(0)
    for c in range(CHUNKS):
        st0[c, mine[0], :] = project(0, c).astype(BF)
        if c < CHUNKS - 1:
            send0(c)

    both = (LEVELS * w0_hbm.shape[1] * w0_hbm.shape[2] + 3 * rank * rank) // cols
    arrive("wg", b_v.at[pl.ds(0, both)])
    arrive("re", w_v.at[0, r])
    w_cols = w_v[0, :, :, mine[0]].reshape(2 * rank, rank)
    for n in range(2):
        h_v[n] = mm(g_v[n], w_cols).astype(BF)
    pair_sum = g_v[2, :, pl.ds(0, rank)].astype(F32) + g_v[2, :, pl.ds(rank, rank)].astype(F32)
    gs_v[:, mine[1]] = pair_sum.astype(BF)
    gs_send = share(gs_v.at[:, mine[1]], near, "gs")

    def cross(c):
        z1[c] = send(p1_s.at[c], st1.at[c, mine[1], :], near, f"z{max(c, 1)}")

    gather_q(1)
    for c in range(CHUNKS):
        part = project(1, c) - mm(h_v[0], st0[c, mine[0], :])
        p1f[c] = part
        p1_s[c] = part.astype(BF)
        if c < ZFIRST:
            st1[c, mine[1], :] = part.astype(BF)
        if c < 2:
            cross(c)
        if c == 3:
            send1(c)

    gs_send.wait_recv()
    h_v[2] = mm(gs_v[...], w_v[1, :, :, mine[1]].reshape(2 * rank, rank)).astype(BF)

    gather_q(2)
    spot = 2 * sides[1] + sides[0]
    spots = (3 - spot, flip(spot, 1), flip(spot, 2), spot)
    leaves = (flip(flip(i, 1), 2), flip(i, 1), flip(i, 2))
    odd_team = [{"leaf": leaf, "rhs": 2 * chip + 1} for leaf in leaves]
    odd_keys = [[slot(f"t{w}{h}") for h in range(2)] for w in range(2)]

    def part_of(who, h):
        return 2 * h + lax.div(who, 2), slice(None), span(lax.rem(who, 2), hw)

    for h in range(2):
        for c in (2 * h, 2 * h + 1):
            part = project(2, c) - mm(h_v[1], st0[c, mine[0], :]) - mm(h_v[2], p1_s[c])
            p2f[c] = part
            p2_s[c] = part.astype(BF)
        for n in range(3):
            send(p2_s.at[part_of(spots[n], h)], p2_r.at[core, h, n], odd_team[n], f"t0{h}", extra=2 * core)
        p2o[core, h] = p2f[part_of(spot, h)]

    @pl.when(core == 0)
    def _():
        send(p2o.at[0], p2o.at[0], mate, "tf", keep=False)

    cross(2)
    send0(CHUNKS - 1)
    arrive("wl", w_v.at[pl.ds(0, 2), r])
    for l in range(3):
        lanes = span(1 - sides[l], rank) if l < 2 else pl.ds(0, 2 * rank)
        share(w_v.at[l, over, :, lanes], mate, "rl")

    def answer_rows(l):
        return w_v[l, pl.ds(pl.multiple_of(sides[l] * 2, 2), 2), :, :].reshape(rank, 2 * rank)


    def first(pair):
        arrive(f"x{pair[0] // 2}", st0.at[pl.ds(pair[0], 2), mine[0], :])
        for c in pair:
            b_v[pl.ds(depth, rank), pl.ds(c * cw, cw)] = (-mm(answer_rows(0), st0[c])).astype(BF)

    def second_sum(c):
        x1[c].wait_recv()
        st1[c, mine[1], :] = (p1f[c] + p1_r[c].astype(F32)).astype(BF)
        z1[c] = share(st1.at[c, mine[1], :], near, f"z{c}")

    def second(c):
        z1[c].wait_recv()
        b_v[pl.ds(depth + rank, rank), pl.ds(c * cw, cw)] = (-mm(answer_rows(1), st1[c])).astype(BF)

    def second_part(c):
        if c == 0:
            arrive("z1", st1.at[pl.ds(0, 2), mine[1], :])
        elif c > 1:
            z1[c].wait_recv()
        part = mm(answer_rows(1), st1[c])
        uf[c] = part
        u_s[c] = part.astype(BF)
        u1[c] = send(u_s.at[c], u_r.at[c], sib, f"u{max(c, 1)}")

    def second_join(c):
        if c == 0:
            arrive("u1", u_r.at[pl.ds(0, 2)])
        elif c > 1:
            u1[c].wait_recv()
        b_v[pl.ds(depth + rank, rank), pl.ds(c * cw, cw)] = (-(uf[c] + u_r[c].astype(F32))).astype(BF)

    where = [(pl.ds(depth + 2 * rank, rank), span(4 * j + spot, hw)) for j in range(2)]
    same_team = [{"leaf": leaf} for leaf in leaves]
    even_team = [{"leaf": leaf, "rhs": flip(r, 1)} for leaf in leaves] + [mate]

    def third_far(w, j):
        total = p2o[w, j]
        arrive(f"t{w}{j}", p2_r.at[w, j])
        for n in range(3):
            total = total + p2_r[w, j, n].astype(F32)
        st2[w, j, mine[2], :] = total.astype(BF)
        ours = st2.at[w, j, mine[2], :]
        send(ours, ours, far, f"f{j}", keep=False)

    def third(w, j):
        if w == 0:
            arrive(f"f{j}", st2.at[:, j, mine[2], :])
        value = (-mm(answer_rows(2), st2[w, j])).astype(BF)
        if w == 1:
            b_v[where[j]] = value
            for to in same_team:
                send(b_v.at[where[j]], b_v.at[where[j]], to, f"n{j}", keep=False)
        else:
            a2_s[j] = value
            for to in even_team:
                send(a2_s.at[j], b_v.at[where[j]], to, f"n{j}", keep=False)

    def relay_piece(k):
        if k == 1:
            arrive("a1", a_v.at[block, pl.ds(0, SPLIT[2][0] * unit)])
        elif k > 1:
            a_across[k].wait_recv()
        relay[k] = share(a_v.at[span(over, blk), pieces[k]], mate, "rf" if k == final else "r")

    early = SPLIT[final][0] * unit

    def add_pieces():
        for c in range(CHUNKS):
            own = pl.ds(c * cw, cw)
            acc[other_rows, own] = mm(a_v[other_rows, pl.ds(0, early)], b_v[pl.ds(0, early), own])

    def add_last():
        deep = pieces[final]
        for c in range(CHUNKS):
            own = pl.ds(c * cw, cw)
            acc[other_rows, own] = acc[other_rows, own] + mm(a_v[other_rows, deep], b_v[deep, own])

    def finish(c):
        own = pl.ds(c * cw, cw)
        deep = pl.ds(depth, LEVELS * rank)
        out_v[:, own] = (acc[:, own] + mm(a_v[:, deep], b_v[deep, own])).astype(BF)

    arrive("rl", w_v.at[pl.ds(0, 2), r])
    first((0, 1))
    second_part(0)
    second_part(1)
    relay_piece(1)
    relay_piece(0)

    @pl.when(inner == 1)
    def _():
        pl.semaphore_wait(msem, 1)

    @pl.when(core == 1)
    def _():
        arrive("tf", p2o.at[0])
        for j in range(2):
            third_far(1, j)
            third_far(0, j)

    relay_piece(2)
    second_part(2)
    second_sum(3)
    first((2, 3))
    relay_piece(3)

    @pl.when(core == 1)
    def _():
        for j in range(2):
            third(0, j)
            third(1, j)

    second_join(0)
    second_join(1)
    relay_piece(final)
    arrive("r", a_v.at[block, pl.ds(0, early)])
    add_pieces()
    second(3)
    second_join(2)
    relay[final].wait_recv()
    add_last()
    answers = pl.ds(depth + 2 * rank, rank)

    for j in range(2):

        @pl.when(core == 1)
        def _():
            arrive(f"n{j}", b_v.at[answers, pl.ds(0, 3 * hw)])

        @pl.when(core == 0)
        def _():
            arrive(f"n{j}", b_v.at[answers, pl.ds(0, 4 * hw)])

        finish(2 * j)
        finish(2 * j + 1)
    assert len(slots) == RECVS and len(places) == FETCHES, (len(slots), len(places))
    for copy in copies:
        copy.wait_send()

    def sent(ref):
        pltpu.make_async_copy(ref, ref, ssem.at[0]).wait()

    @pl.when(core == 1)
    def _():
        for w in range(2):
            sent(b_v.at[answers, pl.ds(0, CHUNKS * cw)])
        sent(st2.at[0, 0])

    @pl.when(core == 0)
    def _():
        sent(p2o.at[0])


def local(right_sides, leaf_inverse, project_factors, correct_factors, *couplings):
    rows, cols = right_sides.shape
    blk, depth = leaf_inverse.shape
    levels, _, rank = project_factors.shape
    parts = lax.axis_size("rhs")
    cw = cols // CHUNKS
    whole = lambda dtype: pltpu.VMEM((CHUNKS, rank, cw), dtype)
    any_spec = pl.BlockSpec(memory_space=pltpu.HBM)
    return pl.pallas_call(
        kernel,
        out_shape=jax.ShapeDtypeStruct((rows, cols), BF),
        in_specs=[any_spec] * 7,
        out_specs=pl.BlockSpec(memory_space=pltpu.VMEM),
        scratch_shapes=[
            pltpu.VMEM((depth + levels * rank, cols), BF),
            pltpu.VMEM((rows, depth + levels * rank), BF),
            pltpu.VMEM((rows, levels * rank), BF),
            pltpu.VMEM((levels, rank, rows), BF),
            pltpu.VMEM((levels, parts) + couplings[0].shape[1:], BF),
            pltpu.VMEM((3, rank, 2 * rank), BF),
            pltpu.VMEM((rank, 2 * rank), BF),
            pltpu.VMEM((3, rank, rank), BF),
            pltpu.VMEM((levels, rank, depth // 2), F32),
            pltpu.VMEM((levels, rank, depth // 2), BF),
            pltpu.VMEM((levels, rank, depth // 2), BF),
            pltpu.VMEM((levels, 2, rank, depth // 2), BF),
            whole(F32),
            pltpu.VMEM((CHUNKS, 2 * rank, cw), BF),
            whole(F32), whole(BF), whole(BF),
            whole(F32), whole(BF), pltpu.VMEM((2, 2, rank, cw // 2), F32),
            pltpu.VMEM((2, 2, 3, rank, cw // 2), BF),
            pltpu.VMEM((CHUNKS, 2 * rank, cw), BF),
            pltpu.VMEM((2, 2, 2 * rank, cw // 2), BF),
            pltpu.VMEM((2, rank, cw // 2), BF),
            pltpu.VMEM((ZFIRST, rank, cw), F32),
            pltpu.VMEM((ZFIRST, rank, cw), BF),
            pltpu.VMEM((ZFIRST, rank, cw), BF),
            pltpu.VMEM((rows, cols), F32),
            pltpu.SemaphoreType.DMA((FETCHES,)),
            pltpu.SemaphoreType.DMA((1,)),
            pltpu.SemaphoreType.DMA((RECVS,)),
            pltpu.SemaphoreType.REGULAR,
        ],
        compiler_params=pltpu.CompilerParams(
            collective_id=0, has_side_effects=True, vmem_limit_bytes=40 * 1024 * 1024
        ),
    )(*(
        pltpu.with_memory_space_constraint(x, pltpu.HBM)
        for x in (right_sides, leaf_inverse, project_factors, correct_factors, *couplings)
    ))


def solution(mesh):
    in_specs = (
        P("leaf", "rhs"),
        P(("leaf", "rhs"), None),
        P(None, "leaf", None),
        P(None, "leaf", None),
        P(None, "rhs", None),
        P(None, "rhs", None),
        P(None, "rhs", None),
    )
    out_specs = P("leaf", "rhs")
    return jax.shard_map(local, mesh=mesh, in_specs=in_specs, out_specs=out_specs, check_vma=False)
```

```python
import jax
import jax.numpy as jnp
from jax import lax
from jax.experimental import pallas as pl
from jax.experimental.pallas import tpu as pltpu
from jax.sharding import PartitionSpec as P

LEVELS = 3
CHUNKS = 4
SPLIT = ((0, 1), (1, 2), (3, 2), (5, 2), (7, 1))
UNITS = 8
ZFIRST = 3
RECVS = 37
FETCHES = 8
BF = jnp.bfloat16
F32 = jnp.float32


def mm(a, b):
    return jnp.dot(a, b, preferred_element_type=F32)


def bit_of(index, stride):
    return lax.rem(lax.div(index, stride), 2)


def flip(index, stride):
    return index + stride * (1 - 2 * bit_of(index, stride))


def span(which, size):
    return pl.ds(pl.multiple_of(which * size, size), size)


def kernel(
    b_hbm, a_hbm, p_hbm, c_hbm, w0_hbm, w1_hbm, w2_hbm, out_v,
    b_v, a_v, p_v, pt_v, w_v, g_v, gs_v, h_v, qf, q_s, q_r, q_v,
    pf, st0, p1f, p1_s, p1_r, p2f, p2_s, p2o, p2_r, st1, st2, a2_s, uf, u_s, u_r, acc,
    lsem, ssem, rsem, msem,
):
    i = lax.axis_index("leaf")
    r = lax.axis_index("rhs")
    blk = a_hbm.shape[0]
    depth = a_hbm.shape[1]
    cols = b_hbm.shape[1]
    rank = p_hbm.shape[2]
    cw = cols // CHUNKS
    hw = cw // 2
    half = depth // 2
    unit = depth // UNITS
    pieces = [pl.ds(at * unit, size * unit) for at, size in SPLIT]
    final = len(SPLIT) - 1
    mate = {"rhs": flip(r, 1)}
    across = {"rhs": flip(r, 2)}
    sib = {"leaf": flip(i, 1)}
    near = {"leaf": flip(i, 2)}
    far = {"leaf": flip(i, 4)}
    mid = {"leaf": flip(flip(i, 2), 4)}
    sides = [bit_of(i, 1), bit_of(i, 2), bit_of(i, 4)]
    core = bit_of(r, 1)
    chip = bit_of(r, 2)

    copies = []
    slots = {}

    def slot(key):
        return slots.setdefault(key, len(slots))

    def send(src, dst, to, key, extra=None, keep=True):
        place = slot(key) if extra is None else slot(key) + extra
        copy = pltpu.make_async_remote_copy(
            src_ref=src, dst_ref=dst, send_sem=ssem.at[0], recv_sem=rsem.at[place],
            device_id=to, device_id_type=pl.DeviceIdType.MESH,
        )
        copy.start()
        if keep:
            copies.append(copy)
        return copy

    def arrive(key, ref):
        pltpu.make_async_copy(ref, ref, rsem.at[slot(key)]).wait()

    def fetched(key, ref):
        pltpu.make_async_copy(ref, ref, lsem.at[places[key]]).wait()

    def share(ref, to, key):
        return send(ref, ref, to, key)

    places = {}

    def fetch(src, dst, key):
        copy = pltpu.make_async_copy(src, dst, lsem.at[places.setdefault(key, len(places))])
        copy.start()
        return copy

    mine = [span(s, rank) for s in sides]
    block = span(r, blk)
    pair_rows = span(chip, 2 * blk)
    other_rows = span(1 - chip, 2 * blk)
    half_cols = span(core, half)
    rest_cols = span(1 - core, half)

    la = fetch(a_hbm.at[:, rest_cols], a_v.at[block, rest_cols], "a")
    lo = fetch(a_hbm.at[:, half_cols], a_v.at[block, half_cols], "o")
    lp = [fetch(p_hbm.at[0], p_v.at[:, pl.ds(0, rank)], "p0")]
    [
        fetch(w_hbm.at[lax.div(i, 2 << level)], w_v.at[level, r], "w")
        for level, w_hbm in enumerate((w0_hbm, w1_hbm, w2_hbm))
    ]
    lp += [fetch(p_hbm.at[l], p_v.at[:, pl.ds(l * rank, rank)], f"p{l}") for l in range(1, LEVELS)]
    [fetch(c_hbm.at[l], a_v.at[:, pl.ds(depth + l * rank, rank)], "c") for l in range(LEVELS)]
    lb = fetch(b_hbm, b_v.at[pl.ds(0, depth)], "b")

    barrier = pltpu.get_barrier_semaphore()
    inner = lax.rem(sides[1] + sides[2], 2)
    for to in (mate, across, sib, near):
        pl.semaphore_signal(barrier, inc=1, device_id=to, device_id_type=pl.DeviceIdType.MESH)

    @pl.when(inner == 1)
    def _():
        pl.semaphore_signal(barrier, inc=1, device_id=mid, device_id_type=pl.DeviceIdType.MESH)

    la.wait()
    pl.semaphore_wait(barrier, 4 + inner)

    @pl.when(inner == 1)
    def _():
        pl.semaphore_signal(msem, inc=1, device_id=mid, device_id_type=pl.DeviceIdType.MESH)


    a_mate = share(a_v.at[block, rest_cols], mate, "am")
    lo.wait()
    a_across = [share(a_v.at[block, pieces[0]], across, "a1")]
    fetched("w", w_v.at[:, r])
    [share(w_v.at[l, r, :, mine[l]], across, "we") for l in range(2)]
    lp[0].wait()
    pt_v[0] = p_v[:, pl.ds(0, rank)].T
    a_mate.wait_recv()
    q_across = []
    for l in range(LEVELS):
        if l > 0:
            lp[l].wait()
            pt_v[l] = p_v[:, pl.ds(l * rank, rank)].T
        part = mm(pt_v[l, :, pair_rows], a_v[pair_rows, half_cols])
        qf[l] = part
        q_s[l] = part.astype(BF)
        q_across.append(send(q_s.at[l], q_r.at[l], across, f"q{l}"))
    a_mate2 = share(a_v.at[block, half_cols], mate, "an")
    w_mate = share(w_v.at[:, r], mate, "wg")
    [share(w_v.at[l, r, :, span(1 - sides[l], rank)], across, "wl") for l in range(2)]
    share(w_v.at[2, r], across, "wl")
    for k in range(1, len(SPLIT)):
        a_across.append(share(a_v.at[block, pieces[k]], across, f"a{k}"))

    fetched("c", a_v.at[:, pl.ds(depth, LEVELS * rank)])
    for n, (l, k) in enumerate(((1, 0), (2, 0), (2, 1))):
        g_v[n, :, mine[0]] = mm(pt_v[l], a_v[:, pl.ds(depth + k * rank, rank)]).astype(BF)
    g_send = share(g_v.at[:, :, mine[0]], sib, "wg")

    over = flip(r, 2)
    arrive("we", w_v.at[0, r])
    for l in range(2):
        share(w_v.at[l, over, :, mine[l]], mate, "re")
    lb.wait()
    a_mate2.wait_recv()
    for c in range(CHUNKS):
        own = pl.ds(c * cw, cw)
        acc[pair_rows, own] = mm(a_v[pair_rows, pl.ds(0, depth)], b_v[pl.ds(0, depth), own])

    def gather_q(l):
        q_across[l].wait_recv()
        q_v[l, core] = (qf[l] + q_r[l].astype(F32)).astype(BF)
        relayed = share(q_v.at[l, core], mate, f"m{l}")
        for c in range(CHUNKS):
            pf[c] = mm(q_v[l, core], b_v[half_cols, pl.ds(c * cw, cw)])
        relayed.wait_recv()

    def project(l, c):
        return pf[c] + mm(q_v[l, 1 - core], b_v[rest_cols, span(c, cw)])

    x1, z1, f1, u1, relay = {}, {}, {}, {}, {}

    def send0(c):
        share(st0.at[c, mine[0], :], sib, f"x{c // 2}")

    def send1(c):
        x1[c] = send(p1_s.at[c], p1_r.at[c], sib, f"y{c}")

    gather_q(0)
    for c in range(CHUNKS):
        st0[c, mine[0], :] = project(0, c).astype(BF)
        send0(c)

    both = (LEVELS * w0_hbm.shape[1] * w0_hbm.shape[2] + 3 * rank * rank) // cols
    arrive("wg", b_v.at[pl.ds(0, both)])
    arrive("re", w_v.at[0, r])
    w_cols = w_v[0, :, :, mine[0]].reshape(2 * rank, rank)
    for n in range(2):
        h_v[n] = mm(g_v[n], w_cols).astype(BF)
    pair_sum = g_v[2, :, pl.ds(0, rank)].astype(F32) + g_v[2, :, pl.ds(rank, rank)].astype(F32)
    gs_v[:, mine[1]] = pair_sum.astype(BF)
    gs_send = share(gs_v.at[:, mine[1]], near, "gs")

    def cross(c):
        z1[c] = send(p1_s.at[c], st1.at[c, mine[1], :], near, f"z{max(c, 1)}")

    gather_q(1)
    for c in range(CHUNKS):
        part = project(1, c) - mm(h_v[0], st0[c, mine[0], :])
        p1f[c] = part
        p1_s[c] = part.astype(BF)
        if c < ZFIRST:
            st1[c, mine[1], :] = part.astype(BF)
        if c < 2:
            cross(c)

    gs_send.wait_recv()
    h_v[2] = mm(gs_v[...], w_v[1, :, :, mine[1]].reshape(2 * rank, rank)).astype(BF)

    gather_q(2)
    spot = 2 * sides[1] + sides[0]
    spots = (3 - spot, flip(spot, 1), flip(spot, 2), spot)
    leaves = (flip(flip(i, 1), 2), flip(i, 1), flip(i, 2))
    odd_team = [{"leaf": leaf, "rhs": 2 * chip + 1} for leaf in leaves]
    odd_keys = [[slot(f"t{w}{h}") for h in range(2)] for w in range(2)]

    def part_of(who, h):
        return 2 * h + lax.div(who, 2), slice(None), span(lax.rem(who, 2), hw)

    for h in range(2):
        for c in (2 * h, 2 * h + 1):
            part = project(2, c) - mm(h_v[1], st0[c, mine[0], :]) - mm(h_v[2], p1_s[c])
            p2f[c] = part
            p2_s[c] = part.astype(BF)
        for n in range(3):
            send(p2_s.at[part_of(spots[n], h)], p2_r.at[core, h, n], odd_team[n], f"t0{h}", extra=2 * core)
        p2o[core, h] = p2f[part_of(spot, h)]

    @pl.when(core == 0)
    def _():
        send(p2o.at[0], p2o.at[0], mate, "tf", keep=False)

    cross(2)
    send1(3)
    arrive("wl", w_v.at[pl.ds(0, 2), r])
    for l in range(3):
        lanes = span(1 - sides[l], rank) if l < 2 else pl.ds(0, 2 * rank)
        share(w_v.at[l, over, :, lanes], mate, "rl")

    def answer_rows(l):
        return w_v[l, pl.ds(pl.multiple_of(sides[l] * 2, 2), 2), :, :].reshape(rank, 2 * rank)


    def first(pair):
        arrive(f"x{pair[0] // 2}", st0.at[pl.ds(pair[0], 2), mine[0], :])
        for c in pair:
            b_v[pl.ds(depth, rank), pl.ds(c * cw, cw)] = (-mm(answer_rows(0), st0[c])).astype(BF)

    def second_sum(c):
        x1[c].wait_recv()
        st1[c, mine[1], :] = (p1f[c] + p1_r[c].astype(F32)).astype(BF)
        z1[c] = share(st1.at[c, mine[1], :], near, f"z{c}")

    def second(c):
        z1[c].wait_recv()
        b_v[pl.ds(depth + rank, rank), pl.ds(c * cw, cw)] = (-mm(answer_rows(1), st1[c])).astype(BF)

    def second_part(c):
        if c == 0:
            arrive("z1", st1.at[pl.ds(0, 2), mine[1], :])
        elif c > 1:
            z1[c].wait_recv()
        part = mm(answer_rows(1), st1[c])
        uf[c] = part
        u_s[c] = part.astype(BF)
        u1[c] = send(u_s.at[c], u_r.at[c], sib, f"u{max(c, 1)}")

    def second_join(c):
        if c == 0:
            arrive("u1", u_r.at[pl.ds(0, 2)])
        elif c > 1:
            u1[c].wait_recv()
        b_v[pl.ds(depth + rank, rank), pl.ds(c * cw, cw)] = (-(uf[c] + u_r[c].astype(F32))).astype(BF)

    where = [(pl.ds(depth + 2 * rank, rank), span(4 * j + spot, hw)) for j in range(2)]
    same_team = [{"leaf": leaf} for leaf in leaves]
    even_team = [{"leaf": leaf, "rhs": flip(r, 1)} for leaf in leaves] + [mate]

    def third_far(w, j):
        total = p2o[w, j]
        arrive(f"t{w}{j}", p2_r.at[w, j])
        for n in range(3):
            total = total + p2_r[w, j, n].astype(F32)
        st2[w, j, mine[2], :] = total.astype(BF)
        ours = st2.at[w, j, mine[2], :]
        send(ours, ours, far, f"f{j}", keep=False)

    def third(w, j):
        if w == 0:
            arrive(f"f{j}", st2.at[:, j, mine[2], :])
        value = (-mm(answer_rows(2), st2[w, j])).astype(BF)
        if w == 1:
            b_v[where[j]] = value
            for to in same_team:
                send(b_v.at[where[j]], b_v.at[where[j]], to, f"n{j}", keep=False)
        else:
            a2_s[j] = value
            for to in even_team:
                send(a2_s.at[j], b_v.at[where[j]], to, f"n{j}", keep=False)

    def relay_piece(k):
        if k == 1:
            arrive("a1", a_v.at[block, pl.ds(0, SPLIT[2][0] * unit)])
        elif k > 1:
            a_across[k].wait_recv()
        relay[k] = share(a_v.at[span(over, blk), pieces[k]], mate, "rf" if k == final else "r")

    early = SPLIT[final][0] * unit

    def add_pieces():
        for c in range(CHUNKS):
            own = pl.ds(c * cw, cw)
            acc[other_rows, own] = mm(a_v[other_rows, pl.ds(0, early)], b_v[pl.ds(0, early), own])

    def add_last():
        deep = pieces[final]
        for c in range(CHUNKS):
            own = pl.ds(c * cw, cw)
            acc[other_rows, own] = acc[other_rows, own] + mm(a_v[other_rows, deep], b_v[deep, own])

    def finish(c):
        own = pl.ds(c * cw, cw)
        deep = pl.ds(depth, LEVELS * rank)
        out_v[:, own] = (acc[:, own] + mm(a_v[:, deep], b_v[deep, own])).astype(BF)

    arrive("rl", w_v.at[pl.ds(0, 2), r])
    first((0, 1))
    second_part(0)
    second_part(1)
    relay_piece(1)
    relay_piece(0)

    @pl.when(inner == 1)
    def _():
        pl.semaphore_wait(msem, 1)

    @pl.when(core == 1)
    def _():
        arrive("tf", p2o.at[0])
        for j in range(2):
            third_far(1, j)
            third_far(0, j)

    relay_piece(2)
    first((2, 3))
    second_part(2)
    second_sum(3)
    relay_piece(3)

    @pl.when(core == 1)
    def _():
        for j in range(2):
            third(0, j)
            third(1, j)

    second_join(0)
    second_join(1)
    relay_piece(final)
    arrive("r", a_v.at[block, pl.ds(0, early)])
    add_pieces()
    second(3)
    second_join(2)
    relay[final].wait_recv()
    add_last()
    answers = pl.ds(depth + 2 * rank, rank)

    for j in range(2):

        @pl.when(core == 1)
        def _():
            arrive(f"n{j}", b_v.at[answers, pl.ds(0, 3 * hw)])

        @pl.when(core == 0)
        def _():
            arrive(f"n{j}", b_v.at[answers, pl.ds(0, 4 * hw)])

        finish(2 * j)
        finish(2 * j + 1)
    assert len(slots) == RECVS and len(places) == FETCHES, (len(slots), len(places))
    for copy in copies:
        copy.wait_send()

    def sent(ref):
        pltpu.make_async_copy(ref, ref, ssem.at[0]).wait()

    @pl.when(core == 1)
    def _():
        for w in range(2):
            sent(b_v.at[answers, pl.ds(0, CHUNKS * cw)])
        sent(st2.at[0, 0])

    @pl.when(core == 0)
    def _():
        sent(p2o.at[0])


def local(right_sides, leaf_inverse, project_factors, correct_factors, *couplings):
    rows, cols = right_sides.shape
    blk, depth = leaf_inverse.shape
    levels, _, rank = project_factors.shape
    parts = lax.axis_size("rhs")
    cw = cols // CHUNKS
    whole = lambda dtype: pltpu.VMEM((CHUNKS, rank, cw), dtype)
    any_spec = pl.BlockSpec(memory_space=pltpu.HBM)
    return pl.pallas_call(
        kernel,
        out_shape=jax.ShapeDtypeStruct((rows, cols), BF),
        in_specs=[any_spec] * 7,
        out_specs=pl.BlockSpec(memory_space=pltpu.VMEM),
        scratch_shapes=[
            pltpu.VMEM((depth + levels * rank, cols), BF),
            pltpu.VMEM((rows, depth + levels * rank), BF),
            pltpu.VMEM((rows, levels * rank), BF),
            pltpu.VMEM((levels, rank, rows), BF),
            pltpu.VMEM((levels, parts) + couplings[0].shape[1:], BF),
            pltpu.VMEM((3, rank, 2 * rank), BF),
            pltpu.VMEM((rank, 2 * rank), BF),
            pltpu.VMEM((3, rank, rank), BF),
            pltpu.VMEM((levels, rank, depth // 2), F32),
            pltpu.VMEM((levels, rank, depth // 2), BF),
            pltpu.VMEM((levels, rank, depth // 2), BF),
            pltpu.VMEM((levels, 2, rank, depth // 2), BF),
            whole(F32),
            pltpu.VMEM((CHUNKS, 2 * rank, cw), BF),
            whole(F32), whole(BF), whole(BF),
            whole(F32), whole(BF), pltpu.VMEM((2, 2, rank, cw // 2), F32),
            pltpu.VMEM((2, 2, 3, rank, cw // 2), BF),
            pltpu.VMEM((CHUNKS, 2 * rank, cw), BF),
            pltpu.VMEM((2, 2, 2 * rank, cw // 2), BF),
            pltpu.VMEM((2, rank, cw // 2), BF),
            pltpu.VMEM((ZFIRST, rank, cw), F32),
            pltpu.VMEM((ZFIRST, rank, cw), BF),
            pltpu.VMEM((ZFIRST, rank, cw), BF),
            pltpu.VMEM((rows, cols), F32),
            pltpu.SemaphoreType.DMA((FETCHES,)),
            pltpu.SemaphoreType.DMA((1,)),
            pltpu.SemaphoreType.DMA((RECVS,)),
            pltpu.SemaphoreType.REGULAR,
        ],
        compiler_params=pltpu.CompilerParams(
            collective_id=0, has_side_effects=True, vmem_limit_bytes=40 * 1024 * 1024
        ),
    )(*(
        pltpu.with_memory_space_constraint(x, pltpu.HBM)
        for x in (right_sides, leaf_inverse, project_factors, correct_factors, *couplings)
    ))


def solution(mesh):
    in_specs = (
        P("leaf", "rhs"),
        P(("leaf", "rhs"), None),
        P(None, "leaf", None),
        P(None, "leaf", None),
        P(None, "rhs", None),
        P(None, "rhs", None),
        P(None, "rhs", None),
    )
    out_specs = P("leaf", "rhs")
    return jax.shard_map(local, mesh=mesh, in_specs=in_specs, out_specs=out_specs, check_vma=False)
```

```python
import jax
import jax.numpy as jnp
from jax import lax
from jax.experimental import pallas as pl
from jax.experimental.pallas import tpu as pltpu
from jax.sharding import PartitionSpec as P

LEVELS = 3
CHUNKS = 4
SPLIT = ((0, 1), (1, 2), (3, 2), (5, 2), (7, 1))
UNITS = 8
ZFIRST = 3
RECVS = 37
FETCHES = 8
BF = jnp.bfloat16
F32 = jnp.float32


def mm(a, b):
    return jnp.dot(a, b, preferred_element_type=F32)


def bit_of(index, stride):
    return lax.rem(lax.div(index, stride), 2)


def flip(index, stride):
    return index + stride * (1 - 2 * bit_of(index, stride))


def span(which, size):
    return pl.ds(pl.multiple_of(which * size, size), size)


def kernel(
    b_hbm, a_hbm, p_hbm, c_hbm, w0_hbm, w1_hbm, w2_hbm, out_v,
    b_v, a_v, p_v, pt_v, w_v, g_v, gs_v, h_v, qf, q_s, q_r, q_v,
    pf, st0, p1f, p1_s, p1_r, p2f, p2_s, p2o, p2_r, st1, st2, a2_s, uf, u_s, u_r, acc,
    lsem, ssem, rsem, msem,
):
    i = lax.axis_index("leaf")
    r = lax.axis_index("rhs")
    blk = a_hbm.shape[0]
    depth = a_hbm.shape[1]
    cols = b_hbm.shape[1]
    rank = p_hbm.shape[2]
    cw = cols // CHUNKS
    hw = cw // 2
    half = depth // 2
    unit = depth // UNITS
    pieces = [pl.ds(at * unit, size * unit) for at, size in SPLIT]
    final = len(SPLIT) - 1
    mate = {"rhs": flip(r, 1)}
    across = {"rhs": flip(r, 2)}
    sib = {"leaf": flip(i, 1)}
    near = {"leaf": flip(i, 2)}
    far = {"leaf": flip(i, 4)}
    mid = {"leaf": flip(flip(i, 2), 4)}
    sides = [bit_of(i, 1), bit_of(i, 2), bit_of(i, 4)]
    core = bit_of(r, 1)
    chip = bit_of(r, 2)

    copies = []
    slots = {}

    def slot(key):
        return slots.setdefault(key, len(slots))

    def send(src, dst, to, key, extra=None, keep=True):
        place = slot(key) if extra is None else slot(key) + extra
        copy = pltpu.make_async_remote_copy(
            src_ref=src, dst_ref=dst, send_sem=ssem.at[0], recv_sem=rsem.at[place],
            device_id=to, device_id_type=pl.DeviceIdType.MESH,
        )
        copy.start()
        if keep:
            copies.append(copy)
        return copy

    def arrive(key, ref):
        pltpu.make_async_copy(ref, ref, rsem.at[slot(key)]).wait()

    def fetched(key, ref):
        pltpu.make_async_copy(ref, ref, lsem.at[places[key]]).wait()

    def share(ref, to, key):
        return send(ref, ref, to, key)

    places = {}

    def fetch(src, dst, key):
        copy = pltpu.make_async_copy(src, dst, lsem.at[places.setdefault(key, len(places))])
        copy.start()
        return copy

    mine = [span(s, rank) for s in sides]
    block = span(r, blk)
    pair_rows = span(chip, 2 * blk)
    other_rows = span(1 - chip, 2 * blk)
    half_cols = span(core, half)
    rest_cols = span(1 - core, half)

    la = fetch(a_hbm.at[:, rest_cols], a_v.at[block, rest_cols], "a")
    lo = fetch(a_hbm.at[:, half_cols], a_v.at[block, half_cols], "o")
    lp = [fetch(p_hbm.at[0], p_v.at[:, pl.ds(0, rank)], "p0")]
    [
        fetch(w_hbm.at[lax.div(i, 2 << level)], w_v.at[level, r], "w")
        for level, w_hbm in enumerate((w0_hbm, w1_hbm, w2_hbm))
    ]
    lp += [fetch(p_hbm.at[l], p_v.at[:, pl.ds(l * rank, rank)], f"p{l}") for l in range(1, LEVELS)]
    [fetch(c_hbm.at[l], a_v.at[:, pl.ds(depth + l * rank, rank)], "c") for l in range(LEVELS)]
    lb = fetch(b_hbm, b_v.at[pl.ds(0, depth)], "b")

    barrier = pltpu.get_barrier_semaphore()
    inner = lax.rem(sides[1] + sides[2], 2)
    for to in (mate, across, sib, near):
        pl.semaphore_signal(barrier, inc=1, device_id=to, device_id_type=pl.DeviceIdType.MESH)

    @pl.when(inner == 1)
    def _():
        pl.semaphore_signal(barrier, inc=1, device_id=mid, device_id_type=pl.DeviceIdType.MESH)

    la.wait()
    pl.semaphore_wait(barrier, 4 + inner)

    @pl.when(inner == 1)
    def _():
        pl.semaphore_signal(msem, inc=1, device_id=mid, device_id_type=pl.DeviceIdType.MESH)


    a_mate = share(a_v.at[block, rest_cols], mate, "am")
    lo.wait()
    a_across = [share(a_v.at[block, pieces[0]], across, "a1")]
    fetched("w", w_v.at[:, r])
    [share(w_v.at[l, r, :, mine[l]], across, "we") for l in range(2)]
    lp[0].wait()
    pt_v[0] = p_v[:, pl.ds(0, rank)].T
    a_mate.wait_recv()
    q_across = []
    for l in range(LEVELS):
        if l > 0:
            lp[l].wait()
            pt_v[l] = p_v[:, pl.ds(l * rank, rank)].T
        part = mm(pt_v[l, :, pair_rows], a_v[pair_rows, half_cols])
        qf[l] = part
        q_s[l] = part.astype(BF)
        q_across.append(send(q_s.at[l], q_r.at[l], across, f"q{l}"))
    a_mate2 = share(a_v.at[block, half_cols], mate, "an")
    w_mate = share(w_v.at[:, r], mate, "wg")
    [share(w_v.at[l, r, :, span(1 - sides[l], rank)], across, "wl") for l in range(2)]
    share(w_v.at[2, r], across, "wl")
    for k in range(1, len(SPLIT)):
        a_across.append(share(a_v.at[block, pieces[k]], across, f"a{k}"))

    fetched("c", a_v.at[:, pl.ds(depth, LEVELS * rank)])
    for n, (l, k) in enumerate(((1, 0), (2, 0), (2, 1))):
        g_v[n, :, mine[0]] = mm(pt_v[l], a_v[:, pl.ds(depth + k * rank, rank)]).astype(BF)
    g_send = share(g_v.at[:, :, mine[0]], sib, "wg")

    over = flip(r, 2)
    arrive("we", w_v.at[0, r])
    for l in range(2):
        share(w_v.at[l, over, :, mine[l]], mate, "re")
    lb.wait()
    a_mate2.wait_recv()
    for c in range(CHUNKS):
        own = pl.ds(c * cw, cw)
        acc[pair_rows, own] = mm(a_v[pair_rows, pl.ds(0, depth)], b_v[pl.ds(0, depth), own])

    def gather_q(l):
        q_across[l].wait_recv()
        q_v[l, core] = (qf[l] + q_r[l].astype(F32)).astype(BF)
        relayed = share(q_v.at[l, core], mate, f"m{l}")
        for c in range(CHUNKS):
            pf[c] = mm(q_v[l, core], b_v[half_cols, pl.ds(c * cw, cw)])
        relayed.wait_recv()

    def project(l, c):
        return pf[c] + mm(q_v[l, 1 - core], b_v[rest_cols, span(c, cw)])

    x1, z1, f1, u1, relay = {}, {}, {}, {}, {}

    def send0(c):
        share(st0.at[c, mine[0], :], sib, f"x{c // 2}")

    def send1(c):
        x1[c] = send(p1_s.at[c], p1_r.at[c], sib, f"y{c}")

    gather_q(0)
    for c in range(CHUNKS):
        st0[c, mine[0], :] = project(0, c).astype(BF)
        send0(c)

    both = (LEVELS * w0_hbm.shape[1] * w0_hbm.shape[2] + 3 * rank * rank) // cols
    arrive("wg", b_v.at[pl.ds(0, both)])
    arrive("re", w_v.at[0, r])
    w_cols = w_v[0, :, :, mine[0]].reshape(2 * rank, rank)
    for n in range(2):
        h_v[n] = mm(g_v[n], w_cols).astype(BF)
    pair_sum = g_v[2, :, pl.ds(0, rank)].astype(F32) + g_v[2, :, pl.ds(rank, rank)].astype(F32)
    gs_v[:, mine[1]] = pair_sum.astype(BF)
    gs_send = share(gs_v.at[:, mine[1]], near, "gs")

    def cross(c):
        z1[c] = send(p1_s.at[c], st1.at[c, mine[1], :], near, f"z{max(c, 1)}")

    gather_q(1)
    for c in range(CHUNKS):
        part = project(1, c) - mm(h_v[0], st0[c, mine[0], :])
        p1f[c] = part
        p1_s[c] = part.astype(BF)
        if c < ZFIRST:
            st1[c, mine[1], :] = part.astype(BF)
        if c < 2:
            cross(c)

    gs_send.wait_recv()
    h_v[2] = mm(gs_v[...], w_v[1, :, :, mine[1]].reshape(2 * rank, rank)).astype(BF)

    gather_q(2)
    spot = 2 * sides[1] + sides[0]
    spots = (3 - spot, flip(spot, 1), flip(spot, 2), spot)
    leaves = (flip(flip(i, 1), 2), flip(i, 1), flip(i, 2))
    odd_team = [{"leaf": leaf, "rhs": 2 * chip + 1} for leaf in leaves]
    odd_keys = [[slot(f"t{w}{h}") for h in range(2)] for w in range(2)]

    def part_of(who, h):
        return 2 * h + lax.div(who, 2), slice(None), span(lax.rem(who, 2), hw)

    for h in range(2):
        for c in (2 * h, 2 * h + 1):
            part = project(2, c) - mm(h_v[1], st0[c, mine[0], :]) - mm(h_v[2], p1_s[c])
            p2f[c] = part
            p2_s[c] = part.astype(BF)
        for n in range(3):
            send(p2_s.at[part_of(spots[n], h)], p2_r.at[core, h, n], odd_team[n], f"t0{h}", extra=2 * core)
        p2o[core, h] = p2f[part_of(spot, h)]

    @pl.when(core == 0)
    def _():
        send(p2o.at[0], p2o.at[0], mate, "tf", keep=False)

    cross(2)
    send1(3)
    arrive("wl", w_v.at[pl.ds(0, 2), r])
    for l in range(3):
        lanes = span(1 - sides[l], rank) if l < 2 else pl.ds(0, 2 * rank)
        share(w_v.at[l, over, :, lanes], mate, "rl")

    def answer_rows(l):
        return w_v[l, pl.ds(pl.multiple_of(sides[l] * 2, 2), 2), :, :].reshape(rank, 2 * rank)


    def first(pair):
        arrive(f"x{pair[0] // 2}", st0.at[pl.ds(pair[0], 2), mine[0], :])
        for c in pair:
            b_v[pl.ds(depth, rank), pl.ds(c * cw, cw)] = (-mm(answer_rows(0), st0[c])).astype(BF)

    def second_sum(c):
        x1[c].wait_recv()
        st1[c, mine[1], :] = (p1f[c] + p1_r[c].astype(F32)).astype(BF)
        z1[c] = share(st1.at[c, mine[1], :], near, f"z{c}")

    def second(c):
        z1[c].wait_recv()
        b_v[pl.ds(depth + rank, rank), pl.ds(c * cw, cw)] = (-mm(answer_rows(1), st1[c])).astype(BF)

    def second_part(c):
        if c == 0:
            arrive("z1", st1.at[pl.ds(0, 2), mine[1], :])
        elif c > 1:
            z1[c].wait_recv()
        part = mm(answer_rows(1), st1[c])
        uf[c] = part
        u_s[c] = part.astype(BF)
        u1[c] = send(u_s.at[c], u_r.at[c], sib, f"u{max(c, 1)}")

    def second_join(c):
        if c == 0:
            arrive("u1", u_r.at[pl.ds(0, 2)])
        elif c > 1:
            u1[c].wait_recv()
        b_v[pl.ds(depth + rank, rank), pl.ds(c * cw, cw)] = (-(uf[c] + u_r[c].astype(F32))).astype(BF)

    where = [(pl.ds(depth + 2 * rank, rank), span(4 * j + spot, hw)) for j in range(2)]
    same_team = [{"leaf": leaf} for leaf in leaves]
    even_team = [{"leaf": leaf, "rhs": flip(r, 1)} for leaf in leaves] + [mate]

    def third_far(w, j):
        total = p2o[w, j]
        arrive(f"t{w}{j}", p2_r.at[w, j])
        for n in range(3):
            total = total + p2_r[w, j, n].astype(F32)
        st2[w, j, mine[2], :] = total.astype(BF)
        ours = st2.at[w, j, mine[2], :]
        send(ours, ours, far, f"f{j}", keep=False)

    def third(w, j):
        if w == 0:
            arrive(f"f{j}", st2.at[:, j, mine[2], :])
        value = (-mm(answer_rows(2), st2[w, j])).astype(BF)
        if w == 1:
            b_v[where[j]] = value
            for to in same_team:
                send(b_v.at[where[j]], b_v.at[where[j]], to, f"n{j}", keep=False)
        else:
            a2_s[j] = value
            for to in even_team:
                send(a2_s.at[j], b_v.at[where[j]], to, f"n{j}", keep=False)

    def relay_piece(k):
        if k == 1:
            arrive("a1", a_v.at[block, pl.ds(0, SPLIT[2][0] * unit)])
        elif k > 1:
            a_across[k].wait_recv()
        relay[k] = share(a_v.at[span(over, blk), pieces[k]], mate, "rf" if k == final else "r")

    early = SPLIT[final][0] * unit

    def add_pieces():
        for c in range(CHUNKS):
            own = pl.ds(c * cw, cw)
            acc[other_rows, own] = mm(a_v[other_rows, pl.ds(0, early)], b_v[pl.ds(0, early), own])

    def add_last():
        deep = pieces[final]
        for c in range(CHUNKS):
            own = pl.ds(c * cw, cw)
            acc[other_rows, own] = acc[other_rows, own] + mm(a_v[other_rows, deep], b_v[deep, own])

    def finish(c):
        own = pl.ds(c * cw, cw)
        deep = pl.ds(depth, LEVELS * rank)
        out_v[:, own] = (acc[:, own] + mm(a_v[:, deep], b_v[deep, own])).astype(BF)

    arrive("rl", w_v.at[pl.ds(0, 2), r])
    first((0, 1))
    second_part(0)
    second_part(1)
    relay_piece(1)
    relay_piece(0)

    @pl.when(inner == 1)
    def _():
        pl.semaphore_wait(msem, 1)

    @pl.when(core == 1)
    def _():
        arrive("tf", p2o.at[0])
        for j in range(2):
            for w in ((1, 0) if j == 0 else (0, 1)):
                third_far(w, j)

    relay_piece(2)
    first((2, 3))
    second_sum(3)
    second_part(2)
    relay_piece(3)

    @pl.when(core == 1)
    def _():
        for j in range(2):
            third(0, j)
            third(1, j)

    second_join(0)
    second_join(1)
    relay_piece(final)
    arrive("r", a_v.at[block, pl.ds(0, early)])
    add_pieces()
    second(3)
    second_join(2)
    relay[final].wait_recv()
    add_last()
    answers = pl.ds(depth + 2 * rank, rank)

    for j in range(2):

        @pl.when(core == 1)
        def _():
            arrive(f"n{j}", b_v.at[answers, pl.ds(0, 3 * hw)])

        @pl.when(core == 0)
        def _():
            arrive(f"n{j}", b_v.at[answers, pl.ds(0, 4 * hw)])

        finish(2 * j)
        finish(2 * j + 1)
    assert len(slots) == RECVS and len(places) == FETCHES, (len(slots), len(places))
    for copy in copies:
        copy.wait_send()

    def sent(ref):
        pltpu.make_async_copy(ref, ref, ssem.at[0]).wait()

    @pl.when(core == 1)
    def _():
        for w in range(2):
            sent(b_v.at[answers, pl.ds(0, CHUNKS * cw)])
        sent(st2.at[0, 0])

    @pl.when(core == 0)
    def _():
        sent(p2o.at[0])


def local(right_sides, leaf_inverse, project_factors, correct_factors, *couplings):
    rows, cols = right_sides.shape
    blk, depth = leaf_inverse.shape
    levels, _, rank = project_factors.shape
    parts = lax.axis_size("rhs")
    cw = cols // CHUNKS
    whole = lambda dtype: pltpu.VMEM((CHUNKS, rank, cw), dtype)
    any_spec = pl.BlockSpec(memory_space=pltpu.HBM)
    return pl.pallas_call(
        kernel,
        out_shape=jax.ShapeDtypeStruct((rows, cols), BF),
        in_specs=[any_spec] * 7,
        out_specs=pl.BlockSpec(memory_space=pltpu.VMEM),
        scratch_shapes=[
            pltpu.VMEM((depth + levels * rank, cols), BF),
            pltpu.VMEM((rows, depth + levels * rank), BF),
            pltpu.VMEM((rows, levels * rank), BF),
            pltpu.VMEM((levels, rank, rows), BF),
            pltpu.VMEM((levels, parts) + couplings[0].shape[1:], BF),
            pltpu.VMEM((3, rank, 2 * rank), BF),
            pltpu.VMEM((rank, 2 * rank), BF),
            pltpu.VMEM((3, rank, rank), BF),
            pltpu.VMEM((levels, rank, depth // 2), F32),
            pltpu.VMEM((levels, rank, depth // 2), BF),
            pltpu.VMEM((levels, rank, depth // 2), BF),
            pltpu.VMEM((levels, 2, rank, depth // 2), BF),
            whole(F32),
            pltpu.VMEM((CHUNKS, 2 * rank, cw), BF),
            whole(F32), whole(BF), whole(BF),
            whole(F32), whole(BF), pltpu.VMEM((2, 2, rank, cw // 2), F32),
            pltpu.VMEM((2, 2, 3, rank, cw // 2), BF),
            pltpu.VMEM((CHUNKS, 2 * rank, cw), BF),
            pltpu.VMEM((2, 2, 2 * rank, cw // 2), BF),
            pltpu.VMEM((2, rank, cw // 2), BF),
            pltpu.VMEM((ZFIRST, rank, cw), F32),
            pltpu.VMEM((ZFIRST, rank, cw), BF),
            pltpu.VMEM((ZFIRST, rank, cw), BF),
            pltpu.VMEM((rows, cols), F32),
            pltpu.SemaphoreType.DMA((FETCHES,)),
            pltpu.SemaphoreType.DMA((1,)),
            pltpu.SemaphoreType.DMA((RECVS,)),
            pltpu.SemaphoreType.REGULAR,
        ],
        compiler_params=pltpu.CompilerParams(
            collective_id=0, has_side_effects=True, vmem_limit_bytes=40 * 1024 * 1024
        ),
    )(*(
        pltpu.with_memory_space_constraint(x, pltpu.HBM)
        for x in (right_sides, leaf_inverse, project_factors, correct_factors, *couplings)
    ))


def solution(mesh):
    in_specs = (
        P("leaf", "rhs"),
        P(("leaf", "rhs"), None),
        P(None, "leaf", None),
        P(None, "leaf", None),
        P(None, "rhs", None),
        P(None, "rhs", None),
        P(None, "rhs", None),
    )
    out_specs = P("leaf", "rhs")
    return jax.shard_map(local, mesh=mesh, in_specs=in_specs, out_specs=out_specs, check_vma=False)
```
